16 devices in a mesh: dp: 2 (over z), tp: 8 (over y, x, core).
Axes of the slice: x: 2, y: 2, z: 2, core: 2. Of those that a mesh axis runs over, the one named last changes fastest.
Arguments:
- hidden: bfloat16 [320, 512], P('dp'), parts along dimension 0
- positions: int32 [320], P('dp'), parts along dimension 0
- self_keys: bfloat16 [2, 320, 448, 8, 64], P(None, 'dp', None, 'tp'), parts along dimension 1
- self_vals: bfloat16 [2, 320, 448, 8, 64], P(None, 'dp', None, 'tp'), parts along dimension 1
- cross_keys: bfloat16 [2, 64, 1500, 8, 64], P(None, 'dp', None, 'tp'), parts along dimension 1
- cross_vals: bfloat16 [2, 64, 1500, 8, 64], P(None, 'dp', None, 'tp'), parts along dimension 1
- ln_gain: bfloat16 [2, 3, 512], replicated
- ln_bias: bfloat16 [2, 3, 512], replicated
- w_query: bfloat16 [2, 512, 512], P(None, None, 'tp')
- b_query: bfloat16 [2, 512], P(None, 'tp')
- w_key: bfloat16 [2, 512, 512], P(None, None, 'tp')
- w_value: bfloat16 [2, 512, 512], P(None, None, 'tp')
- b_value: bfloat16 [2, 512], P(None, 'tp')
- w_out: bfloat16 [2, 512, 512], P(None, 'tp')
- b_out: bfloat16 [2, 512], replicated
- w_cquery: bfloat16 [2, 512, 512], P(None, None, 'tp')
- b_cquery: bfloat16 [2, 512], P(None, 'tp')
- w_cout: bfloat16 [2, 512, 512], P(None, 'tp')
- b_cout: bfloat16 [2, 512], replicated
- w_fc1: bfloat16 [2, 512, 2048], P(None, None, 'tp')
- b_fc1: bfloat16 [2, 2048], P(None, 'tp')
- w_fc2: bfloat16 [2, 2048, 512], P(None, 'tp')
- b_fc2: bfloat16 [2, 512], replicated
Outputs:
- output 1: bfloat16 [320, 512], P('dp'), parts along dimension 0
- output 2: bfloat16 [2, 320, 448, 8, 64], P(None, 'dp', None, 'tp'), parts along dimension 1
- output 3: bfloat16 [2, 320, 448, 8, 64], P(None, 'dp', None, 'tp'), parts along dimension 1
There are 2 independent parts. The reference program is written for one: setup_inputs(seed, part) draws one part's arguments, and reference() takes and returns one part's arrays. A program takes and returns all parts, laid end to end along the dimension named above; an argument that names none is the same for every part.
All inputs are finite; a program needn't handle non-finite values.
Results may differ from the reference program's by a relative error of at most 0.02.
Values are sent between devices in bfloat16 or wider.
A program may use at most 1 GiB of HBM per device.

```python
import jax
import jax.numpy as jnp
from jax import lax

D = 512
HEADS = 8
HEAD = 64
FF = 2048
FRAMES = 1500
CTX = 448
BEAMS = 5
AUDIOS = 32
LAYERS = 2

BATCH = AUDIOS * BEAMS
QK_SCALE = HEAD ** -0.25
EPS = 1e-5


def setup_inputs(seed: int = 0, part: int = 0) -> dict:
    part_keys = jax.random.split(jax.random.fold_in(jax.random.key(seed), part), 6)
    shared_keys = jax.random.split(jax.random.key(seed + 1), 17)

    def draw_array(key, shape, scale, offset=0.0):
        return (offset + scale * jax.random.normal(key, shape, jnp.float32)).astype(jnp.bfloat16)

    audio_pos = jax.random.randint(part_keys[1], (AUDIOS,), 3, CTX - 7)
    positions = jnp.repeat(audio_pos, BEAMS).astype(jnp.int32)
    cache_shape = (LAYERS, BATCH, CTX, HEADS, HEAD)
    cross_shape = (LAYERS, AUDIOS, FRAMES, HEADS, HEAD)
    width_scale = D ** -0.5
    return {
        'hidden': draw_array(part_keys[0], (BATCH, D), 1.0),
        'positions': positions,
        'self_keys': draw_array(part_keys[2], cache_shape, 0.3),
        'self_vals': draw_array(part_keys[3], cache_shape, 1.0),
        'cross_keys': draw_array(part_keys[4], cross_shape, 1.0),
        'cross_vals': draw_array(part_keys[5], cross_shape, 1.0),
        'ln_gain': draw_array(shared_keys[0], (LAYERS, 3, D), 0.3, 1.0),
        'ln_bias': draw_array(shared_keys[1], (LAYERS, 3, D), 0.3),
        'w_query': draw_array(shared_keys[2], (LAYERS, D, D), width_scale),
        'b_query': draw_array(shared_keys[3], (LAYERS, D), 0.3),
        'w_key': draw_array(shared_keys[4], (LAYERS, D, D), 2.0 * width_scale),
        'w_value': draw_array(shared_keys[5], (LAYERS, D, D), width_scale),
        'b_value': draw_array(shared_keys[6], (LAYERS, D), 1.0),
        'w_out': draw_array(shared_keys[7], (LAYERS, D, D), width_scale),
        'b_out': draw_array(shared_keys[8], (LAYERS, D), 0.3),
        'w_cquery': draw_array(shared_keys[9], (LAYERS, D, D), width_scale),
        'b_cquery': draw_array(shared_keys[10], (LAYERS, D), 0.3),
        'w_cout': draw_array(shared_keys[11], (LAYERS, D, D), width_scale),
        'b_cout': draw_array(shared_keys[12], (LAYERS, D), 0.3),
        'w_fc1': draw_array(shared_keys[13], (LAYERS, D, FF), width_scale),
        'b_fc1': draw_array(shared_keys[14], (LAYERS, FF), 0.3),
        'w_fc2': draw_array(shared_keys[15], (LAYERS, FF, D), FF ** -0.5),
        'b_fc2': draw_array(shared_keys[16], (LAYERS, D), 0.3),
    }


def layer_norm(values, gain_row, bias_row):
    wide_vals = values.astype(jnp.float32)
    center = wide_vals - jnp.mean(wide_vals, axis=-1, keepdims=True)
    var_est = jnp.mean(center * center, axis=-1, keepdims=True)
    return (center * lax.rsqrt(var_est + EPS) * gain_row.astype(jnp.float32) + bias_row.astype(jnp.float32)).astype(jnp.bfloat16)


def project(normed, weight, bias_row):
    return jnp.dot(normed, weight, preferred_element_type=jnp.float32) + bias_row.astype(jnp.float32)


def reference(hidden, positions, self_keys, self_vals, cross_keys, cross_vals, ln_gain, ln_bias, w_query, b_query, w_key, w_value, b_value, w_out, b_out, w_cquery, b_cquery, w_cout, b_cout, w_fc1, b_fc1, w_fc2, b_fc2):
    slot_ids = jnp.arange(CTX)[None, :]
    slot_hit = (slot_ids == positions[:, None])[:, :, None, None]
    slot_mask = (slot_ids <= positions[:, None])[:, None, :]

    def one_layer(hidden_in, layer_w):
        normed = layer_norm(hidden_in, layer_w['ln_gain'][0], layer_w['ln_bias'][0])
        query_heads = (project(normed, layer_w['w_query'], layer_w['b_query']) * QK_SCALE).astype(jnp.bfloat16).reshape(BATCH, HEADS, HEAD)
        new_key = (jnp.dot(normed, layer_w['w_key'], preferred_element_type=jnp.float32) * QK_SCALE).astype(jnp.bfloat16).reshape(BATCH, 1, HEADS, HEAD)
        new_val = project(normed, layer_w['w_value'], layer_w['b_value']).astype(jnp.bfloat16).reshape(BATCH, 1, HEADS, HEAD)
        cache_k = jnp.where(slot_hit, new_key, layer_w['cache_k'])
        cache_v = jnp.where(slot_hit, new_val, layer_w['cache_v'])
        raw_scores = jnp.einsum('bhd,bshd->bhs', query_heads.astype(jnp.float32), cache_k.astype(jnp.float32))
        attn_probs = jax.nn.softmax(jnp.where(slot_mask, raw_scores, -1e30), axis=-1).astype(jnp.bfloat16)
        attn_out = jnp.einsum('bhs,bshd->bhd', attn_probs.astype(jnp.float32), cache_v.astype(jnp.float32)).astype(jnp.bfloat16).reshape(BATCH, HEADS * HEAD)
        hidden_mid = (hidden_in.astype(jnp.float32) + project(attn_out, layer_w['w_out'], layer_w['b_out'])).astype(jnp.bfloat16)

        normed = layer_norm(hidden_mid, layer_w['ln_gain'][1], layer_w['ln_bias'][1])
        cross_query = (project(normed, layer_w['w_cquery'], layer_w['b_cquery']) * QK_SCALE).astype(jnp.bfloat16).reshape(AUDIOS, BEAMS, HEADS, HEAD)
        cross_scores = jnp.einsum('abhd,afhd->abhf', cross_query.astype(jnp.float32), layer_w['cross_k'].astype(jnp.float32))
        cross_probs = jax.nn.softmax(cross_scores, axis=-1).astype(jnp.bfloat16)
        cross_out = jnp.einsum('abhf,afhd->abhd', cross_probs.astype(jnp.float32), layer_w['cross_v'].astype(jnp.float32)).astype(jnp.bfloat16).reshape(BATCH, HEADS * HEAD)
        hidden_mid = (hidden_mid.astype(jnp.float32) + project(cross_out, layer_w['w_cout'], layer_w['b_cout'])).astype(jnp.bfloat16)

        normed = layer_norm(hidden_mid, layer_w['ln_gain'][2], layer_w['ln_bias'][2])
        mlp_inner = jax.nn.gelu(project(normed, layer_w['w_fc1'], layer_w['b_fc1']), approximate=False).astype(jnp.bfloat16)
        hidden_next = (hidden_mid.astype(jnp.float32) + project(mlp_inner, layer_w['w_fc2'], layer_w['b_fc2'])).astype(jnp.bfloat16)
        return hidden_next, (cache_k, cache_v)

    layer_stack = {'cache_k': self_keys, 'cache_v': self_vals, 'cross_k': cross_keys, 'cross_v': cross_vals, 'ln_gain': ln_gain, 'ln_bias': ln_bias, 'w_query': w_query, 'b_query': b_query, 'w_key': w_key, 'w_value': w_value, 'b_value': b_value, 'w_out': w_out, 'b_out': b_out, 'w_cquery': w_cquery, 'b_cquery': b_cquery, 'w_cout': w_cout, 'b_cout': b_cout, 'w_fc1': w_fc1, 'b_fc1': b_fc1, 'w_fc2': w_fc2, 'b_fc2': b_fc2}
    hidden_out, cache_pair = lax.scan(one_layer, hidden, layer_stack)
    return hidden_out, cache_pair[0], cache_pair[1]
```

```python
import functools

import jax
import jax.numpy as jnp
from jax import lax
from jax.experimental import pallas as pl
from jax.experimental.pallas import tpu as pltpu
from jax.sharding import PartitionSpec as P

EPS = 1e-5
F32 = jnp.float32
BF16 = jnp.bfloat16
NT = (((1,), (1,)), ((), ()))
MESH = pl.DeviceIdType.MESH
PARAM_NAMES = ('ln_gain', 'ln_bias', 'w_query', 'b_query', 'w_key', 'w_value', 'b_value', 'w_out', 'b_out', 'w_cquery', 'b_cquery', 'w_cout', 'b_cout', 'w_fc1', 'b_fc1', 'w_fc2', 'b_fc2')

BATCH = 160
AUD = 32
BEAMS = 5
HD = 64
CTX = 448
FRAMES = 1500
D = 512
TP = 8
SCALE = HD ** -0.25
GB = 8
GROUPS = BATCH // GB
GA = 8
AGROUPS = AUD // GA
GR = GA * BEAMS


def layer_norm(wide, gain, bias):
    center = wide - jnp.mean(wide, axis=-1, keepdims=True)
    var_est = jnp.mean(center * center, axis=-1, keepdims=True)
    return (center * lax.rsqrt(var_est + EPS) * gain + bias).astype(BF16)


def row_of(ref, *idx):
    return ref[idx].astype(F32)


def dot_nt(a, b):
    return lax.dot_general(a, b, NT, preferred_element_type=F32)


def dot(a, b):
    return jnp.dot(a, b, preferred_element_type=F32)


def fold_heads(wide, keep):
    wide = jnp.where(keep, wide, 0.0)
    part = (wide[:, 0:128] + wide[:, 128:256]) + (wide[:, 256:384] + wide[:, 384:512])
    return part[:, :HD] + part[:, HD:]


def self_kernel(layer, pos_ref, h_ref, gain_ref, bias_ref, wq_ref, bq_ref, wk_ref, wv_ref, bv_ref, kin, vin, *rest):
    if layer:
        rest = rest[2:]
    o_ref, kout, vout, kbuf, vbuf, q_scr, a_scr, kt_scr, vt_scr, o_scr, in_sem, out_sem = rest

    def rows(g):
        return pl.ds(pl.multiple_of(g * GB, GB), GB)

    def fetch(g, which):
        src, buf = ((kin, kbuf), (vin, vbuf))[which]
        return pltpu.make_async_copy(src.at[layer, rows(g)], buf.at[rows(g)], in_sem.at[which, g])

    def put(g, which):
        buf, dst = ((kbuf, kout), (vbuf, vout))[which]
        return pltpu.make_async_copy(buf.at[rows(g)], dst.at[layer, rows(g)], out_sem.at[which, g])

    def start_fetch(g, carry):
        fetch(g, 0).start()
        fetch(g, 1).start()
        return carry

    lax.fori_loop(0, GROUPS, start_fetch, 0)

    normed = layer_norm(h_ref[...].astype(F32), row_of(gain_ref, 0, pl.ds(layer, 1)), row_of(bias_ref, 0, pl.ds(layer, 1)))
    query = ((dot_nt(normed, wq_ref[layer]) + row_of(bq_ref, pl.ds(layer, 1))) * SCALE).astype(BF16).astype(F32)
    q_scr[...] = jnp.concatenate([query, query], axis=1)
    a_scr[...] = normed.astype(F32)
    eye = lax.broadcasted_iota(jnp.int32, (HD, HD), 0) == lax.broadcasted_iota(jnp.int32, (HD, HD), 1)
    bv_col = jnp.sum(jnp.where(eye, row_of(bv_ref, pl.ds(layer, 1)), 0.0), axis=1, keepdims=True)

    def project(g, carry):
        part = a_scr[rows(g)].astype(BF16)
        kt_scr[g] = dot_nt(wk_ref[layer], part) * SCALE
        vt_scr[g] = dot_nt(wv_ref[layer], part) + bv_col
        return carry

    lax.fori_loop(0, GROUPS, project, 0, unroll=4)

    lane128 = lax.broadcasted_iota(jnp.int32, (HD, 128), 1)
    lane64 = lax.broadcasted_iota(jnp.int32, (HD, HD), 1) + 384
    lane_ctx = lax.broadcasted_iota(jnp.int32, (GB, CTX), 1)
    row_id = lax.broadcasted_iota(jnp.int32, (GB, 1), 0)
    keep = lax.broadcasted_iota(jnp.int32, (GB, D), 1) // HD == lax.broadcasted_iota(jnp.int32, (GB, D), 0)

    def attend(g, carry):
        fetch(g, 0).wait()
        fetch(g, 1).wait()
        pos_col = jnp.zeros((GB, 1), jnp.int32)
        for j in range(GB):
            beam = g * GB + j
            pos = pos_ref[beam]
            pos_col = jnp.where(row_id == j, pos, pos_col)
            off = pl.multiple_of(jnp.minimum(pos // 128, 2) * 128, 128)
            for buf, col_scr in ((kbuf, kt_scr), (vbuf, vt_scr)):
                col = jnp.broadcast_to(col_scr[g][:, j:j + 1], (HD, 128)).astype(BF16)
                view = buf.at[beam, :, pl.ds(off, 128)]
                view[...] = jnp.where(lane128 + off == pos, col, view[...])
                tail = buf.at[beam, :, pl.ds(384, 64)]
                tail[...] = jnp.where(lane64 == pos, col[:, :HD], tail[...])
        q8 = q_scr[rows(g)]
        qblk = jnp.where(keep, jnp.concatenate([q8, q8, q8, q8], axis=1), 0.0).astype(BF16)
        score = dot(qblk, kbuf[rows(g)].reshape(GB * HD, CTX))
        score = jnp.where(lane_ctx <= pos_col, score, -1e30)
        expd = jnp.exp(score - jnp.max(score, axis=1, keepdims=True))
        probs = (expd / jnp.sum(expd, axis=1, keepdims=True)).astype(BF16)
        wide = dot_nt(probs, vbuf[rows(g)].reshape(GB * HD, CTX))
        o_scr[rows(g)] = fold_heads(wide, keep)
        put(g, 0).start()
        put(g, 1).start()
        return carry

    lax.fori_loop(0, GROUPS, attend, 0)
    o_ref[...] = jnp.concatenate([o_scr[0:80], o_scr[80:160]], axis=1).astype(BF16)

    def finish(g, carry):
        put(g, 0).wait()
        put(g, 1).wait()
        return carry

    lax.fori_loop(0, GROUPS, finish, 0)


def erf_gelu(x):
    return 0.5 * x * (1.0 + lax.erf(x * (2.0 ** -0.5)))


def mid_kernel(layer, h_ref, o_ref, gain_ref, bias_ref, wo_ref, bo_ref, wcq_ref, bcq_ref, wco_ref, bco_ref, w1_ref, b1_ref, w2_ref, b2_ref,
               kin, vin, out_ref, kbuf, vbuf, wofull, wcofull, obuf1, obuf2, o2_ref, q_scr, o_scr, pbuf, rbuf, base_scr, hblk, hfull,
               ck_sem, send_sem, recv_sem):
    me = lax.axis_index('tp')
    peers = [lax.rem(me + d, TP) for d in range(1, TP)]

    def auds(g):
        return pl.ds(pl.multiple_of(g * GA, GA), GA)

    def fetch(g, which):
        src, buf = ((kin, kbuf), (vin, vbuf))[which]
        return pltpu.make_async_copy(src.at[layer, auds(g)], buf.at[auds(g)], ck_sem.at[which, g])

    for g in range(AGROUPS):
        fetch(g, 0).start()
        fetch(g, 1).start()

    barrier = pltpu.get_barrier_semaphore()
    for peer in peers:
        pl.semaphore_signal(barrier, inc=1, device_id={'tp': peer}, device_id_type=MESH)
    pl.semaphore_wait(barrier, TP - 1)

    def send(phase, src, dst, peer):
        return pltpu.make_async_remote_copy(src_ref=src, dst_ref=dst, send_sem=send_sem.at[phase, peer], recv_sem=recv_sem.at[phase, me],
                                            device_id={'tp': peer}, device_id_type=MESH)

    def arrival(phase, dst, peer):
        return pltpu.make_async_remote_copy(src_ref=dst, dst_ref=dst, send_sem=send_sem.at[phase, peer], recv_sem=recv_sem.at[phase, peer],
                                            device_id={'tp': peer}, device_id_type=MESH)

    def gather_start(phase, src, slots):
        for peer in peers:
            send(phase, src, slots.at[me], peer).start()

    def gather_wait(phase, src, slots):
        for peer in peers:
            arrival(phase, slots.at[peer], peer).wait_recv()
        for peer in peers:
            send(phase, src, slots.at[me], peer).wait_send()

    gather_start(0, o_ref, obuf1)
    gather_start(1, wo_ref.at[layer], wofull)
    gather_start(2, wco_ref.at[layer], wcofull)
    obuf1[me] = o_ref[...]
    wofull[me] = wo_ref[layer]
    wcofull[me] = wco_ref[layer]

    low = lax.broadcasted_iota(jnp.int32, (80, 128), 1) < HD

    def head_rows(slots):
        top, bottom = [], []
        for pair in range(TP // 2):
            left = slots[2 * pair].astype(F32)
            right = slots[2 * pair + 1].astype(F32)
            top.append(jnp.where(low, left, pltpu.roll(right, HD, 1)))
            bottom.append(jnp.where(low, pltpu.roll(left, HD, 1), right))
        return jnp.concatenate([jnp.concatenate(top, axis=1), jnp.concatenate(bottom, axis=1)], axis=0).astype(BF16)

    gather_wait(0, o_ref, obuf1)
    gather_wait(1, wo_ref.at[layer], wofull)
    hid = h_ref[...].astype(F32) + (dot(head_rows(obuf1), wofull[...].reshape(D, D)) + row_of(bo_ref, pl.ds(layer, 1)))
    hid = hid.astype(BF16).astype(F32)
    normed = layer_norm(hid, row_of(gain_ref, 1, pl.ds(layer, 1)), row_of(bias_ref, 1, pl.ds(layer, 1)))
    query = ((dot_nt(normed, wcq_ref[layer]) + row_of(bcq_ref, pl.ds(layer, 1))) * SCALE).astype(BF16).astype(F32)
    q_scr[...] = jnp.concatenate([query, query], axis=1)

    keep = lax.broadcasted_iota(jnp.int32, (GR, D), 1) // HD == lax.broadcasted_iota(jnp.int32, (GR, D), 0) // BEAMS

    def attend(g, carry):
        fetch(g, 0).wait()
        fetch(g, 1).wait()
        rows = pl.ds(pl.multiple_of(g * GR, GR), GR)
        q40 = q_scr[rows]
        qblk = jnp.where(keep, jnp.concatenate([q40, q40, q40, q40], axis=1), 0.0).astype(BF16)
        score = dot(qblk, kbuf[auds(g)].reshape(GA * HD, FRAMES))
        expd = jnp.exp(score - jnp.max(score, axis=1, keepdims=True))
        probs = (expd / jnp.sum(expd, axis=1, keepdims=True)).astype(BF16)
        wide = dot_nt(probs, vbuf[auds(g)].reshape(GA * HD, FRAMES))
        o_scr[rows] = fold_heads(wide, keep)
        return carry

    lax.fori_loop(0, AGROUPS, attend, 0)
    o2_ref[...] = jnp.concatenate([o_scr[0:80], o_scr[80:160]], axis=1).astype(BF16)
    gather_start(3, o2_ref, obuf2)
    obuf2[me] = o2_ref[...]
    gather_wait(2, wco_ref.at[layer], wcofull)
    gather_wait(3, o2_ref, obuf2)
    hid = hid + (dot(head_rows(obuf2), wcofull[...].reshape(D, D)) + row_of(bco_ref, pl.ds(layer, 1)))
    hid = hid.astype(BF16).astype(F32)

    normed = layer_norm(hid, row_of(gain_ref, 2, pl.ds(layer, 1)), row_of(bias_ref, 2, pl.ds(layer, 1)))
    inner = erf_gelu(dot(normed, w1_ref[layer]) + row_of(b1_ref, pl.ds(layer, 1))).astype(BF16)
    part = dot(inner, w2_ref[layer]).astype(BF16)
    for t in range(TP):
        pbuf[t] = part[80 * (t % 2):80 * (t % 2) + 80, 128 * (t // 2):128 * (t // 2) + 128]
    base_scr[...] = hid + row_of(b2_ref, pl.ds(layer, 1))
    for peer in peers:
        send(4, pbuf.at[peer], rbuf.at[me], peer).start()
    rbuf[me] = pbuf[me]
    for peer in peers:
        arrival(4, rbuf.at[peer], peer).wait_recv()
    for peer in peers:
        send(4, pbuf.at[peer], rbuf.at[me], peer).wait_send()

    def block(t):
        return pl.ds(pl.multiple_of(80 * lax.rem(t, 2), 80), 80), pl.ds(pl.multiple_of(128 * lax.div(t, 2), 128), 128)

    mine = block(me)
    total = rbuf[0].astype(F32)
    for t in range(1, TP):
        total = total + rbuf[t].astype(F32)
    hblk[...] = (base_scr[mine] + total).astype(BF16)
    for peer in peers:
        send(5, hblk, hfull.at[mine], peer).start()
    hfull[mine] = hblk[...]
    for peer in peers:
        arrival(5, hfull.at[block(peer)], peer).wait_recv()
    for peer in peers:
        send(5, hblk, hfull.at[mine], peer).wait_send()
    out_ref[...] = hfull[...]


VM = pl.BlockSpec(memory_space=pltpu.VMEM)
ANY = pl.BlockSpec(memory_space=pltpu.HBM)
SM = pl.BlockSpec(memory_space=pltpu.SMEM)


def self_call(layer, positions, hidden, w, keys, vals, prev):
    cache = jax.ShapeDtypeStruct(keys.shape, BF16)
    args = [positions, hidden, w['ln_gain'], w['ln_bias'], w['w_query'], w['b_query'], w['w_key'], w['w_value'], w['b_value'], keys, vals] + list(prev)
    specs = [SM] + [VM] * 8 + [ANY] * (2 + len(prev))
    return pl.pallas_call(
        functools.partial(self_kernel, layer),
        out_shape=(jax.ShapeDtypeStruct((BATCH // 2, 2 * HD), BF16), cache, cache),
        in_specs=specs,
        out_specs=(VM, ANY, ANY),
        input_output_aliases={11: 1, 12: 2} if prev else {},
        scratch_shapes=[
            pltpu.VMEM((BATCH, HD, CTX), BF16),
            pltpu.VMEM((BATCH, HD, CTX), BF16),
            pltpu.VMEM((BATCH, 2 * HD), F32),
            pltpu.VMEM((BATCH, D), F32),
            pltpu.VMEM((GROUPS, HD, GB), F32),
            pltpu.VMEM((GROUPS, HD, GB), F32),
            pltpu.VMEM((BATCH, HD), F32),
            pltpu.SemaphoreType.DMA((2, GROUPS)),
            pltpu.SemaphoreType.DMA((2, GROUPS)),
        ],
        compiler_params=pltpu.CompilerParams(vmem_limit_bytes=40 * 2 ** 20),
        name=f'self_attention_{layer}',
    )(*args)


def mid_call(layer, hidden, heads, w, cross_k, cross_v):
    names = ('ln_gain', 'ln_bias', 'w_out', 'b_out', 'w_cquery', 'b_cquery', 'w_cout', 'b_cout', 'w_fc1', 'b_fc1', 'w_fc2', 'b_fc2')
    args = [hidden, heads] + [w[name] for name in names] + [cross_k, cross_v]
    return pl.pallas_call(
        functools.partial(mid_kernel, layer),
        out_shape=jax.ShapeDtypeStruct((BATCH, D), BF16),
        in_specs=[VM] * (2 + len(names)) + [ANY] * 2,
        out_specs=VM,
        scratch_shapes=[
            pltpu.VMEM((AUD, HD, FRAMES), BF16),
            pltpu.VMEM((AUD, HD, FRAMES), BF16),
            pltpu.VMEM((TP, HD, D), BF16),
            pltpu.VMEM((TP, HD, D), BF16),
            pltpu.VMEM((TP, BATCH // 2, 2 * HD), BF16),
            pltpu.VMEM((TP, BATCH // 2, 2 * HD), BF16),
            pltpu.VMEM((BATCH // 2, 2 * HD), BF16),
            pltpu.VMEM((BATCH, 2 * HD), F32),
            pltpu.VMEM((BATCH, HD), F32),
            pltpu.VMEM((TP, 80, 128), BF16),
            pltpu.VMEM((TP, 80, 128), BF16),
            pltpu.VMEM((BATCH, D), F32),
            pltpu.VMEM((80, 128), BF16),
            pltpu.VMEM((BATCH, D), BF16),
            pltpu.SemaphoreType.DMA((2, AGROUPS)),
            pltpu.SemaphoreType.DMA((6, TP)),
            pltpu.SemaphoreType.DMA((6, TP)),
        ],
        compiler_params=pltpu.CompilerParams(vmem_limit_bytes=40 * 2 ** 20, collective_id=layer, has_side_effects=True),
        name=f'cross_mlp_{layer}',
    )(*args)


def solution(mesh):
    cache_spec = P(None, 'dp', None, 'tp', None)
    col_spec = P(None, None, 'tp')
    row_spec = P(None, 'tp', None)
    vec_spec = P(None, 'tp')
    param_specs = {'ln_gain': P(), 'ln_bias': P(), 'w_query': col_spec, 'b_query': vec_spec, 'w_key': col_spec, 'w_value': col_spec, 'b_value': vec_spec, 'w_out': row_spec, 'b_out': P(), 'w_cquery': col_spec, 'b_cquery': vec_spec, 'w_cout': row_spec, 'b_cout': P(), 'w_fc1': col_spec, 'b_fc1': vec_spec, 'w_fc2': row_spec, 'b_fc2': P()}
    in_specs = (P('dp', None), P('dp'), cache_spec, cache_spec, cache_spec, cache_spec) + tuple(param_specs[param_name] for param_name in PARAM_NAMES)

    def lanes_last(cache):
        return jnp.transpose(cache, (0, 1, 3, 4, 2)).reshape(cache.shape[0], cache.shape[1], cache.shape[4], cache.shape[2])

    def slots_back(cache):
        layers, beams, width, slots = cache.shape
        return jnp.transpose(cache.reshape(layers, beams, 1, width, slots), (0, 1, 4, 2, 3))

    def local_step(hidden, positions, self_keys, self_vals, cross_keys, cross_vals, *layer_params):
        w = dict(zip(PARAM_NAMES, layer_params))
        for name in ('w_query', 'w_key', 'w_value', 'w_cquery'):
            w[name] = jnp.transpose(w[name], (0, 2, 1))
        for name in ('ln_gain', 'ln_bias'):
            w[name] = jnp.transpose(w[name], (1, 0, 2))
        keys, vals, cross_k, cross_v = (lanes_last(c) for c in (self_keys, self_vals, cross_keys, cross_vals))
        prev = ()
        for layer in range(2):
            heads, *prev = self_call(layer, positions, hidden, w, keys, vals, prev)
            hidden = mid_call(layer, hidden, heads, w, cross_k, cross_v)
        return hidden, slots_back(prev[0]), slots_back(prev[1])

    return jax.shard_map(local_step, mesh=mesh, in_specs=in_specs, out_specs=(P('dp', None), cache_spec, cache_spec), check_vma=False)
```

```python
import functools

import jax
import jax.numpy as jnp
from jax import lax
from jax.experimental import pallas as pl
from jax.experimental.pallas import tpu as pltpu
from jax.sharding import PartitionSpec as P

EPS = 1e-5
F32 = jnp.float32
BF16 = jnp.bfloat16
NT = (((1,), (1,)), ((), ()))
MESH = pl.DeviceIdType.MESH
PARAM_NAMES = ('ln_gain', 'ln_bias', 'w_query', 'b_query', 'w_key', 'w_value', 'b_value', 'w_out', 'b_out', 'w_cquery', 'b_cquery', 'w_cout', 'b_cout', 'w_fc1', 'b_fc1', 'w_fc2', 'b_fc2')

BATCH = 160
AUD = 32
BEAMS = 5
HD = 64
CTX = 448
FRAMES = 1500
D = 512
TP = 8
SCALE = HD ** -0.25
GB = 8
GROUPS = BATCH // GB
VMEM_LIMIT = 67_000_000
UNROLL = 2
GA = 8
AGROUPS = AUD // GA
GR = GA * BEAMS


def layer_norm(wide, gain, bias):
    center = wide - jnp.mean(wide, axis=-1, keepdims=True)
    var_est = jnp.mean(center * center, axis=-1, keepdims=True)
    return (center * lax.rsqrt(var_est + EPS) * gain + bias).astype(BF16)


def row_of(ref, *idx):
    return ref[idx].astype(F32)


def dot_nt(a, b):
    return lax.dot_general(a, b, NT, preferred_element_type=F32)


def dot(a, b):
    return jnp.dot(a, b, preferred_element_type=F32)


def fold_heads(wide, keep):
    wide = jnp.where(keep, wide, 0.0)
    part = (wide[:, 0:128] + wide[:, 128:256]) + (wide[:, 256:384] + wide[:, 384:512])
    return part[:, :HD] + part[:, HD:]


def self_kernel(layer, pos_in, h_in, gain_in, bias_in, wq_in, bq_in, wk_in, wv_in, bv_in, kin, vin, *rest):
    if layer:
        rest = rest[2:]
    (o_out, kout, vout, o_ref, kbuf, vbuf, pos_ref, h_ref, gain_ref, bias_ref, wq_ref, bq_ref, wk_ref, wv_ref, bv_ref,
     q_scr, a_scr, kt_scr, vt_scr, o_scr, par_sem, in_sem, out_sem) = rest

    def rows(g):
        return pl.ds(pl.multiple_of(g * GB, GB), GB)

    def fetch(g, which):
        src, buf = ((kin, kbuf), (vin, vbuf))[which]
        return pltpu.make_async_copy(src.at[layer, rows(g)], buf.at[rows(g)], in_sem.at[which, g])

    def put(g, which):
        buf, dst = ((kbuf, kout), (vbuf, vout))[which]
        return pltpu.make_async_copy(buf.at[rows(g)], dst.at[layer, rows(g)], out_sem.at[which, g])

    params = [(pos_in, pos_ref), (gain_in, gain_ref), (bias_in, bias_ref), (bq_in, bq_ref), (bv_in, bv_ref),
              (wq_in.at[layer], wq_ref), (wk_in.at[layer], wk_ref), (wv_in.at[layer], wv_ref)]
    params.append((h_in, h_ref))
    copies = [pltpu.make_async_copy(src, dst, par_sem.at[i]) for i, (src, dst) in enumerate(params)]
    for copy in copies:
        copy.start()

    def start_fetch(g, carry):
        fetch(g, 0).start()
        fetch(g, 1).start()
        return carry

    lax.fori_loop(0, GROUPS, start_fetch, 0)
    for copy in copies:
        copy.wait()

    normed = layer_norm(h_ref[...].astype(F32), row_of(gain_ref, 0, pl.ds(layer, 1)), row_of(bias_ref, 0, pl.ds(layer, 1)))
    query = ((dot_nt(normed, wq_ref[...]) + row_of(bq_ref, pl.ds(layer, 1))) * SCALE).astype(BF16).astype(F32)
    q_scr[...] = jnp.concatenate([query, query], axis=1)
    a_scr[...] = normed.astype(F32)
    eye = lax.broadcasted_iota(jnp.int32, (HD, HD), 0) == lax.broadcasted_iota(jnp.int32, (HD, HD), 1)
    bv_col = jnp.sum(jnp.where(eye, row_of(bv_ref, pl.ds(layer, 1)), 0.0), axis=1, keepdims=True)

    def project(g, carry):
        part = a_scr[rows(g)].astype(BF16)
        kt_scr[g] = dot_nt(wk_ref[...], part) * SCALE
        vt_scr[g] = dot_nt(wv_ref[...], part) + bv_col
        return carry

    lax.fori_loop(0, GROUPS, project, 0, unroll=4)

    lane128 = lax.broadcasted_iota(jnp.int32, (HD, 128), 1)
    lane64 = lax.broadcasted_iota(jnp.int32, (HD, HD), 1) + 384
    lane_ctx = lax.broadcasted_iota(jnp.int32, (GB, CTX), 1)
    row_id = lax.broadcasted_iota(jnp.int32, (GB, 1), 0)
    keep = lax.broadcasted_iota(jnp.int32, (GB, D), 1) // HD == lax.broadcasted_iota(jnp.int32, (GB, D), 0)

    def attend(step, carry):
        groups = [step * UNROLL + u for u in range(UNROLL)]
        pos_cols, scores, probs = [], [], []
        for g in groups:
            fetch(g, 0).wait()
            fetch(g, 1).wait()
        for g in groups:
            pos_col = jnp.zeros((GB, 1), jnp.int32)
            for j in range(GB):
                beam = g * GB + j
                pos = pos_ref[beam]
                pos_col = jnp.where(row_id == j, pos, pos_col)
                off = pl.multiple_of(jnp.minimum(pos // 128, 2) * 128, 128)
                for buf, col_scr in ((kbuf, kt_scr), (vbuf, vt_scr)):
                    col = jnp.broadcast_to(col_scr[g][:, j:j + 1], (HD, 128)).astype(BF16)
                    view = buf.at[beam, :, pl.ds(off, 128)]
                    view[...] = jnp.where(lane128 + off == pos, col, view[...])
                    tail = buf.at[beam, :, pl.ds(384, 64)]
                    tail[...] = jnp.where(lane64 == pos, col[:, :HD], tail[...])
            pos_cols.append(pos_col)
        for g, pos_col in zip(groups, pos_cols):
            q8 = q_scr[rows(g)]
            qblk = jnp.where(keep, jnp.concatenate([q8, q8, q8, q8], axis=1), 0.0).astype(BF16)
            scores.append(jnp.where(lane_ctx <= pos_col, dot(qblk, kbuf[rows(g)].reshape(GB * HD, CTX)), -1e30))
        for score in scores:
            expd = jnp.exp(score - jnp.max(score, axis=1, keepdims=True))
            probs.append((expd / jnp.sum(expd, axis=1, keepdims=True)).astype(BF16))
        wides = [dot_nt(prob, vbuf[rows(g)].reshape(GB * HD, CTX)) for g, prob in zip(groups, probs)]
        for g, wide in zip(groups, wides):
            o_scr[rows(g)] = fold_heads(wide, keep)
            put(g, 0).start()
            put(g, 1).start()
        return carry

    lax.fori_loop(0, GROUPS // UNROLL, attend, 0)
    for half in range(2):
        o_ref[half] = jnp.concatenate([o_scr[80 * half:80 * half + 40], o_scr[80 * half + 40:80 * half + 80]], axis=1).astype(BF16)
    heads_copy = pltpu.make_async_copy(o_ref, o_out, par_sem.at[0])
    heads_copy.start()

    def finish(g, carry):
        put(g, 0).wait()
        put(g, 1).wait()
        return carry

    lax.fori_loop(0, GROUPS, finish, 0)
    heads_copy.wait()


def erf_gelu(x):
    return 0.5 * x * (1.0 + lax.erf(x * (2.0 ** -0.5)))


def mid_kernel(layer, h_in, o_in, gain_in, bias_in, wo0, wo2, wo4, wo6, bo_in, wcq_in, bcq_in, wco0, wco2, wco4, wco6, bco_in,
               w1_in, b1_in, w2_in, b2_in, kin, vin, out,
               h_ref, o_ref, gain_ref, bias_ref, bo_ref, wcq_ref, bcq_ref, bco_ref, w1_ref, b1_ref, w2_ref, b2_ref, out_ref,
               kbuf, vbuf, wofull, wcofull, obuf1, obuf2, o2_ref, q_scr, pbuf, rbuf, base_scr, hblk, hslots,
               par_sem, wpar_sem, ck_sem, wsend, wrecv, send_sem, recv_sem):
    me = lax.axis_index('tp')
    peers = [lax.rem(me + d, TP) for d in (6, 4, 2, 7, 5, 3, 1)]
    core = lax.rem(me, 2)
    chip_x = lax.rem(lax.div(me, 2), 2)
    sibling = me + 1 - 2 * core
    flip_x = 2 - 4 * chip_x
    across = lax.rem(me + 4, TP)
    holders = [me, me + flip_x, across, across + flip_x]

    def auds(g):
        return pl.ds(pl.multiple_of(g * GA, GA), GA)

    def fetch(g, which):
        src, buf = ((kin, kbuf), (vin, vbuf))[which]
        return pltpu.make_async_copy(src.at[layer, auds(g)], buf.at[auds(g)], ck_sem.at[which, g])

    params = [(o_in, o_ref), (h_in, h_ref), (gain_in, gain_ref), (bias_in, bias_ref), (bo_in, bo_ref), (wcq_in.at[layer], wcq_ref), (bcq_in, bcq_ref),
              (bco_in, bco_ref), (w1_in.at[layer], w1_ref), (b1_in, b1_ref), (w2_in.at[layer], w2_ref), (b2_in, b2_ref)]
    copies = [pltpu.make_async_copy(src, dst, par_sem.at[i]) for i, (src, dst) in enumerate(params)]
    own = [pltpu.make_async_copy(src[k].at[layer], slots.at[holders[k]], wpar_sem.at[which, k])
           for which, (src, slots) in enumerate((((wo0, wo2, wo4, wo6), wofull), ((wco0, wco2, wco4, wco6), wcofull))) for k in range(4)]

    barrier = pltpu.get_barrier_semaphore()
    for peer in peers:
        pl.semaphore_signal(barrier, inc=1, device_id={'tp': peer}, device_id_type=MESH)
    for copy in copies + own:
        copy.start()
    for g in range(AGROUPS):
        fetch(g, 0).start()
        fetch(g, 1).start()
    copies[0].wait()
    pl.semaphore_wait(barrier, TP - 1)

    def send(phase, src, dst, peer):
        return pltpu.make_async_remote_copy(src_ref=src, dst_ref=dst, send_sem=send_sem.at[phase, peer], recv_sem=recv_sem.at[phase, me],
                                            device_id={'tp': peer}, device_id_type=MESH)

    def arrival(phase, dst, peer):
        return pltpu.make_async_remote_copy(src_ref=dst, dst_ref=dst, send_sem=send_sem.at[phase, peer], recv_sem=recv_sem.at[phase, peer],
                                            device_id={'tp': peer}, device_id_type=MESH)

    def gather_start(phase, src, slots):
        for peer in peers:
            send(phase, src, slots.at[me], peer).start()

    def gather_wait(phase, src, slots):
        for peer in peers:
            arrival(phase, slots.at[peer], peer).wait_recv()
        for peer in peers:
            send(phase, src, slots.at[me], peer).wait_send()

    def weight_copy(which, k):
        src, slots = (((wo0, wo2, wo4, wo6), wofull), ((wco0, wco2, wco4, wco6), wcofull))[which]
        return pltpu.make_async_remote_copy(src_ref=src[k].at[layer], dst_ref=slots.at[holders[k]], send_sem=wsend.at[which, k],
                                            recv_sem=wrecv.at[which, k], device_id={'tp': sibling}, device_id_type=MESH)

    def weight_wait(which):
        for k in range(4):
            weight_copy(which, k).wait()

    for half in range(2):
        gather_start(half, o_ref.at[half], obuf1.at[half])
    for which in range(2):
        for k in range(4):
            weight_copy(which, k).start()
    for half in range(2):
        obuf1[half, me] = o_ref[half]
    for copy in copies[1:] + own:
        copy.wait()

    low = lax.broadcasted_iota(jnp.int32, (40, 128), 1) < HD

    def head_rows(slots, half):
        top, bottom = [], []
        for pair in range(TP // 2):
            left = slots[half, 2 * pair].astype(F32)
            right = slots[half, 2 * pair + 1].astype(F32)
            top.append(jnp.where(low, left, pltpu.roll(right, HD, 1)))
            bottom.append(jnp.where(low, pltpu.roll(left, HD, 1), right))
        return jnp.concatenate([jnp.concatenate(top, axis=1), jnp.concatenate(bottom, axis=1)], axis=0).astype(BF16)

    keep = lax.broadcasted_iota(jnp.int32, (GR, D), 1) // HD == lax.broadcasted_iota(jnp.int32, (GR, D), 0) // BEAMS
    hids = []
    for half in range(2):
        gather_wait(half, o_ref.at[half], obuf1.at[half])
        if half == 0:
            weight_wait(0)
        hid = h_ref[80 * half:80 * half + 80].astype(F32) + (dot(head_rows(obuf1, half), wofull[...].reshape(D, D)) + row_of(bo_ref, pl.ds(layer, 1)))
        hid = hid.astype(BF16).astype(F32)
        hids.append(hid)
        normed = layer_norm(hid, row_of(gain_ref, 1, pl.ds(layer, 1)), row_of(bias_ref, 1, pl.ds(layer, 1)))
        query = ((dot_nt(normed, wcq_ref[...]) + row_of(bcq_ref, pl.ds(layer, 1))) * SCALE).astype(BF16).astype(F32)
        q_scr[...] = jnp.concatenate([query, query], axis=1)
        groups = (2 * half, 2 * half + 1)
        for g in groups:
            fetch(g, 0).wait()
            fetch(g, 1).wait()
        scores, probs = [], []
        for i, g in enumerate(groups):
            q40 = q_scr[GR * i:GR * i + GR]
            qblk = jnp.where(keep, jnp.concatenate([q40, q40, q40, q40], axis=1), 0.0).astype(BF16)
            scores.append(dot(qblk, kbuf[GA * g:GA * g + GA].reshape(GA * HD, FRAMES)))
        for score in scores:
            expd = jnp.exp(score - jnp.max(score, axis=1, keepdims=True))
            probs.append((expd / jnp.sum(expd, axis=1, keepdims=True)).astype(BF16))
        outs = [fold_heads(dot_nt(prob, vbuf[GA * g:GA * g + GA].reshape(GA * HD, FRAMES)), keep) for g, prob in zip(groups, probs)]
        o2_ref[half] = jnp.concatenate(outs, axis=1).astype(BF16)
        gather_start(2 + half, o2_ref.at[half], obuf2.at[half])
        obuf2[half, me] = o2_ref[half]

    weight_wait(1)
    for half in range(2):
        gather_wait(2 + half, o2_ref.at[half], obuf2.at[half])
        hid = hids[half] + (dot(head_rows(obuf2, half), wcofull[...].reshape(D, D)) + row_of(bco_ref, pl.ds(layer, 1)))
        hid = hid.astype(BF16).astype(F32)
        normed = layer_norm(hid, row_of(gain_ref, 2, pl.ds(layer, 1)), row_of(bias_ref, 2, pl.ds(layer, 1)))
        inner = erf_gelu(dot(normed, w1_ref[...]) + row_of(b1_ref, pl.ds(layer, 1))).astype(BF16)
        part = dot(inner, w2_ref[...]).astype(BF16)
        for t in range(TP):
            pbuf[half, t] = part[40 * (t % 2):40 * (t % 2) + 40, 128 * (t // 2):128 * (t // 2) + 128]
        for peer in peers:
            send(4 + half, pbuf.at[half, peer], rbuf.at[half, me], peer).start()
        rbuf[half, me] = pbuf[half, me]
        base_scr[half] = hid + row_of(b2_ref, pl.ds(layer, 1))

    for half in range(2):
        for peer in peers:
            arrival(4 + half, rbuf.at[half, peer], peer).wait_recv()
        total = rbuf[half, 0].astype(F32)
        for t in range(1, TP):
            total = total + rbuf[half, t].astype(F32)
        mine = base_scr[half, pl.ds(pl.multiple_of(40 * core, 8), 40), pl.ds(pl.multiple_of(128 * lax.div(me, 2), 128), 128)]
        hblk[half] = (mine + total).astype(BF16)
        gather_start(6 + half, hblk.at[half], hslots.at[half])
        hslots[half, me] = hblk[half]

    for half in range(2):
        gather_wait(6 + half, hblk.at[half], hslots.at[half])
        for peer in peers:
            send(4 + half, pbuf.at[half, peer], rbuf.at[half, me], peer).wait_send()
        cols = [jnp.concatenate([hslots[half, 2 * c].astype(F32), hslots[half, 2 * c + 1].astype(F32)], axis=0) for c in range(TP // 2)]
        out_ref[80 * half:80 * half + 80] = jnp.concatenate(cols, axis=1).astype(BF16)
    final = pltpu.make_async_copy(out_ref, out, par_sem.at[0])
    final.start()
    final.wait()


HBM = pl.BlockSpec(memory_space=pltpu.HBM)


def self_call(layer, positions, hidden, w, keys, vals, prev):
    cache = jax.ShapeDtypeStruct(keys.shape, BF16)
    args = [positions, hidden, w['ln_gain'], w['ln_bias'], w['w_query'], w['b_query'], w['w_key'], w['w_value'], w['b_value'], keys, vals] + list(prev)
    return pl.pallas_call(
        functools.partial(self_kernel, layer),
        out_shape=(jax.ShapeDtypeStruct((2, BATCH // 4, 2 * HD), BF16), cache, cache),
        in_specs=[HBM] * len(args),
        out_specs=(HBM, HBM, HBM),
        input_output_aliases={11: 1, 12: 2} if prev else {},
        scratch_shapes=[
            pltpu.VMEM((2, BATCH // 4, 2 * HD), BF16),
            pltpu.VMEM((BATCH, HD, CTX), BF16),
            pltpu.VMEM((BATCH, HD, CTX), BF16),
            pltpu.SMEM((BATCH,), jnp.int32),
            pltpu.VMEM((BATCH, D), BF16),
            pltpu.VMEM((3, 2, D), BF16),
            pltpu.VMEM((3, 2, D), BF16),
            pltpu.VMEM((HD, D), BF16),
            pltpu.VMEM((2, HD), BF16),
            pltpu.VMEM((HD, D), BF16),
            pltpu.VMEM((HD, D), BF16),
            pltpu.VMEM((2, HD), BF16),
            pltpu.VMEM((BATCH, 2 * HD), F32),
            pltpu.VMEM((BATCH, D), F32),
            pltpu.VMEM((GROUPS, HD, GB), F32),
            pltpu.VMEM((GROUPS, HD, GB), F32),
            pltpu.VMEM((BATCH, HD), F32),
            pltpu.SemaphoreType.DMA((9,)),
            pltpu.SemaphoreType.DMA((2, GROUPS)),
            pltpu.SemaphoreType.DMA((2, GROUPS)),
        ],
        compiler_params=pltpu.CompilerParams(vmem_limit_bytes=VMEM_LIMIT),
        cost_estimate=pl.CostEstimate(flops=10 ** 10, bytes_accessed=42 * 2 ** 20, transcendentals=BATCH * CTX),
        name=f'self_attention_{layer}',
    )(*args)


def mid_call(layer, hidden, heads, w, wo, wco, cross_k, cross_v):
    args = [hidden, heads, w['ln_gain'], w['ln_bias'], *wo, w['b_out'], w['w_cquery'], w['b_cquery'], *wco, w['b_cout'],
            w['w_fc1'], w['b_fc1'], w['w_fc2'], w['b_fc2'], cross_k, cross_v]
    return pl.pallas_call(
        functools.partial(mid_kernel, layer),
        out_shape=jax.ShapeDtypeStruct((BATCH, D), BF16),
        in_specs=[HBM] * len(args),
        out_specs=HBM,
        scratch_shapes=[
            pltpu.VMEM((BATCH, D), BF16),
            pltpu.VMEM((2, BATCH // 4, 2 * HD), BF16),
            pltpu.VMEM((3, 2, D), BF16),
            pltpu.VMEM((3, 2, D), BF16),
            pltpu.VMEM((2, D), BF16),
            pltpu.VMEM((HD, D), BF16),
            pltpu.VMEM((2, HD), BF16),
            pltpu.VMEM((2, D), BF16),
            pltpu.VMEM((D, 256), BF16),
            pltpu.VMEM((2, 256), BF16),
            pltpu.VMEM((256, D), BF16),
            pltpu.VMEM((2, D), BF16),
            pltpu.VMEM((BATCH, D), BF16),
            pltpu.VMEM((AUD, HD, FRAMES), BF16),
            pltpu.VMEM((AUD, HD, FRAMES), BF16),
            pltpu.VMEM((TP, HD, D), BF16),
            pltpu.VMEM((TP, HD, D), BF16),
            pltpu.VMEM((2, TP, 40, 128), BF16),
            pltpu.VMEM((2, TP, 40, 128), BF16),
            pltpu.VMEM((2, 40, 128), BF16),
            pltpu.VMEM((BATCH // 2, 2 * HD), F32),
            pltpu.VMEM((2, TP, 40, 128), BF16),
            pltpu.VMEM((2, TP, 40, 128), BF16),
            pltpu.VMEM((2, BATCH // 2, D), F32),
            pltpu.VMEM((2, 40, 128), BF16),
            pltpu.VMEM((2, TP, 40, 128), BF16),
            pltpu.SemaphoreType.DMA((12,)),
            pltpu.SemaphoreType.DMA((2, 4)),
            pltpu.SemaphoreType.DMA((2, AGROUPS)),
            pltpu.SemaphoreType.DMA((2, 4)),
            pltpu.SemaphoreType.DMA((2, 4)),
            pltpu.SemaphoreType.DMA((8, TP)),
            pltpu.SemaphoreType.DMA((8, TP)),
        ],
        compiler_params=pltpu.CompilerParams(vmem_limit_bytes=VMEM_LIMIT, collective_id=layer, has_side_effects=True),
        cost_estimate=pl.CostEstimate(flops=10 ** 10, bytes_accessed=13 * 2 ** 20, transcendentals=BATCH * FRAMES),
        name=f'cross_mlp_{layer}',
    )(*args)


def solution(mesh):
    cache_spec = P(None, 'dp', None, 'tp', None)
    col_spec = P(None, None, 'tp')
    row_spec = P(None, 'tp', None)
    vec_spec = P(None, 'tp')
    param_specs = {'ln_gain': P(), 'ln_bias': P(), 'w_query': col_spec, 'b_query': vec_spec, 'w_key': col_spec, 'w_value': col_spec, 'b_value': vec_spec, 'w_out': row_spec, 'b_out': P(), 'w_cquery': col_spec, 'b_cquery': vec_spec, 'w_cout': row_spec, 'b_cout': P(), 'w_fc1': col_spec, 'b_fc1': vec_spec, 'w_fc2': row_spec, 'b_fc2': P()}
    in_specs = (P('dp', None), P('dp'), cache_spec, cache_spec, cache_spec, cache_spec) + tuple(param_specs[param_name] for param_name in PARAM_NAMES)

    def lanes_last(cache):
        return jnp.transpose(cache, (0, 1, 3, 4, 2)).reshape(cache.shape[0], cache.shape[1], cache.shape[4], cache.shape[2])

    def slots_back(cache):
        layers, beams, width, slots = cache.shape
        return jnp.transpose(cache.reshape(layers, beams, 1, width, slots), (0, 1, 4, 2, 3))

    def local_step(hidden, positions, self_keys, self_vals, cross_keys, cross_vals, *layer_params):
        w = dict(zip(PARAM_NAMES, layer_params))
        for name in ('w_query', 'w_key', 'w_value', 'w_cquery'):
            w[name] = jnp.transpose(w[name], (0, 2, 1))
        for name in ('ln_gain', 'ln_bias'):
            w[name] = jnp.transpose(w[name], (1, 0, 2))
        keys, vals, cross_k, cross_v = (lanes_last(c) for c in (self_keys, self_vals, cross_keys, cross_vals))
        wo, wco = ([w[name]] + [lax.ppermute(w[name], 'tp', [(i, i ^ flip) for i in range(TP)]) for flip in (2, 4, 6)] for name in ('w_out', 'w_cout'))
        prev = ()
        for layer in range(2):
            heads, *prev = self_call(layer, positions, hidden, w, keys, vals, prev)
            hidden = mid_call(layer, hidden, heads, w, wo, wco, cross_k, cross_v)
        return hidden, slots_back(prev[0]), slots_back(prev[1])

    return jax.shard_map(local_step, mesh=mesh, in_specs=in_specs, out_specs=(P('dp', None), cache_spec, cache_spec), check_vma=False)
```

```python
import functools

import jax
import jax.numpy as jnp
from jax import lax
from jax.experimental import pallas as pl
from jax.experimental.pallas import tpu as pltpu
from jax.sharding import PartitionSpec as P

EPS = 1e-5
F32 = jnp.float32
BF16 = jnp.bfloat16
NT = (((1,), (1,)), ((), ()))
MESH = pl.DeviceIdType.MESH
PARAM_NAMES = ('ln_gain', 'ln_bias', 'w_query', 'b_query', 'w_key', 'w_value', 'b_value', 'w_out', 'b_out', 'w_cquery', 'b_cquery', 'w_cout', 'b_cout', 'w_fc1', 'b_fc1', 'w_fc2', 'b_fc2')

BATCH = 160
AUD = 32
BEAMS = 5
HD = 64
CTX = 448
FRAMES = 1500
D = 512
TP = 8
SCALE = HD ** -0.25
GB = 8
GROUPS = BATCH // GB
VMEM_LIMIT = 67_000_000
TAIL_LIMIT = 30 * 2 ** 20
WRITE_LIMIT = 12 * 2 ** 20
SELF_UNROLL = 5
UNROLL = 4
GA = 8
AGROUPS = AUD // GA
GR = GA * BEAMS
HALF = BATCH // 2
QUART = BATCH // 4
HALVES = range(2)
LANES = 128


def layer_norm(wide, gain, bias):
    center = wide - jnp.mean(wide, axis=-1, keepdims=True)
    var_est = jnp.mean(center * center, axis=-1, keepdims=True)
    return (center * lax.rsqrt(var_est + EPS) * gain + bias).astype(BF16)


def row_of(ref, *idx):
    return ref[idx].astype(F32)


def dot_nt(a, b):
    return lax.dot_general(a, b, NT, preferred_element_type=F32)


def dot(a, b):
    return jnp.dot(a, b, preferred_element_type=F32)


def fold_heads(wide, keep):
    wide = jnp.where(keep, wide, 0.0)
    part = (wide[:, 0:LANES] + wide[:, LANES:256]) + (wide[:, 256:384] + wide[:, 384:512])
    return part[:, :HD] + part[:, HD:]


def insert_columns(g, pos_ref, pairs):
    lane128 = lax.broadcasted_iota(jnp.int32, (HD, LANES), 1)
    lane64 = lax.broadcasted_iota(jnp.int32, (HD, HD), 1) + 384
    row_id = lax.broadcasted_iota(jnp.int32, (GB, 1), 0)
    pos_col = jnp.zeros((GB, 1), jnp.int32)
    for j in range(GB):
        beam = g * GB + j
        pos = pos_ref[beam]
        pos_col = jnp.where(row_id == j, pos, pos_col)
        off = pl.multiple_of(jnp.minimum(pos // LANES, 2) * LANES, LANES)
        for buf, cols in pairs:
            col = jnp.broadcast_to(cols[:, j:j + 1], (HD, LANES)).astype(BF16)
            view = buf.at[beam, :, pl.ds(off, LANES)]
            view[...] = jnp.where(lane128 + off == pos, col, view[...])
            tail = buf.at[beam, :, pl.ds(384, 64)]
            tail[...] = jnp.where(lane64 == pos, col[:, :HD], tail[...])
    return pos_col


def self_kernel(layer, pos_in, h_in, gain_in, bias_in, wq_in, bq_in, wk_in, wv_in, bv_in, kin, vin, *rest):
    (o_out, kout, vout, o_ref, kbuf, vbuf, pos_ref, h_ref, gain_ref, bias_ref, wq_ref, bq_ref, wk_ref, wv_ref, bv_ref,
     q_scr, a_scr, kt_scr, vt_scr, o_scr, par_sem, in_sem, out_sem) = rest

    def rows(g):
        return pl.ds(pl.multiple_of(g * GB, GB), GB)

    def fetch(g, which):
        src, buf = ((kin, kbuf), (vin, vbuf))[which]
        return pltpu.make_async_copy(src.at[layer, rows(g)], buf.at[rows(g)], in_sem.at[which, g])

    def put(g, which):
        buf, dst = ((kbuf, kout), (vbuf, vout))[which]
        return pltpu.make_async_copy(buf.at[rows(g)], dst.at[layer, rows(g)], out_sem.at[which, g])

    params = [(pos_in, pos_ref), (gain_in, gain_ref), (bias_in, bias_ref), (bq_in, bq_ref), (bv_in, bv_ref),
              (wq_in.at[layer], wq_ref), (wk_in.at[layer], wk_ref), (wv_in.at[layer], wv_ref)]
    params.append((h_in, h_ref))
    copies = [pltpu.make_async_copy(src, dst, par_sem.at[i]) for i, (src, dst) in enumerate(params)]
    for copy in copies:
        copy.start()

    def start_fetch(g, carry):
        fetch(g, 0).start()
        fetch(g, 1).start()
        return carry

    lax.fori_loop(0, GROUPS, start_fetch, 0)
    for copy in copies:
        copy.wait()

    normed = layer_norm(h_ref[...].astype(F32), row_of(gain_ref, 0, pl.ds(layer, 1)), row_of(bias_ref, 0, pl.ds(layer, 1)))
    query = ((dot_nt(normed, wq_ref[...]) + row_of(bq_ref, pl.ds(layer, 1))) * SCALE).astype(BF16).astype(F32)
    q_scr[...] = jnp.concatenate([query, query], axis=1)
    a_scr[...] = normed.astype(F32)
    eye = lax.broadcasted_iota(jnp.int32, (HD, HD), 0) == lax.broadcasted_iota(jnp.int32, (HD, HD), 1)
    bv_col = jnp.sum(jnp.where(eye, row_of(bv_ref, pl.ds(layer, 1)), 0.0), axis=1, keepdims=True)

    def project(g, carry):
        part = a_scr[rows(g)].astype(BF16)
        kt_scr[g] = dot_nt(wk_ref[...], part) * SCALE
        vt_scr[g] = dot_nt(wv_ref[...], part) + bv_col
        return carry

    lax.fori_loop(0, GROUPS, project, 0, unroll=4)

    lane_ctx = lax.broadcasted_iota(jnp.int32, (GB, CTX), 1)
    keep = lax.broadcasted_iota(jnp.int32, (GB, D), 1) // HD == lax.broadcasted_iota(jnp.int32, (GB, D), 0)

    def attend(step, carry):
        groups = [step * UNROLL + u for u in range(UNROLL)]
        pos_cols, scores, probs = [], [], []
        for g in groups:
            fetch(g, 0).wait()
            fetch(g, 1).wait()
        for g in groups:
            pos_cols.append(insert_columns(g, pos_ref, ((kbuf, kt_scr[g]), (vbuf, vt_scr[g]))))
        for g, pos_col in zip(groups, pos_cols):
            q8 = q_scr[rows(g)]
            qblk = jnp.where(keep, jnp.concatenate([q8, q8, q8, q8], axis=1), 0.0).astype(BF16)
            scores.append(jnp.where(lane_ctx <= pos_col, dot(qblk, kbuf[rows(g)].reshape(GB * HD, CTX)), -1e30))
        for score in scores:
            expd = jnp.exp(score - jnp.max(score, axis=1, keepdims=True))
            probs.append((expd / jnp.sum(expd, axis=1, keepdims=True)).astype(BF16))
        wides = [dot_nt(prob, vbuf[rows(g)].reshape(GB * HD, CTX)) for g, prob in zip(groups, probs)]
        for g, wide in zip(groups, wides):
            o_scr[rows(g)] = fold_heads(wide, keep)
            put(g, 0).start()
            put(g, 1).start()
        return carry

    lax.fori_loop(0, GROUPS // UNROLL, attend, 0)
    for half in HALVES:
        o_ref[half] = jnp.concatenate([o_scr[HALF * half:HALF * half + QUART], o_scr[HALF * half + QUART:HALF * half + HALF]], axis=1).astype(BF16)
    heads_copy = pltpu.make_async_copy(o_ref, o_out, par_sem.at[0])
    heads_copy.start()

    def finish(g, carry):
        put(g, 0).wait()
        put(g, 1).wait()
        return carry

    lax.fori_loop(0, GROUPS, finish, 0)
    heads_copy.wait()


def erf_gelu(x):
    return 0.5 * x * (1.0 + lax.erf(x * (2.0 ** -0.5)))


def tail_kernel(h_in, o_in, pos_in, gain_in, bias_in, wq_in, bq_in, wk_in, wv_in, bv_in, wo0, wo2, wo4, wo6, bo_in, wcq_in, bcq_in, wco_in, bco_in,
                w1_in, b1_in, w2_in, b2_in, ckin, cvin, skin, svin,
                out_ref, knew_ref, vnew_ref, sk, sv,
                h_ref, o_ref, pos_ref, gain_ref, bias_ref, wq_ref, bq_ref, wk_ref, wv_ref, bv_ref, bo_ref, wcq_ref, bcq_ref, bco_ref,
                w1_ref, b1_ref, w2_ref, b2_ref,
                kbuf, vbuf, wofull, wcofull, obuf, osend, q_scr, kv_scr, o_scr, hid_scr, pbuf, rbuf, base_scr, hblk, hslots,
                par_sem, wpar_sem, ck_sem, sk_sem, wsend, wrecv, send_sem, recv_sem):
    me = lax.axis_index('tp')
    peers = [lax.rem(me + d, TP) for d in (6, 4, 2, 7, 5, 3, 1)]
    core = lax.rem(me, 2)
    chip_x = lax.rem(lax.div(me, 2), 2)
    sibling = me + 1 - 2 * core
    flip_x = 2 - 4 * chip_x
    across = lax.rem(me + 4, TP)
    holders = [me, me + flip_x, across, across + flip_x]

    def fetch_cross(layer, g, which):
        src, buf = ((ckin, kbuf), (cvin, vbuf))[which]
        return pltpu.make_async_copy(src.at[layer, pl.ds(GA * g, GA)], buf.at[pl.ds(GA * g, GA)], ck_sem.at[layer, which, g])

    def fetch_self(half, which):
        src, buf = ((skin, sk), (svin, sv))[which]
        return pltpu.make_async_copy(src.at[1, pl.ds(HALF * half, HALF)], buf.at[pl.ds(HALF * half, HALF)], sk_sem.at[which, half])

    params = [(o_in, o_ref), (h_in, h_ref), (gain_in, gain_ref), (bias_in, bias_ref), (bo_in, bo_ref), (wcq_in, wcq_ref), (bcq_in, bcq_ref),
              (bco_in, bco_ref), (w1_in, w1_ref), (b1_in, b1_ref), (w2_in, w2_ref), (b2_in, b2_ref), (pos_in, pos_ref), (wq_in.at[1], wq_ref),
              (bq_in, bq_ref), (wk_in.at[1], wk_ref), (wv_in.at[1], wv_ref), (bv_in, bv_ref)]
    copies = [pltpu.make_async_copy(src, dst, par_sem.at[i]) for i, (src, dst) in enumerate(params)]
    wo_src = (wo0, wo2, wo4, wo6)
    own = [pltpu.make_async_copy(wo_src[k], wofull.at[holders[k]], wpar_sem.at[k]) for k in range(4)]
    own.append(pltpu.make_async_copy(wco_in, wcofull.at[me], wpar_sem.at[4]))

    barrier = pltpu.get_barrier_semaphore()
    for peer in peers:
        pl.semaphore_signal(barrier, inc=1, device_id={'tp': peer}, device_id_type=MESH)
    for copy in copies + own:
        copy.start()
    for g in range(AGROUPS):
        fetch_cross(0, g, 0).start()
        fetch_cross(0, g, 1).start()
    for half in HALVES:
        fetch_self(half, 0).start()
        fetch_self(half, 1).start()
    copies[0].wait()
    pl.semaphore_wait(barrier, TP - 1)

    def send(phase, src, dst, peer):
        return pltpu.make_async_remote_copy(src_ref=src, dst_ref=dst, send_sem=send_sem.at[phase, peer], recv_sem=recv_sem.at[phase, me],
                                            device_id={'tp': peer}, device_id_type=MESH)

    def arrival(phase, dst, peer):
        return pltpu.make_async_remote_copy(src_ref=dst, dst_ref=dst, send_sem=send_sem.at[phase, peer], recv_sem=recv_sem.at[phase, peer],
                                            device_id={'tp': peer}, device_id_type=MESH)

    def gather_start(phase, src, slots):
        for peer in peers:
            send(phase, src, slots.at[me], peer).start()

    def gather_wait(phase, src, slots):
        for peer in peers:
            arrival(phase, slots.at[peer], peer).wait_recv()
        for peer in peers:
            send(phase, src, slots.at[me], peer).wait_send()

    def weight_copy(row, k, src, dst, target):
        return pltpu.make_async_remote_copy(src_ref=src, dst_ref=dst, send_sem=wsend.at[row, k], recv_sem=wrecv.at[row, k],
                                            device_id={'tp': target}, device_id_type=MESH)

    wo_fwd = [weight_copy(0, k, wo_src[k], wofull.at[holders[k]], sibling) for k in range(4)]
    wco_out = [weight_copy(1, k, wco_in, wcofull.at[me], holders[k]) for k in range(1, 4)]
    wco_fwd = [weight_copy(2, 0, wco_in, wcofull.at[me], sibling)] + [
        weight_copy(2, k, wcofull.at[holders[k]], wcofull.at[holders[k]], sibling) for k in range(1, 4)]

    for half in HALVES:
        gather_start(half, o_ref.at[half], obuf.at[0, half])
    for copy in wo_fwd + wco_out + wco_fwd[:1]:
        copy.start()
    for half in HALVES:
        obuf[0, half, me] = o_ref[half]
    for copy in copies[1:] + own:
        copy.wait()

    low = lax.broadcasted_iota(jnp.int32, (QUART, LANES), 1) < HD

    def head_rows(stage, half):
        top, bottom = [], []
        for pair in range(TP // 2):
            left = obuf[stage, half, 2 * pair].astype(F32)
            right = obuf[stage, half, 2 * pair + 1].astype(F32)
            top.append(jnp.where(low, left, pltpu.roll(right, HD, 1)))
            bottom.append(jnp.where(low, pltpu.roll(left, HD, 1), right))
        return jnp.concatenate([jnp.concatenate(top, axis=1), jnp.concatenate(bottom, axis=1)], axis=0).astype(BF16)

    def norm_of(hid, layer, k):
        return layer_norm(hid, row_of(gain_ref, k, pl.ds(layer, 1)), row_of(bias_ref, k, pl.ds(layer, 1)))

    keep = lax.broadcasted_iota(jnp.int32, (GR, D), 1) // HD == lax.broadcasted_iota(jnp.int32, (GR, D), 0) // BEAMS

    def gathered_out(stage, half, full, layer, bias):
        return dot(head_rows(stage, half), full[:, layer].reshape(D, D)) + row_of(bias, pl.ds(layer, 1))

    def cross_half(layer, half, hid):
        stage = 2 * layer
        hid = hid + gathered_out(stage, half, wofull, layer, bo_ref)
        hid = hid.astype(BF16).astype(F32)
        hid_scr[half] = hid
        query = ((dot_nt(norm_of(hid, layer, 1), wcq_ref[layer]) + row_of(bcq_ref, pl.ds(layer, 1))) * SCALE).astype(BF16).astype(F32)
        q_scr[...] = jnp.concatenate([query, query], axis=1)
        groups = (2 * half, 2 * half + 1)
        for g in groups:
            fetch_cross(layer, g, 0).wait()
            fetch_cross(layer, g, 1).wait()
        scores, probs = [], []
        for i, g in enumerate(groups):
            q40 = q_scr[GR * i:GR * i + GR]
            qblk = jnp.where(keep, jnp.concatenate([q40, q40, q40, q40], axis=1), 0.0).astype(BF16)
            scores.append(dot(qblk, kbuf[GA * g:GA * g + GA].reshape(GA * HD, FRAMES)))
        for score in scores:
            expd = jnp.exp(score - jnp.max(score, axis=1, keepdims=True))
            probs.append((expd / jnp.sum(expd, axis=1, keepdims=True)).astype(BF16))
        outs = [fold_heads(dot_nt(prob, vbuf[GA * g:GA * g + GA].reshape(GA * HD, FRAMES)), keep) for g, prob in zip(groups, probs)]
        osend[stage, half] = jnp.concatenate(outs, axis=1).astype(BF16)
        gather_start(8 * layer + 2 + half, osend.at[stage, half], obuf.at[stage + 1, half])
        obuf[stage + 1, half, me] = osend[stage, half]

    def mlp_half(layer, half):
        stage = 2 * layer
        gather_wait(8 * layer + 2 + half, osend.at[stage, half], obuf.at[stage + 1, half])
        hid = hid_scr[half] + gathered_out(stage + 1, half, wcofull, layer, bco_ref)
        hid = hid.astype(BF16).astype(F32)
        inner = erf_gelu(dot(norm_of(hid, layer, 2), w1_ref[layer]) + row_of(b1_ref, pl.ds(layer, 1))).astype(BF16)
        part = dot(inner, w2_ref[layer]).astype(BF16)
        for t in range(TP):
            pbuf[layer, half, t] = part[QUART * (t % 2):QUART * (t % 2) + QUART, LANES * (t // 2):LANES * (t // 2) + LANES]
        for peer in peers:
            send(8 * layer + 4 + half, pbuf.at[layer, half, peer], rbuf.at[layer, half, me], peer).start()
        rbuf[layer, half, me] = pbuf[layer, half, me]
        base_scr[half] = hid + row_of(b2_ref, pl.ds(layer, 1))

    def reduce_half(layer, half):
        for peer in peers:
            arrival(8 * layer + 4 + half, rbuf.at[layer, half, peer], peer).wait_recv()
        total = rbuf[layer, half, 0].astype(F32)
        for t in range(1, TP):
            total = total + rbuf[layer, half, t].astype(F32)
        mine = base_scr[half, pl.ds(pl.multiple_of(QUART * core, 8), QUART), pl.ds(pl.multiple_of(LANES * lax.div(me, 2), LANES), LANES)]
        hblk[layer, half] = (mine + total).astype(BF16)
        gather_start(8 * layer + 6 + half, hblk.at[layer, half], hslots.at[layer, half])
        hslots[layer, half, me] = hblk[layer, half]

    def next_hidden(layer, half):
        gather_wait(8 * layer + 6 + half, hblk.at[layer, half], hslots.at[layer, half])
        for peer in peers:
            send(8 * layer + 4 + half, pbuf.at[layer, half, peer], rbuf.at[layer, half, me], peer).wait_send()
        cols = [jnp.concatenate([hslots[layer, half, 2 * c].astype(F32), hslots[layer, half, 2 * c + 1].astype(F32)], axis=0) for c in range(TP // 2)]
        return jnp.concatenate(cols, axis=1)

    lane_ctx = lax.broadcasted_iota(jnp.int32, (GB, CTX), 1)
    row_id = lax.broadcasted_iota(jnp.int32, (GB, 1), 0)
    keep8 = lax.broadcasted_iota(jnp.int32, (GB, D), 1) // HD == lax.broadcasted_iota(jnp.int32, (GB, D), 0)

    def self_half(half, hid):
        hid_scr[half] = hid
        normed = norm_of(hid, 1, 0)
        query = ((dot_nt(normed, wq_ref[...]) + row_of(bq_ref, pl.ds(1, 1))) * SCALE).astype(BF16)
        key = (dot_nt(normed, wk_ref[...]) * SCALE).astype(BF16)
        val = (dot_nt(normed, wv_ref[...]) + row_of(bv_ref, pl.ds(1, 1))).astype(BF16)
        knew_ref[half] = key
        vnew_ref[half] = val
        query = query.astype(F32)
        q_scr[...] = jnp.concatenate([query, query], axis=1)
        kv_scr[0] = jnp.broadcast_to(jnp.sum(query * key.astype(F32), axis=1, keepdims=True), (HALF, HD))
        kv_scr[1] = val.astype(F32)
        fetch_self(half, 0).wait()
        fetch_self(half, 1).wait()

        def attend(step, carry):
            local = [step * SELF_UNROLL + u for u in range(SELF_UNROLL)]
            rows = [pl.ds(pl.multiple_of(g * GB, GB), GB) for g in local]
            slabs = [pl.ds(pl.multiple_of(HALF * half + g * GB, GB), GB) for g in local]
            scores, hits, probs, wides = [], [], [], []
            for g, row, slab in zip(local, rows, slabs):
                pos_col = jnp.zeros((GB, 1), jnp.int32)
                for j in range(GB):
                    pos_col = jnp.where(row_id == j, pos_ref[HALF * half + g * GB + j], pos_col)
                q8 = q_scr[row]
                qblk = jnp.where(keep8, jnp.concatenate([q8, q8, q8, q8], axis=1), 0.0).astype(BF16)
                score = dot(qblk, sk[slab].reshape(GB * HD, CTX))
                hit = lane_ctx == pos_col
                score = jnp.where(hit, kv_scr[0, row][:, :1], score)
                scores.append(jnp.where(lane_ctx <= pos_col, score, -1e30))
                hits.append(hit)
            for score in scores:
                expd = jnp.exp(score - jnp.max(score, axis=1, keepdims=True))
                probs.append((expd / jnp.sum(expd, axis=1, keepdims=True)).astype(BF16).astype(F32))
            for slab, prob, hit in zip(slabs, probs, hits):
                wides.append(dot_nt(jnp.where(hit, 0.0, prob).astype(BF16), sv[slab].reshape(GB * HD, CTX)))
            for row, wide, prob, hit in zip(rows, wides, probs, hits):
                fresh = jnp.sum(jnp.where(hit, prob, 0.0), axis=1, keepdims=True) * kv_scr[1, row]
                o_scr[row] = fold_heads(wide, keep8) + fresh
            return carry

        lax.fori_loop(0, 10 // SELF_UNROLL, attend, 0)
        osend[1, half] = jnp.concatenate([o_scr[0:QUART], o_scr[QUART:HALF]], axis=1).astype(BF16)
        gather_start(8 + half, osend.at[1, half], obuf.at[2, half])
        obuf[2, half, me] = osend[1, half]

    for half in HALVES:
        gather_wait(half, o_ref.at[half], obuf.at[0, half])
        if half == 0:
            for copy in wo_fwd:
                copy.wait()
        cross_half(0, half, h_ref[HALF * half:HALF * half + HALF].astype(F32))
        if half == 0:
            for k in range(1, 4):
                weight_copy(1, k, wco_in, wcofull.at[holders[k]], holders[k]).wait_recv()
            for copy in wco_fwd[1:]:
                copy.start()
    for copy in wco_out + wco_fwd:
        copy.wait_send()
    for k in range(4):
        other = holders[k] + 1 - 2 * core
        weight_copy(2, k, wco_in, wcofull.at[other], sibling).wait_recv()
    for g in range(AGROUPS):
        fetch_cross(1, g, 0).start()
        fetch_cross(1, g, 1).start()
    for half in HALVES:
        mlp_half(0, half)
    for half in HALVES:
        reduce_half(0, half)
    for half in HALVES:
        self_half(half, next_hidden(0, half))
    for half in HALVES:
        gather_wait(8 + half, osend.at[1, half], obuf.at[2, half])
        cross_half(1, half, hid_scr[half])
    for half in HALVES:
        mlp_half(1, half)
    for half in HALVES:
        reduce_half(1, half)
    for half in HALVES:
        out_ref[HALF * half:HALF * half + HALF] = next_hidden(1, half).astype(BF16)


def write_kernel(pos_in, h_ref, knew_ref, vnew_ref, sk_in, sv_in, kprev, vprev, h_out, kout, vout, sk, sv, pos_ref, new_scr, sem, out_sem):
    load = pltpu.make_async_copy(pos_in, pos_ref, sem.at[0])
    load.start()
    hidden = pltpu.make_async_copy(h_ref, h_out, sem.at[1])
    hidden.start()
    for half in HALVES:
        new_scr[0, HALF * half:HALF * half + HALF] = knew_ref[half].astype(F32)
        new_scr[1, HALF * half:HALF * half + HALF] = vnew_ref[half].astype(F32)
    eye = (lax.broadcasted_iota(jnp.int32, (HD, HD), 0) == lax.broadcasted_iota(jnp.int32, (HD, HD), 1)).astype(BF16)
    load.wait()

    def rows(g):
        return pl.ds(pl.multiple_of(g * GB, GB), GB)

    def put(g, which):
        buf, dst = ((sk, kout), (sv, vout))[which]
        return pltpu.make_async_copy(buf.at[rows(g)], dst.at[1, rows(g)], out_sem.at[which, g])

    def insert(step, carry):
        groups = [step * 2 + u for u in HALVES]
        cols = [[dot_nt(eye, new_scr[which, rows(g)].astype(BF16)) for which in HALVES] for g in groups]
        for g, pair in zip(groups, cols):
            insert_columns(g, pos_ref, ((sk, pair[0]), (sv, pair[1])))
        for g in groups:
            put(g, 0).start()
            put(g, 1).start()
        return carry

    lax.fori_loop(0, GROUPS // 2, insert, 0)

    def finish(g, carry):
        put(g, 0).wait()
        put(g, 1).wait()
        return carry

    lax.fori_loop(0, GROUPS, finish, 0)
    hidden.wait()


HBM = pl.BlockSpec(memory_space=pltpu.HBM)
VM = pl.BlockSpec(memory_space=pltpu.VMEM)


def in_hbm(*arrays):
    return [pltpu.with_memory_space_constraint(array, pltpu.HBM) for array in arrays]


def self_call(layer, positions, hidden, w, keys, vals):
    cache = jax.ShapeDtypeStruct(keys.shape, BF16)
    args = [positions, hidden, w['ln_gain'], w['ln_bias'], w['w_query'], w['b_query'], w['w_key'], w['w_value'], w['b_value'], keys, vals]
    return pl.pallas_call(
        functools.partial(self_kernel, layer),
        out_shape=(jax.ShapeDtypeStruct((2, BATCH // 4, 2 * HD), BF16), cache, cache),
        in_specs=[HBM] * len(args),
        out_specs=(HBM, HBM, HBM),
        scratch_shapes=[
            pltpu.VMEM((2, BATCH // 4, 2 * HD), BF16),
            pltpu.VMEM((BATCH, HD, CTX), BF16),
            pltpu.VMEM((BATCH, HD, CTX), BF16),
            pltpu.SMEM((BATCH,), jnp.int32),
            pltpu.VMEM((BATCH, D), BF16),
            pltpu.VMEM((3, 2, D), BF16),
            pltpu.VMEM((3, 2, D), BF16),
            pltpu.VMEM((HD, D), BF16),
            pltpu.VMEM((2, HD), BF16),
            pltpu.VMEM((HD, D), BF16),
            pltpu.VMEM((HD, D), BF16),
            pltpu.VMEM((2, HD), BF16),
            pltpu.VMEM((BATCH, 2 * HD), F32),
            pltpu.VMEM((BATCH, D), F32),
            pltpu.VMEM((GROUPS, HD, GB), F32),
            pltpu.VMEM((GROUPS, HD, GB), F32),
            pltpu.VMEM((BATCH, HD), F32),
            pltpu.SemaphoreType.DMA((9,)),
            pltpu.SemaphoreType.DMA((2, GROUPS)),
            pltpu.SemaphoreType.DMA((2, GROUPS)),
        ],
        compiler_params=pltpu.CompilerParams(vmem_limit_bytes=VMEM_LIMIT),
        cost_estimate=pl.CostEstimate(flops=10 ** 10, bytes_accessed=42 * 2 ** 20, transcendentals=BATCH * CTX),
        name=f'self_attention_{layer}',
    )(*in_hbm(*args))


def tail_call(positions, hidden, heads, w, wo, cross_k, cross_v, keys, vals):
    args = [hidden, heads, positions, w['ln_gain'], w['ln_bias'], w['w_query'], w['b_query'], w['w_key'], w['w_value'], w['b_value'], *wo, w['b_out'],
            w['w_cquery'], w['b_cquery'], w['w_cout'], w['b_cout'], w['w_fc1'], w['b_fc1'], w['w_fc2'], w['b_fc2'], cross_k, cross_v, keys, vals]
    new = jax.ShapeDtypeStruct((2, BATCH // 2, HD), BF16)
    cache = jax.ShapeDtypeStruct((BATCH, HD, CTX), BF16)
    pair = (2, TP, QUART, LANES)
    return pl.pallas_call(
        tail_kernel,
        out_shape=(jax.ShapeDtypeStruct((BATCH, D), BF16), new, new, cache, cache),
        in_specs=[HBM] * len(args),
        out_specs=(VM,) * 5,
        scratch_shapes=[
            pltpu.VMEM((BATCH, D), BF16),
            pltpu.VMEM((2, BATCH // 4, 2 * HD), BF16),
            pltpu.SMEM((BATCH,), jnp.int32),
            pltpu.VMEM((3, 2, D), BF16),
            pltpu.VMEM((3, 2, D), BF16),
            pltpu.VMEM((HD, D), BF16),
            pltpu.VMEM((2, HD), BF16),
            pltpu.VMEM((HD, D), BF16),
            pltpu.VMEM((HD, D), BF16),
            pltpu.VMEM((2, HD), BF16),
            pltpu.VMEM((2, D), BF16),
            pltpu.VMEM((2, HD, D), BF16),
            pltpu.VMEM((2, HD), BF16),
            pltpu.VMEM((2, D), BF16),
            pltpu.VMEM((2, D, 256), BF16),
            pltpu.VMEM((2, 256), BF16),
            pltpu.VMEM((2, 256, D), BF16),
            pltpu.VMEM((2, D), BF16),
            pltpu.VMEM((AUD, HD, FRAMES), BF16),
            pltpu.VMEM((AUD, HD, FRAMES), BF16),
            pltpu.VMEM((TP, 2, HD, D), BF16),
            pltpu.VMEM((TP, 2, HD, D), BF16),
            pltpu.VMEM((4,) + pair, BF16),
            pltpu.VMEM((3, 2, QUART, LANES), BF16),
            pltpu.VMEM((BATCH // 2, 2 * HD), F32),
            pltpu.VMEM((2, BATCH // 2, HD), F32),
            pltpu.VMEM((BATCH // 2, HD), F32),
            pltpu.VMEM((2, BATCH // 2, D), F32),
            pltpu.VMEM((2,) + pair, BF16),
            pltpu.VMEM((2,) + pair, BF16),
            pltpu.VMEM((2, BATCH // 2, D), F32),
            pltpu.VMEM((2, 2, QUART, LANES), BF16),
            pltpu.VMEM((2,) + pair, BF16),
            pltpu.SemaphoreType.DMA((18,)),
            pltpu.SemaphoreType.DMA((5,)),
            pltpu.SemaphoreType.DMA((2, 2, AGROUPS)),
            pltpu.SemaphoreType.DMA((2, 2)),
            pltpu.SemaphoreType.DMA((3, 4)),
            pltpu.SemaphoreType.DMA((3, 4)),
            pltpu.SemaphoreType.DMA((16, TP)),
            pltpu.SemaphoreType.DMA((16, TP)),
        ],
        compiler_params=pltpu.CompilerParams(vmem_limit_bytes=TAIL_LIMIT, collective_id=0, has_side_effects=True),
        cost_estimate=pl.CostEstimate(flops=10 ** 10, bytes_accessed=46 * 2 ** 20, transcendentals=2 * BATCH * FRAMES),
        name='cross_mlp_and_next_layer',
    )(*in_hbm(*args))


def write_call(positions, hidden, knew, vnew, sk, sv, kprev, vprev):
    held = jax.ShapeDtypeStruct(sk.shape, BF16)
    cache = jax.ShapeDtypeStruct(kprev.shape, BF16)
    return pl.pallas_call(
        write_kernel,
        out_shape=(jax.ShapeDtypeStruct(hidden.shape, BF16), cache, cache, held, held),
        in_specs=[HBM, VM, VM, VM, VM, VM, HBM, HBM],
        out_specs=(HBM, HBM, HBM, VM, VM),
        input_output_aliases={4: 3, 5: 4, 6: 1, 7: 2},
        scratch_shapes=[
            pltpu.SMEM((BATCH,), jnp.int32),
            pltpu.VMEM((2, BATCH, HD), F32),
            pltpu.SemaphoreType.DMA((2,)),
            pltpu.SemaphoreType.DMA((2, GROUPS)),
        ],
        compiler_params=pltpu.CompilerParams(vmem_limit_bytes=WRITE_LIMIT),
        cost_estimate=pl.CostEstimate(flops=10 ** 8, bytes_accessed=21 * 2 ** 20, transcendentals=0),
        name='write_caches',
    )(*in_hbm(positions), hidden, knew, vnew, sk, sv, *in_hbm(kprev, vprev))


def solution(mesh):
    cache_spec = P(None, 'dp', None, 'tp', None)
    col_spec = P(None, None, 'tp')
    row_spec = P(None, 'tp', None)
    vec_spec = P(None, 'tp')
    param_specs = {'ln_gain': P(), 'ln_bias': P(), 'w_query': col_spec, 'b_query': vec_spec, 'w_key': col_spec, 'w_value': col_spec, 'b_value': vec_spec, 'w_out': row_spec, 'b_out': P(), 'w_cquery': col_spec, 'b_cquery': vec_spec, 'w_cout': row_spec, 'b_cout': P(), 'w_fc1': col_spec, 'b_fc1': vec_spec, 'w_fc2': row_spec, 'b_fc2': P()}
    in_specs = (P('dp', None), P('dp'), cache_spec, cache_spec, cache_spec, cache_spec) + tuple(param_specs[param_name] for param_name in PARAM_NAMES)

    def lanes_last(cache):
        return jnp.transpose(cache, (0, 1, 3, 4, 2)).reshape(cache.shape[0], cache.shape[1], cache.shape[4], cache.shape[2])

    def slots_back(cache):
        layers, beams, width, slots = cache.shape
        return jnp.transpose(cache.reshape(layers, beams, 1, width, slots), (0, 1, 4, 2, 3))

    def local_step(hidden, positions, self_keys, self_vals, cross_keys, cross_vals, *layer_params):
        w = dict(zip(PARAM_NAMES, layer_params))
        for name in ('w_query', 'w_key', 'w_value', 'w_cquery'):
            w[name] = jnp.transpose(w[name], (0, 2, 1))
        for name in ('ln_gain', 'ln_bias'):
            w[name] = jnp.transpose(w[name], (1, 0, 2))
        keys, vals, cross_k, cross_v = (lanes_last(c) for c in (self_keys, self_vals, cross_keys, cross_vals))
        wo = [w['w_out']] + [lax.ppermute(w['w_out'], 'tp', [(i, i ^ flip) for i in range(TP)]) for flip in (2, 4, 6)]
        heads, *prev = self_call(0, positions, hidden, w, keys, vals)
        hidden, *held = tail_call(positions, hidden, heads, w, wo, cross_k, cross_v, keys, vals)
        hidden, *prev = write_call(positions, hidden, *held, *prev)
        return hidden, slots_back(prev[0]), slots_back(prev[1])

    return jax.shard_map(local_step, mesh=mesh, in_specs=in_specs, out_specs=(P('dp', None), cache_spec, cache_spec), check_vma=False)
```

```python
import functools

import jax
import jax.numpy as jnp
from jax import lax
from jax.experimental import pallas as pl
from jax.experimental.pallas import tpu as pltpu
from jax.sharding import PartitionSpec as P

EPS = 1e-5
F32 = jnp.float32
BF16 = jnp.bfloat16
NT = (((1,), (1,)), ((), ()))
MESH = pl.DeviceIdType.MESH
PARAM_NAMES = ('ln_gain', 'ln_bias', 'w_query', 'b_query', 'w_key', 'w_value', 'b_value', 'w_out', 'b_out', 'w_cquery', 'b_cquery', 'w_cout', 'b_cout', 'w_fc1', 'b_fc1', 'w_fc2', 'b_fc2')

BATCH = 160
AUD = 32
BEAMS = 5
HD = 64
CTX = 448
FRAMES = 1500
D = 512
TP = 8
SCALE = HD ** -0.25
GB = 8
GROUPS = BATCH // GB // 2
VMEM_LIMIT = 67_000_000
TAIL_LIMIT = 20 * 2 ** 20
WRITE_LIMIT = 12 * 2 ** 20
SELF_UNROLL = 5
UNROLL = 2
GA = 8
AGROUPS = AUD // GA
GR = GA * BEAMS
HALF = BATCH // 2
QUART = BATCH // 4
HALVES = range(2)
LANES = 128


def layer_norm(wide, gain, bias):
    center = wide - jnp.mean(wide, axis=-1, keepdims=True)
    var_est = jnp.mean(center * center, axis=-1, keepdims=True)
    return (center * lax.rsqrt(var_est + EPS) * gain + bias).astype(BF16)


def row_of(ref, *idx):
    return ref[idx].astype(F32)


def dot_nt(a, b):
    return lax.dot_general(a, b, NT, preferred_element_type=F32)


def dot(a, b):
    return jnp.dot(a, b, preferred_element_type=F32)


def fold_heads(wide, keep):
    wide = jnp.where(keep, wide, 0.0)
    part = (wide[:, 0:LANES] + wide[:, LANES:256]) + (wide[:, 256:384] + wide[:, 384:512])
    return part[:, :HD] + part[:, HD:]


def insert_columns(g, pos_ref, first, pairs):
    lane128 = lax.broadcasted_iota(jnp.int32, (HD, LANES), 1)
    lane64 = lax.broadcasted_iota(jnp.int32, (HD, HD), 1) + 384
    row_id = lax.broadcasted_iota(jnp.int32, (GB, 1), 0)
    pos_col = jnp.zeros((GB, 1), jnp.int32)
    for j in range(GB):
        beam = g * GB + j
        pos = pos_ref[first + beam]
        pos_col = jnp.where(row_id == j, pos, pos_col)
        off = pl.multiple_of(jnp.minimum(pos // LANES, 2) * LANES, LANES)
        for buf, cols in pairs:
            col = jnp.broadcast_to(cols[:, j:j + 1], (HD, LANES)).astype(BF16)
            view = buf.at[beam, :, pl.ds(off, LANES)]
            view[...] = jnp.where(lane128 + off == pos, col, view[...])
            tail = buf.at[beam, :, pl.ds(384, 64)]
            tail[...] = jnp.where(lane64 == pos, col[:, :HD], tail[...])
    return pos_col


def self_kernel(layer, pos_in, h_in, gain_in, bias_in, wq_in, bq_in, wk_in, wv_in, bv_in, kin, vin, *rest):
    (o_out, kout, vout, o_ref, kbuf, vbuf, pos_ref, h_ref, gain_ref, bias_ref, wq_ref, bq_ref, wk_ref, wv_ref, bv_ref,
     q_scr, a_scr, kt_scr, vt_scr, o_scr, par_sem, in_sem, out_sem) = rest

    def rows(g):
        return pl.ds(pl.multiple_of(g * GB, GB), GB)

    def fetch(g, which):
        src, buf = ((kin, kbuf), (vin, vbuf))[which]
        return pltpu.make_async_copy(src.at[layer, rows(g)], buf.at[rows(g)], in_sem.at[which, g])

    def put(g, which):
        buf, dst = ((kbuf, kout), (vbuf, vout))[which]
        return pltpu.make_async_copy(buf.at[rows(g)], dst.at[layer, rows(g)], out_sem.at[which, g])

    params = [(pos_in, pos_ref), (gain_in, gain_ref), (bias_in, bias_ref), (bq_in, bq_ref), (bv_in, bv_ref),
              (wq_in.at[layer], wq_ref), (wk_in.at[layer], wk_ref), (wv_in.at[layer], wv_ref)]
    params.append((h_in.at[pl.ds(0, HALF)], h_ref))
    copies = [pltpu.make_async_copy(src, dst, par_sem.at[i]) for i, (src, dst) in enumerate(params)]
    for copy in copies:
        copy.start()

    def start_fetch(g, carry):
        fetch(g, 0).start()
        fetch(g, 1).start()
        return carry

    lax.fori_loop(0, GROUPS, start_fetch, 0)
    for copy in copies:
        copy.wait()

    normed = layer_norm(h_ref[...].astype(F32), row_of(gain_ref, 0, pl.ds(layer, 1)), row_of(bias_ref, 0, pl.ds(layer, 1)))
    query = ((dot_nt(normed, wq_ref[...]) + row_of(bq_ref, pl.ds(layer, 1))) * SCALE).astype(BF16).astype(F32)
    q_scr[...] = jnp.concatenate([query, query], axis=1)
    a_scr[...] = normed.astype(F32)
    eye = lax.broadcasted_iota(jnp.int32, (HD, HD), 0) == lax.broadcasted_iota(jnp.int32, (HD, HD), 1)
    bv_col = jnp.sum(jnp.where(eye, row_of(bv_ref, pl.ds(layer, 1)), 0.0), axis=1, keepdims=True)

    def project(g, carry):
        part = a_scr[rows(g)].astype(BF16)
        kt_scr[g] = dot_nt(wk_ref[...], part) * SCALE
        vt_scr[g] = dot_nt(wv_ref[...], part) + bv_col
        return carry

    lax.fori_loop(0, GROUPS, project, 0, unroll=5)

    lane_ctx = lax.broadcasted_iota(jnp.int32, (GB, CTX), 1)
    keep = lax.broadcasted_iota(jnp.int32, (GB, D), 1) // HD == lax.broadcasted_iota(jnp.int32, (GB, D), 0)

    def attend(step, carry):
        groups = [step * UNROLL + u for u in range(UNROLL)]
        pos_cols, scores, probs = [], [], []
        for g in groups:
            fetch(g, 0).wait()
            fetch(g, 1).wait()
        for g in groups:
            pos_cols.append(insert_columns(g, pos_ref, 0, ((kbuf, kt_scr[g]), (vbuf, vt_scr[g]))))
        for g, pos_col in zip(groups, pos_cols):
            q8 = q_scr[rows(g)]
            qblk = jnp.where(keep, jnp.concatenate([q8, q8, q8, q8], axis=1), 0.0).astype(BF16)
            scores.append(jnp.where(lane_ctx <= pos_col, dot(qblk, kbuf[rows(g)].reshape(GB * HD, CTX)), -1e30))
        for score in scores:
            expd = jnp.exp(score - jnp.max(score, axis=1, keepdims=True))
            probs.append((expd / jnp.sum(expd, axis=1, keepdims=True)).astype(BF16))
        wides = [dot_nt(prob, vbuf[rows(g)].reshape(GB * HD, CTX)) for g, prob in zip(groups, probs)]
        for g, wide in zip(groups, wides):
            o_scr[rows(g)] = fold_heads(wide, keep)
            put(g, 0).start()
            put(g, 1).start()
        return carry

    lax.fori_loop(0, GROUPS // UNROLL, attend, 0)
    o_ref[...] = jnp.concatenate([o_scr[0:QUART], o_scr[QUART:HALF]], axis=1).astype(BF16)
    heads_copy = pltpu.make_async_copy(o_ref, o_out, par_sem.at[0])
    heads_copy.start()

    def finish(g, carry):
        put(g, 0).wait()
        put(g, 1).wait()
        return carry

    lax.fori_loop(0, GROUPS, finish, 0)
    heads_copy.wait()


def erf_gelu(x):
    return 0.5 * x * (1.0 + lax.erf(x * (2.0 ** -0.5)))


def tail_kernel(h_in, o_in, pos_in, gain_in, bias_in, wq_in, bq_in, wk_in, wv_in, bv_in, wo0, wo2, wo4, wo6, bo_in, wcq_in, bcq_in, wco_in, bco_in,
                w1_in, b1_in, w2_in, b2_in, ckin, cvin, skin, svin,
                out_ref, knew_ref, vnew_ref, sk0, sv0, sk, sv,
                h_ref, o_ref, pos_ref, gain_ref, bias_ref, wq_ref, bq_ref, wk_ref, wv_ref, bv_ref, bo_ref, wcq_ref, bcq_ref, bco_ref,
                w1_ref, b1_ref, w2_ref, b2_ref,
                kbuf, vbuf, wofull, wcofull, obuf, osend, csend, q_scr, kv_scr, o_scr, hid_scr, pbuf, rbuf, base_scr, hblk, hslots,
                par_sem, wpar_sem, ck_sem, sk0_sem, sk_sem, wsend, wrecv, send_sem, recv_sem):
    me = lax.axis_index('tp')
    core = lax.rem(me, 2)
    chip_x = lax.rem(lax.div(me, 2), 2)
    sibling = me + 1 - 2 * core
    flip_x = 2 - 4 * chip_x
    across = lax.rem(me + 4, TP)
    holders = [me, me + flip_x, across, across + flip_x]
    far = [holders[3], holders[1], holders[2]]
    peers = far[:1] + [p + 1 - 2 * core for p in far[:1]] + far[1:] + [p + 1 - 2 * core for p in far[1:]] + [sibling]

    def fetch_cross(layer, g, which):
        src, buf = ((ckin, kbuf), (cvin, vbuf))[which]
        return pltpu.make_async_copy(src.at[layer, pl.ds(GA * g, GA)], buf.at[pl.ds(GA * g, GA)], ck_sem.at[layer, which, g])

    def fetch_self(half, which):
        src, buf = ((skin, sk), (svin, sv))[which]
        return pltpu.make_async_copy(src.at[1, pl.ds(HALF * half, HALF)], buf.at[pl.ds(HALF * half, HALF)], sk_sem.at[which, half])

    def fetch_first(step, which):
        src, buf = ((skin, sk0), (svin, sv0))[which]
        size = GB * SELF_UNROLL
        return pltpu.make_async_copy(src.at[0, pl.ds(HALF + size * step, size)], buf.at[pl.ds(size * step, size)], sk0_sem.at[which, step])

    params = [(o_in, o_ref), (h_in, h_ref), (gain_in, gain_ref), (bias_in, bias_ref), (bo_in, bo_ref), (wcq_in, wcq_ref), (bcq_in, bcq_ref),
              (bco_in, bco_ref), (w1_in, w1_ref), (b1_in, b1_ref), (w2_in, w2_ref), (b2_in, b2_ref), (pos_in, pos_ref), (wq_in, wq_ref),
              (bq_in, bq_ref), (wk_in, wk_ref), (wv_in, wv_ref), (bv_in, bv_ref)]
    copies = [pltpu.make_async_copy(src, dst, par_sem.at[i]) for i, (src, dst) in enumerate(params)]
    wo_src = (wo0, wo2, wo4, wo6)
    own = [pltpu.make_async_copy(wo_src[k], wofull.at[holders[k]], wpar_sem.at[k]) for k in range(4)]
    own.append(pltpu.make_async_copy(wco_in, wcofull.at[me], wpar_sem.at[4]))

    barrier = pltpu.get_barrier_semaphore()
    for peer in peers:
        pl.semaphore_signal(barrier, inc=1, device_id={'tp': peer}, device_id_type=MESH)
    for copy in copies + own:
        copy.start()
    for which in (0, 1):
        for step in HALVES:
            fetch_first(step, which).start()
    for g in range(AGROUPS):
        fetch_cross(0, g, 0).start()
        fetch_cross(0, g, 1).start()
    for half in HALVES:
        fetch_self(half, 0).start()
        fetch_self(half, 1).start()
    copies[0].wait()
    pl.semaphore_wait(barrier, TP - 1)

    def send(phase, src, dst, peer):
        return pltpu.make_async_remote_copy(src_ref=src, dst_ref=dst, send_sem=send_sem.at[phase, peer], recv_sem=recv_sem.at[phase, me],
                                            device_id={'tp': peer}, device_id_type=MESH)

    def arrival(phase, dst, peer):
        return pltpu.make_async_remote_copy(src_ref=dst, dst_ref=dst, send_sem=send_sem.at[phase, peer], recv_sem=recv_sem.at[phase, peer],
                                            device_id={'tp': peer}, device_id_type=MESH)

    def gather_start(phase, src, slots):
        for peer in peers:
            send(phase, src, slots.at[me], peer).start()

    def gather_wait(phase, src, slots):
        for peer in peers:
            arrival(phase, slots.at[peer], peer).wait_recv()
        for peer in peers:
            send(phase, src, slots.at[me], peer).wait_send()

    def weight_copy(row, k, src, dst, target):
        return pltpu.make_async_remote_copy(src_ref=src, dst_ref=dst, send_sem=wsend.at[row, k], recv_sem=wrecv.at[row, k],
                                            device_id={'tp': target}, device_id_type=MESH)

    wo_fwd = [weight_copy(0, k, wo_src[k], wofull.at[holders[k]], sibling) for k in range(4)]
    wco_out = [weight_copy(1, k, wco_in, wcofull.at[me], holders[k]) for k in range(1, 4)]
    wco_fwd = [weight_copy(2, 0, wco_in, wcofull.at[me], sibling)] + [
        weight_copy(2, k, wcofull.at[holders[k]], wcofull.at[holders[k]], sibling) for k in range(1, 4)]

    gather_start(0, o_ref, obuf.at[0, 0])
    for copy in wo_fwd + wco_out + wco_fwd[:1]:
        copy.start()
    obuf[0, 0, me] = o_ref[...]
    for copy in copies[1:]:
        copy.wait()

    low = lax.broadcasted_iota(jnp.int32, (QUART, LANES), 1) < HD

    def head_rows(stage, half):
        top, bottom = [], []
        for pair in range(TP // 2):
            left = obuf[stage, half, 2 * pair].astype(F32)
            right = obuf[stage, half, 2 * pair + 1].astype(F32)
            top.append(jnp.where(low, left, pltpu.roll(right, HD, 1)))
            bottom.append(jnp.where(low, pltpu.roll(left, HD, 1), right))
        return jnp.concatenate([jnp.concatenate(top, axis=1), jnp.concatenate(bottom, axis=1)], axis=0).astype(BF16)

    def norm_of(hid, layer, k):
        return layer_norm(hid, row_of(gain_ref, k, pl.ds(layer, 1)), row_of(bias_ref, k, pl.ds(layer, 1)))

    keep = lax.broadcasted_iota(jnp.int32, (GR, D), 1) // HD == lax.broadcasted_iota(jnp.int32, (GR, D), 0) // BEAMS

    def gathered_out(stage, half, full, layer, bias):
        return dot(head_rows(stage, half), full[:, layer].reshape(D, D)) + row_of(bias, pl.ds(layer, 1))

    def cross_half(layer, half, hid):
        stage = 2 * layer
        hid = hid + gathered_out(stage, half, wofull, layer, bo_ref)
        hid = hid.astype(BF16).astype(F32)
        hid_scr[half] = hid
        query = ((dot_nt(norm_of(hid, layer, 1), wcq_ref[layer]) + row_of(bcq_ref, pl.ds(layer, 1))) * SCALE).astype(BF16).astype(F32)
        q_scr[...] = jnp.concatenate([query, query], axis=1)
        groups = (2 * half, 2 * half + 1)
        for g in groups:
            fetch_cross(layer, g, 0).wait()
            fetch_cross(layer, g, 1).wait()
        scores, probs = [], []
        for i, g in enumerate(groups):
            q40 = q_scr[GR * i:GR * i + GR]
            qblk = jnp.where(keep, jnp.concatenate([q40, q40, q40, q40], axis=1), 0.0).astype(BF16)
            scores.append(dot(qblk, kbuf[GA * g:GA * g + GA].reshape(GA * HD, FRAMES)))
        for score in scores:
            expd = jnp.exp(score - jnp.max(score, axis=1, keepdims=True))
            probs.append((expd / jnp.sum(expd, axis=1, keepdims=True)).astype(BF16))
        outs = [fold_heads(dot_nt(prob, vbuf[GA * g:GA * g + GA].reshape(GA * HD, FRAMES)), keep) for g, prob in zip(groups, probs)]
        csend[layer, half] = jnp.concatenate(outs, axis=1).astype(BF16)
        gather_start(8 * layer + 2 + half, csend.at[layer, half], obuf.at[stage + 1, half])
        obuf[stage + 1, half, me] = csend[layer, half]

    def mlp_half(layer, half):
        stage = 2 * layer
        gather_wait(8 * layer + 2 + half, csend.at[layer, half], obuf.at[stage + 1, half])
        hid = hid_scr[half] + gathered_out(stage + 1, half, wcofull, layer, bco_ref)
        hid = hid.astype(BF16).astype(F32)
        inner = erf_gelu(dot(norm_of(hid, layer, 2), w1_ref[layer]) + row_of(b1_ref, pl.ds(layer, 1))).astype(BF16)
        part = dot(inner, w2_ref[layer]).astype(BF16)
        for t in range(TP):
            pbuf[layer, half, t] = part[QUART * (t % 2):QUART * (t % 2) + QUART, LANES * (t // 2):LANES * (t // 2) + LANES]
        for peer in peers:
            send(8 * layer + 4 + half, pbuf.at[layer, half, peer], rbuf.at[layer, half, me], peer).start()
        rbuf[layer, half, me] = pbuf[layer, half, me]
        base_scr[half] = hid + row_of(b2_ref, pl.ds(layer, 1))

    def reduce_half(layer, half):
        for peer in peers:
            arrival(8 * layer + 4 + half, rbuf.at[layer, half, peer], peer).wait_recv()
        total = rbuf[layer, half, 0].astype(F32)
        for t in range(1, TP):
            total = total + rbuf[layer, half, t].astype(F32)
        mine = base_scr[half, pl.ds(pl.multiple_of(QUART * core, 8), QUART), pl.ds(pl.multiple_of(LANES * lax.div(me, 2), LANES), LANES)]
        hblk[layer, half] = (mine + total).astype(BF16)
        gather_start(8 * layer + 6 + half, hblk.at[layer, half], hslots.at[layer, half])
        hslots[layer, half, me] = hblk[layer, half]

    def next_hidden(layer, half):
        gather_wait(8 * layer + 6 + half, hblk.at[layer, half], hslots.at[layer, half])
        for peer in peers:
            send(8 * layer + 4 + half, pbuf.at[layer, half, peer], rbuf.at[layer, half, me], peer).wait_send()
        cols = [jnp.concatenate([hslots[layer, half, 2 * c].astype(F32), hslots[layer, half, 2 * c + 1].astype(F32)], axis=0) for c in range(TP // 2)]
        return jnp.concatenate(cols, axis=1)

    lane_ctx = lax.broadcasted_iota(jnp.int32, (GB, CTX), 1)
    row_id = lax.broadcasted_iota(jnp.int32, (GB, 1), 0)
    keep8 = lax.broadcasted_iota(jnp.int32, (GB, D), 1) // HD == lax.broadcasted_iota(jnp.int32, (GB, D), 0)

    def self_half(layer, half, hid, keys, vals, base, slot):
        normed = norm_of(hid, layer, 0)
        query = ((dot_nt(normed, wq_ref[layer]) + row_of(bq_ref, pl.ds(layer, 1))) * SCALE).astype(BF16)
        key = (dot_nt(normed, wk_ref[layer]) * SCALE).astype(BF16)
        val = (dot_nt(normed, wv_ref[layer]) + row_of(bv_ref, pl.ds(layer, 1))).astype(BF16)
        knew_ref[slot] = key
        vnew_ref[slot] = val
        query = query.astype(F32)
        q_scr[...] = jnp.concatenate([query, query], axis=1)
        kv_scr[0] = jnp.broadcast_to(jnp.sum(query * key.astype(F32), axis=1, keepdims=True), (HALF, HD))
        kv_scr[1] = val.astype(F32)

        def attend(step, carry):
            if layer == 0:
                fetch_first(step, 0).wait()
                fetch_first(step, 1).wait()
            local = [step * SELF_UNROLL + u for u in range(SELF_UNROLL)]
            rows = [pl.ds(pl.multiple_of(g * GB, GB), GB) for g in local]
            slabs = [pl.ds(pl.multiple_of(base + g * GB, GB), GB) for g in local]
            scores, hits, probs, wides = [], [], [], []
            for g, row, slab in zip(local, rows, slabs):
                pos_col = jnp.zeros((GB, 1), jnp.int32)
                for j in range(GB):
                    pos_col = jnp.where(row_id == j, pos_ref[HALF * half + g * GB + j], pos_col)
                q8 = q_scr[row]
                qblk = jnp.where(keep8, jnp.concatenate([q8, q8, q8, q8], axis=1), 0.0).astype(BF16)
                score = dot(qblk, keys[slab].reshape(GB * HD, CTX))
                hit = lane_ctx == pos_col
                score = jnp.where(hit, kv_scr[0, row][:, :1], score)
                scores.append(jnp.where(lane_ctx <= pos_col, score, -1e30))
                hits.append(hit)
            for score in scores:
                expd = jnp.exp(score - jnp.max(score, axis=1, keepdims=True))
                probs.append((expd / jnp.sum(expd, axis=1, keepdims=True)).astype(BF16).astype(F32))
            for slab, prob, hit in zip(slabs, probs, hits):
                wides.append(dot_nt(jnp.where(hit, 0.0, prob).astype(BF16), vals[slab].reshape(GB * HD, CTX)))
            for row, wide, prob, hit in zip(rows, wides, probs, hits):
                fresh = jnp.sum(jnp.where(hit, prob, 0.0), axis=1, keepdims=True) * kv_scr[1, row]
                o_scr[row] = fold_heads(wide, keep8) + fresh
            return carry

        lax.fori_loop(0, GROUPS // SELF_UNROLL, attend, 0)
        osend[slot] = jnp.concatenate([o_scr[0:QUART], o_scr[QUART:HALF]], axis=1).astype(BF16)
        gather_start(8 * layer + half, osend.at[slot], obuf.at[2 * layer, half])
        obuf[2 * layer, half, me] = osend[slot]

    self_half(0, 1, h_ref[HALF:].astype(F32), sk0, sv0, 0, 0)
    for copy in own + wo_fwd:
        copy.wait()
    for half in HALVES:
        gather_wait(half, osend.at[0] if half else o_ref, obuf.at[0, half])
        cross_half(0, half, h_ref[HALF * half:HALF * half + HALF].astype(F32))
        if half == 0:
            for k in range(1, 4):
                weight_copy(1, k, wco_in, wcofull.at[holders[k]], holders[k]).wait_recv()
            for copy in wco_fwd[1:]:
                copy.start()
    for copy in wco_out + wco_fwd:
        copy.wait_send()
    for k in range(4):
        other = holders[k] + 1 - 2 * core
        weight_copy(2, k, wco_in, wcofull.at[other], sibling).wait_recv()
    for g in range(AGROUPS):
        fetch_cross(1, g, 0).start()
        fetch_cross(1, g, 1).start()
    for half in HALVES:
        mlp_half(0, half)
    for half in HALVES:
        reduce_half(0, half)
    for half in HALVES:
        hid_scr[half] = next_hidden(0, half)
        fetch_self(half, 0).wait()
        fetch_self(half, 1).wait()
        self_half(1, half, hid_scr[half], sk, sv, HALF * half, 1 + half)
    for half in HALVES:
        gather_wait(8 + half, osend.at[1 + half], obuf.at[2, half])
        cross_half(1, half, hid_scr[half])
    for half in HALVES:
        mlp_half(1, half)
    for half in HALVES:
        reduce_half(1, half)
    for half in HALVES:
        out_ref[HALF * half:HALF * half + HALF] = next_hidden(1, half).astype(BF16)


def write_kernel(pos_in, h_ref, knew_ref, vnew_ref, sk0_in, sv0_in, sk_in, sv_in, kprev, vprev, h_out, kout, vout, sk0, sv0, sk, sv,
                 pos_ref, new_scr, sem, out_sem):
    load = pltpu.make_async_copy(pos_in, pos_ref, sem.at[0])
    load.start()
    hidden = pltpu.make_async_copy(h_ref, h_out, sem.at[1])
    hidden.start()
    for part in range(3):
        new_scr[0, HALF * part:HALF * part + HALF] = knew_ref[part].astype(F32)
        new_scr[1, HALF * part:HALF * part + HALF] = vnew_ref[part].astype(F32)
    eye = (lax.broadcasted_iota(jnp.int32, (HD, HD), 0) == lax.broadcasted_iota(jnp.int32, (HD, HD), 1)).astype(BF16)
    load.wait()

    def rows(g, first=0):
        return pl.ds(pl.multiple_of(first + g * GB, GB), GB)

    pieces = (((sk0, sv0), 0, HALF, 0, GROUPS), ((sk, sv), 1, 0, HALF, 2 * GROUPS))

    def put(piece, g, which):
        bufs, layer, first = pieces[piece][:3]
        return pltpu.make_async_copy(bufs[which].at[rows(g)], (kout, vout)[which].at[layer, rows(g, first)], out_sem.at[piece, which, g])

    for piece, (bufs, layer, first, new_first, count) in enumerate(pieces):
        def insert(step, carry):
            groups = [step * 2 + u for u in range(2)]
            cols = [[dot_nt(eye, new_scr[which, rows(g, new_first)].astype(BF16)) for which in range(2)] for g in groups]
            for g, pair in zip(groups, cols):
                insert_columns(g, pos_ref, first, tuple(zip(bufs, pair)))
            for g in groups:
                put(piece, g, 0).start()
                put(piece, g, 1).start()
            return carry

        lax.fori_loop(0, count // 2, insert, 0)

    for piece in range(2):
        def finish(g, carry):
            put(piece, g, 0).wait()
            put(piece, g, 1).wait()
            return carry

        lax.fori_loop(0, pieces[piece][4], finish, 0)
    hidden.wait()


HBM = pl.BlockSpec(memory_space=pltpu.HBM)
VM = pl.BlockSpec(memory_space=pltpu.VMEM)


def in_hbm(*arrays):
    return [pltpu.with_memory_space_constraint(array, pltpu.HBM) for array in arrays]


def self_call(layer, positions, hidden, w, keys, vals):
    cache = jax.ShapeDtypeStruct(keys.shape, BF16)
    args = [positions, hidden, w['ln_gain'], w['ln_bias'], w['w_query'], w['b_query'], w['w_key'], w['w_value'], w['b_value'], keys, vals]
    return pl.pallas_call(
        functools.partial(self_kernel, layer),
        out_shape=(jax.ShapeDtypeStruct((QUART, LANES), BF16), cache, cache),
        in_specs=[HBM] * len(args),
        out_specs=(HBM, HBM, HBM),
        scratch_shapes=[
            pltpu.VMEM((QUART, LANES), BF16),
            pltpu.VMEM((HALF, HD, CTX), BF16),
            pltpu.VMEM((HALF, HD, CTX), BF16),
            pltpu.SMEM((BATCH,), jnp.int32),
            pltpu.VMEM((HALF, D), BF16),
            pltpu.VMEM((3, 2, D), BF16),
            pltpu.VMEM((3, 2, D), BF16),
            pltpu.VMEM((HD, D), BF16),
            pltpu.VMEM((2, HD), BF16),
            pltpu.VMEM((HD, D), BF16),
            pltpu.VMEM((HD, D), BF16),
            pltpu.VMEM((2, HD), BF16),
            pltpu.VMEM((HALF, 2 * HD), F32),
            pltpu.VMEM((HALF, D), F32),
            pltpu.VMEM((GROUPS, HD, GB), F32),
            pltpu.VMEM((GROUPS, HD, GB), F32),
            pltpu.VMEM((HALF, HD), F32),
            pltpu.SemaphoreType.DMA((9,)),
            pltpu.SemaphoreType.DMA((2, GROUPS)),
            pltpu.SemaphoreType.DMA((2, GROUPS)),
        ],
        compiler_params=pltpu.CompilerParams(vmem_limit_bytes=VMEM_LIMIT),
        cost_estimate=pl.CostEstimate(flops=10 ** 10, bytes_accessed=21 * 2 ** 20, transcendentals=HALF * CTX),
        name=f'self_attention_{layer}',
    )(*in_hbm(*args))


def tail_call(positions, hidden, heads, w, wo, cross_k, cross_v, keys, vals):
    args = [hidden, heads, positions, w['ln_gain'], w['ln_bias'], w['w_query'], w['b_query'], w['w_key'], w['w_value'], w['b_value'], *wo, w['b_out'],
            w['w_cquery'], w['b_cquery'], w['w_cout'], w['b_cout'], w['w_fc1'], w['b_fc1'], w['w_fc2'], w['b_fc2'], cross_k, cross_v, keys, vals]
    new = jax.ShapeDtypeStruct((3, HALF, HD), BF16)
    half = jax.ShapeDtypeStruct((HALF, HD, CTX), BF16)
    cache = jax.ShapeDtypeStruct((BATCH, HD, CTX), BF16)
    pair = (2, TP, QUART, LANES)
    return pl.pallas_call(
        tail_kernel,
        out_shape=(jax.ShapeDtypeStruct((BATCH, D), BF16), new, new, half, half, cache, cache),
        in_specs=[HBM] * len(args),
        out_specs=(VM,) * 7,
        scratch_shapes=[
            pltpu.VMEM((BATCH, D), BF16),
            pltpu.VMEM((QUART, LANES), BF16),
            pltpu.SMEM((BATCH,), jnp.int32),
            pltpu.VMEM((3, 2, D), BF16),
            pltpu.VMEM((3, 2, D), BF16),
            pltpu.VMEM((2, HD, D), BF16),
            pltpu.VMEM((2, HD), BF16),
            pltpu.VMEM((2, HD, D), BF16),
            pltpu.VMEM((2, HD, D), BF16),
            pltpu.VMEM((2, HD), BF16),
            pltpu.VMEM((2, D), BF16),
            pltpu.VMEM((2, HD, D), BF16),
            pltpu.VMEM((2, HD), BF16),
            pltpu.VMEM((2, D), BF16),
            pltpu.VMEM((2, D, 256), BF16),
            pltpu.VMEM((2, 256), BF16),
            pltpu.VMEM((2, 256, D), BF16),
            pltpu.VMEM((2, D), BF16),
            pltpu.VMEM((AUD, HD, FRAMES), BF16),
            pltpu.VMEM((AUD, HD, FRAMES), BF16),
            pltpu.VMEM((TP, 2, HD, D), BF16),
            pltpu.VMEM((TP, 2, HD, D), BF16),
            pltpu.VMEM((4,) + pair, BF16),
            pltpu.VMEM((3, QUART, LANES), BF16),
            pltpu.VMEM((2, 2, QUART, LANES), BF16),
            pltpu.VMEM((BATCH // 2, 2 * HD), F32),
            pltpu.VMEM((2, BATCH // 2, HD), F32),
            pltpu.VMEM((BATCH // 2, HD), F32),
            pltpu.VMEM((2, BATCH // 2, D), F32),
            pltpu.VMEM((2,) + pair, BF16),
            pltpu.VMEM((2,) + pair, BF16),
            pltpu.VMEM((2, BATCH // 2, D), F32),
            pltpu.VMEM((2, 2, QUART, LANES), BF16),
            pltpu.VMEM((2,) + pair, BF16),
            pltpu.SemaphoreType.DMA((18,)),
            pltpu.SemaphoreType.DMA((5,)),
            pltpu.SemaphoreType.DMA((2, 2, AGROUPS)),
            pltpu.SemaphoreType.DMA((2, 2)),
            pltpu.SemaphoreType.DMA((2, 2)),
            pltpu.SemaphoreType.DMA((3, 4)),
            pltpu.SemaphoreType.DMA((3, 4)),
            pltpu.SemaphoreType.DMA((16, TP)),
            pltpu.SemaphoreType.DMA((16, TP)),
        ],
        compiler_params=pltpu.CompilerParams(vmem_limit_bytes=TAIL_LIMIT, collective_id=0, has_side_effects=True),
        cost_estimate=pl.CostEstimate(flops=10 ** 10, bytes_accessed=46 * 2 ** 20, transcendentals=2 * BATCH * FRAMES),
        name='cross_mlp_and_next_layer',
    )(*in_hbm(*args))


def write_call(positions, hidden, knew, vnew, held, prev):
    shapes = [jax.ShapeDtypeStruct(x.shape, BF16) for x in (hidden, *prev, *held)]
    return pl.pallas_call(
        write_kernel,
        out_shape=tuple(shapes),
        in_specs=[HBM] + [VM] * 7 + [HBM, HBM],
        out_specs=(HBM, HBM, HBM, VM, VM, VM, VM),
        input_output_aliases={4: 3, 5: 4, 6: 5, 7: 6, 8: 1, 9: 2},
        scratch_shapes=[
            pltpu.SMEM((BATCH,), jnp.int32),
            pltpu.VMEM((2, 3 * HALF, HD), F32),
            pltpu.SemaphoreType.DMA((2,)),
            pltpu.SemaphoreType.DMA((2, 2, 2 * GROUPS)),
        ],
        compiler_params=pltpu.CompilerParams(vmem_limit_bytes=WRITE_LIMIT),
        cost_estimate=pl.CostEstimate(flops=10 ** 8, bytes_accessed=32 * 2 ** 20, transcendentals=0),
        name='write_caches',
    )(*in_hbm(positions), hidden, knew, vnew, *held, *in_hbm(*prev))


def solution(mesh):
    cache_spec = P(None, 'dp', None, 'tp', None)
    col_spec = P(None, None, 'tp')
    row_spec = P(None, 'tp', None)
    vec_spec = P(None, 'tp')
    param_specs = {'ln_gain': P(), 'ln_bias': P(), 'w_query': col_spec, 'b_query': vec_spec, 'w_key': col_spec, 'w_value': col_spec, 'b_value': vec_spec, 'w_out': row_spec, 'b_out': P(), 'w_cquery': col_spec, 'b_cquery': vec_spec, 'w_cout': row_spec, 'b_cout': P(), 'w_fc1': col_spec, 'b_fc1': vec_spec, 'w_fc2': row_spec, 'b_fc2': P()}
    in_specs = (P('dp', None), P('dp'), cache_spec, cache_spec, cache_spec, cache_spec) + tuple(param_specs[param_name] for param_name in PARAM_NAMES)

    def lanes_last(cache):
        return jnp.transpose(cache, (0, 1, 3, 4, 2)).reshape(cache.shape[0], cache.shape[1], cache.shape[4], cache.shape[2])

    def slots_back(cache):
        layers, beams, width, slots = cache.shape
        return jnp.transpose(cache.reshape(layers, beams, 1, width, slots), (0, 1, 4, 2, 3))

    def local_step(hidden, positions, self_keys, self_vals, cross_keys, cross_vals, *layer_params):
        w = dict(zip(PARAM_NAMES, layer_params))
        for name in ('w_query', 'w_key', 'w_value', 'w_cquery'):
            w[name] = jnp.transpose(w[name], (0, 2, 1))
        for name in ('ln_gain', 'ln_bias'):
            w[name] = jnp.transpose(w[name], (1, 0, 2))
        keys, vals, cross_k, cross_v = (lanes_last(c) for c in (self_keys, self_vals, cross_keys, cross_vals))
        wo = [w['w_out']] + [lax.ppermute(w['w_out'], 'tp', [(i, i ^ flip) for i in range(TP)]) for flip in (2, 4, 6)]
        heads, *prev = self_call(0, positions, hidden, w, keys, vals)
        hidden, knew, vnew, *held = tail_call(positions, hidden, heads, w, wo, cross_k, cross_v, keys, vals)
        hidden, new_keys, new_vals = write_call(positions, hidden, knew, vnew, held, prev)[:3]
        return hidden, slots_back(new_keys), slots_back(new_vals)

    return jax.shard_map(local_step, mesh=mesh, in_specs=in_specs, out_specs=(P('dp', None), cache_spec, cache_spec), check_vma=False)
```

```python
import functools

import jax
import jax.numpy as jnp
from jax import lax
from jax.experimental import pallas as pl
from jax.experimental.pallas import tpu as pltpu
from jax.sharding import PartitionSpec as P

EPS = 1e-5
F32 = jnp.float32
BF16 = jnp.bfloat16
NT = (((1,), (1,)), ((), ()))
MESH = pl.DeviceIdType.MESH
PARAM_NAMES = ('ln_gain', 'ln_bias', 'w_query', 'b_query', 'w_key', 'w_value', 'b_value', 'w_out', 'b_out', 'w_cquery', 'b_cquery', 'w_cout', 'b_cout', 'w_fc1', 'b_fc1', 'w_fc2', 'b_fc2')

BATCH = 160
AUD = 32
BEAMS = 5
HD = 64
CTX = 448
FRAMES = 1500
D = 512
TP = 8
SCALE = HD ** -0.25
GB = 8
GROUPS = BATCH // GB // 2
VMEM_LIMIT = 67_000_000
TAIL_LIMIT = 20 * 2 ** 20
WRITE_LIMIT = 12 * 2 ** 20
SELF_UNROLL = 5
UNROLL = 2
GA = 8
AGROUPS = AUD // GA
GR = GA * BEAMS
HALF = BATCH // 2
QUART = BATCH // 4
HALVES = range(2)
LANES = 128


def layer_norm(wide, gain, bias):
    center = wide - jnp.mean(wide, axis=-1, keepdims=True)
    var_est = jnp.mean(center * center, axis=-1, keepdims=True)
    return (center * lax.rsqrt(var_est + EPS) * gain + bias).astype(BF16)


def row_of(ref, *idx):
    return ref[idx].astype(F32)


def dot_nt(a, b):
    return lax.dot_general(a, b, NT, preferred_element_type=F32)


def dot(a, b):
    return jnp.dot(a, b, preferred_element_type=F32)


def fold_heads(wide, keep):
    wide = jnp.where(keep, wide, 0.0)
    part = (wide[:, 0:LANES] + wide[:, LANES:256]) + (wide[:, 256:384] + wide[:, 384:512])
    return part[:, :HD] + part[:, HD:]


def insert_columns(g, pos_ref, first, pairs):
    lane128 = lax.broadcasted_iota(jnp.int32, (HD, LANES), 1)
    lane64 = lax.broadcasted_iota(jnp.int32, (HD, HD), 1) + 384
    row_id = lax.broadcasted_iota(jnp.int32, (GB, 1), 0)
    pos_col = jnp.zeros((GB, 1), jnp.int32)
    for j in range(GB):
        beam = g * GB + j
        pos = pos_ref[first + beam]
        pos_col = jnp.where(row_id == j, pos, pos_col)
        off = pl.multiple_of(jnp.minimum(pos // LANES, 2) * LANES, LANES)
        for buf, cols in pairs:
            col = jnp.broadcast_to(cols[:, j:j + 1], (HD, LANES)).astype(BF16)
            view = buf.at[beam, :, pl.ds(off, LANES)]
            view[...] = jnp.where(lane128 + off == pos, col, view[...])
            tail = buf.at[beam, :, pl.ds(384, 64)]
            tail[...] = jnp.where(lane64 == pos, col[:, :HD], tail[...])
    return pos_col


def self_kernel(layer, pos_in, h_in, gain_in, bias_in, wq_in, bq_in, wk_in, wv_in, bv_in, kin, vin, *rest):
    (o_out, kout, vout, o_ref, kbuf, vbuf, pos_ref, h_ref, gain_ref, bias_ref, wq_ref, bq_ref, wk_ref, wv_ref, bv_ref,
     q_scr, a_scr, kt_scr, vt_scr, o_scr, par_sem, in_sem, out_sem) = rest

    def rows(g):
        return pl.ds(pl.multiple_of(g * GB, GB), GB)

    def fetch(g, which):
        src, buf = ((kin, kbuf), (vin, vbuf))[which]
        return pltpu.make_async_copy(src.at[layer, rows(g)], buf.at[rows(g)], in_sem.at[which, g])

    def put(g, which):
        buf, dst = ((kbuf, kout), (vbuf, vout))[which]
        return pltpu.make_async_copy(buf.at[rows(g)], dst.at[layer, rows(g)], out_sem.at[which, g])

    params = [(pos_in, pos_ref), (gain_in, gain_ref), (bias_in, bias_ref), (bq_in, bq_ref), (bv_in, bv_ref),
              (wq_in.at[layer], wq_ref), (wk_in.at[layer], wk_ref), (wv_in.at[layer], wv_ref)]
    params.append((h_in.at[pl.ds(0, HALF)], h_ref))
    copies = [pltpu.make_async_copy(src, dst, par_sem.at[i]) for i, (src, dst) in enumerate(params)]
    for copy in copies:
        copy.start()

    def start_fetch(g, carry):
        fetch(g, 0).start()
        fetch(g, 1).start()
        return carry

    lax.fori_loop(0, GROUPS, start_fetch, 0)
    for copy in copies:
        copy.wait()

    normed = layer_norm(h_ref[...].astype(F32), row_of(gain_ref, 0, pl.ds(layer, 1)), row_of(bias_ref, 0, pl.ds(layer, 1)))
    query = ((dot_nt(normed, wq_ref[...]) + row_of(bq_ref, pl.ds(layer, 1))) * SCALE).astype(BF16).astype(F32)
    q_scr[...] = jnp.concatenate([query, query], axis=1)
    a_scr[...] = normed.astype(F32)
    eye = lax.broadcasted_iota(jnp.int32, (HD, HD), 0) == lax.broadcasted_iota(jnp.int32, (HD, HD), 1)
    bv_col = jnp.sum(jnp.where(eye, row_of(bv_ref, pl.ds(layer, 1)), 0.0), axis=1, keepdims=True)

    def project(g, carry):
        part = a_scr[rows(g)].astype(BF16)
        kt_scr[g] = dot_nt(wk_ref[...], part) * SCALE
        vt_scr[g] = dot_nt(wv_ref[...], part) + bv_col
        return carry

    lax.fori_loop(0, GROUPS, project, 0, unroll=5)

    lane_ctx = lax.broadcasted_iota(jnp.int32, (GB, CTX), 1)
    keep = lax.broadcasted_iota(jnp.int32, (GB, D), 1) // HD == lax.broadcasted_iota(jnp.int32, (GB, D), 0)

    def attend(step, carry):
        groups = [step * UNROLL + u for u in range(UNROLL)]
        pos_cols, scores, probs = [], [], []
        for g in groups:
            fetch(g, 0).wait()
            fetch(g, 1).wait()
        for g in groups:
            pos_cols.append(insert_columns(g, pos_ref, 0, ((kbuf, kt_scr[g]), (vbuf, vt_scr[g]))))
        for g, pos_col in zip(groups, pos_cols):
            q8 = q_scr[rows(g)]
            qblk = jnp.where(keep, jnp.concatenate([q8, q8, q8, q8], axis=1), 0.0).astype(BF16)
            scores.append(jnp.where(lane_ctx <= pos_col, dot(qblk, kbuf[rows(g)].reshape(GB * HD, CTX)), -1e30))
        for score in scores:
            expd = jnp.exp(score - jnp.max(score, axis=1, keepdims=True))
            probs.append((expd / jnp.sum(expd, axis=1, keepdims=True)).astype(BF16))
        wides = [dot_nt(prob, vbuf[rows(g)].reshape(GB * HD, CTX)) for g, prob in zip(groups, probs)]
        for g, wide in zip(groups, wides):
            o_scr[rows(g)] = fold_heads(wide, keep)
            put(g, 0).start()
            put(g, 1).start()
        return carry

    lax.fori_loop(0, GROUPS // UNROLL, attend, 0)
    o_ref[...] = jnp.concatenate([o_scr[0:QUART], o_scr[QUART:HALF]], axis=1).astype(BF16)
    heads_copy = pltpu.make_async_copy(o_ref, o_out, par_sem.at[0])
    heads_copy.start()

    def finish(g, carry):
        put(g, 0).wait()
        put(g, 1).wait()
        return carry

    lax.fori_loop(0, GROUPS, finish, 0)
    heads_copy.wait()


def erf_gelu(x):
    return 0.5 * x * (1.0 + lax.erf(x * (2.0 ** -0.5)))


def tail_kernel(h_in, o_in, pos_in, gain_in, bias_in, wq_in, bq_in, wk_in, wv_in, bv_in, wo_in, bo_in, wcq_in, bcq_in, wco_in, bco_in,
                w1_in, b1_in, w2_in, b2_in, ckin, cvin, skin, svin,
                out_ref, knew_ref, vnew_ref, sk0, sv0, sk, sv,
                h_ref, o_ref, pos_ref, gain_ref, bias_ref, wq_ref, bq_ref, wk_ref, wv_ref, bv_ref, bo_ref, wcq_ref, bcq_ref, bco_ref,
                w1_ref, b1_ref, w2_ref, b2_ref,
                kbuf, vbuf, wofull, wcofull, obuf, osend, csend, q_scr, kv_scr, o_scr, hid_scr, pbuf, rbuf, base_scr, hblk, hslots,
                par_sem, wpar_sem, ck_sem, sk0_sem, sk_sem, wsend, wrecv, send_sem, recv_sem):
    me = lax.axis_index('tp')
    core = lax.rem(me, 2)
    chip_x = lax.rem(lax.div(me, 2), 2)
    sibling = me + 1 - 2 * core
    flip_x = 2 - 4 * chip_x
    across = lax.rem(me + 4, TP)
    holders = [me, me + flip_x, across, across + flip_x]
    far = [holders[3], holders[1], holders[2]]
    peers = far[:1] + [p + 1 - 2 * core for p in far[:1]] + far[1:] + [p + 1 - 2 * core for p in far[1:]] + [sibling]

    def fetch_cross(layer, g, which):
        src, buf = ((ckin, kbuf), (cvin, vbuf))[which]
        return pltpu.make_async_copy(src.at[layer, pl.ds(GA * g, GA)], buf.at[pl.ds(GA * g, GA)], ck_sem.at[layer, which, g])

    def fetch_self(half, which):
        src, buf = ((skin, sk), (svin, sv))[which]
        return pltpu.make_async_copy(src.at[1, pl.ds(HALF * half, HALF)], buf.at[pl.ds(HALF * half, HALF)], sk_sem.at[which, half])

    def fetch_first(step, which):
        src, buf = ((skin, sk0), (svin, sv0))[which]
        size = GB * SELF_UNROLL
        return pltpu.make_async_copy(src.at[0, pl.ds(HALF + size * step, size)], buf.at[pl.ds(size * step, size)], sk0_sem.at[which, step])

    params = [(o_in, o_ref), (h_in, h_ref), (gain_in, gain_ref), (bias_in, bias_ref), (bo_in, bo_ref), (wcq_in, wcq_ref), (bcq_in, bcq_ref),
              (bco_in, bco_ref), (w1_in, w1_ref), (b1_in, b1_ref), (w2_in, w2_ref), (b2_in, b2_ref), (pos_in, pos_ref), (wq_in, wq_ref),
              (bq_in, bq_ref), (wk_in, wk_ref), (wv_in, wv_ref), (bv_in, bv_ref)]
    copies = [pltpu.make_async_copy(src, dst, par_sem.at[i]) for i, (src, dst) in enumerate(params)]
    own = [pltpu.make_async_copy(src, full.at[me], wpar_sem.at[i]) for i, (src, full) in enumerate(((wo_in, wofull), (wco_in, wcofull)))]

    barrier = pltpu.get_barrier_semaphore()
    for peer in peers:
        pl.semaphore_signal(barrier, inc=1, device_id={'tp': peer}, device_id_type=MESH)
    for copy in copies + own:
        copy.start()
    for which in (0, 1):
        for step in HALVES:
            fetch_first(step, which).start()
    for g in range(AGROUPS):
        fetch_cross(0, g, 0).start()
        fetch_cross(0, g, 1).start()
    for half in HALVES:
        fetch_self(half, 0).start()
        fetch_self(half, 1).start()
    copies[0].wait()
    pl.semaphore_wait(barrier, TP - 1)

    def send(phase, src, dst, peer):
        return pltpu.make_async_remote_copy(src_ref=src, dst_ref=dst, send_sem=send_sem.at[phase, peer], recv_sem=recv_sem.at[phase, me],
                                            device_id={'tp': peer}, device_id_type=MESH)

    def arrival(phase, dst, peer):
        return pltpu.make_async_remote_copy(src_ref=dst, dst_ref=dst, send_sem=send_sem.at[phase, peer], recv_sem=recv_sem.at[phase, peer],
                                            device_id={'tp': peer}, device_id_type=MESH)

    def gather_start(phase, src, slots):
        for peer in peers:
            send(phase, src, slots.at[me], peer).start()

    def gather_wait(phase, src, slots):
        for peer in peers:
            arrival(phase, slots.at[peer], peer).wait_recv()
        for peer in peers:
            send(phase, src, slots.at[me], peer).wait_send()

    fulls = (wofull, wcofull)

    def to_chips(which, layer, k, slot):
        row = 2 * which + layer
        block = fulls[which].at[slot, layer]
        return pltpu.make_async_remote_copy(src_ref=block, dst_ref=block, send_sem=wsend.at[0, row, k], recv_sem=wrecv.at[0, row, k],
                                            device_id={'tp': holders[k]}, device_id_type=MESH)

    def to_sibling(which, layer, k, slot):
        row = 2 * which + layer
        block = fulls[which].at[slot, layer]
        return pltpu.make_async_remote_copy(src_ref=block, dst_ref=block, send_sem=wsend.at[1, row, k], recv_sem=wrecv.at[1, row, k],
                                            device_id={'tp': sibling}, device_id_type=MESH)

    def weights_out(which, layer):
        for k in (3, 1, 2):
            to_chips(which, layer, k, me).start()
        to_sibling(which, layer, 0, me).start()

    def weights_forward(which, layer):
        for k in (1, 2, 3):
            to_chips(which, layer, k, holders[k]).wait_recv()
            to_sibling(which, layer, k, holders[k]).start()

    def weights_settle(which, layer):
        for k in range(4):
            to_sibling(which, layer, k, holders[k] + 1 - 2 * core).wait_recv()
            to_sibling(which, layer, k, holders[k]).wait_send()
        for k in (1, 2, 3):
            to_chips(which, layer, k, me).wait_send()

    gather_start(0, o_ref, obuf.at[0, 0])
    for which in (0, 1):
        own[which].wait()
        weights_out(which, 0)
    obuf[0, 0, me] = o_ref[...]
    for copy in copies[1:]:
        copy.wait()

    low = lax.broadcasted_iota(jnp.int32, (QUART, LANES), 1) < HD

    def head_rows(stage, half):
        top, bottom = [], []
        for pair in range(TP // 2):
            left = obuf[stage, half, 2 * pair].astype(F32)
            right = obuf[stage, half, 2 * pair + 1].astype(F32)
            top.append(jnp.where(low, left, pltpu.roll(right, HD, 1)))
            bottom.append(jnp.where(low, pltpu.roll(left, HD, 1), right))
        return jnp.concatenate([jnp.concatenate(top, axis=1), jnp.concatenate(bottom, axis=1)], axis=0).astype(BF16)

    def norm_of(hid, layer, k):
        return layer_norm(hid, row_of(gain_ref, k, pl.ds(layer, 1)), row_of(bias_ref, k, pl.ds(layer, 1)))

    keep = lax.broadcasted_iota(jnp.int32, (GR, D), 1) // HD == lax.broadcasted_iota(jnp.int32, (GR, D), 0) // BEAMS

    def gathered_out(stage, half, full, layer, bias):
        return dot(head_rows(stage, half), full[:, layer].reshape(D, D)) + row_of(bias, pl.ds(layer, 1))

    def cross_half(layer, half, hid):
        stage = 2 * layer
        hid = hid + gathered_out(stage, half, wofull, layer, bo_ref)
        hid = hid.astype(BF16).astype(F32)
        hid_scr[half] = hid
        query = ((dot_nt(norm_of(hid, layer, 1), wcq_ref[layer]) + row_of(bcq_ref, pl.ds(layer, 1))) * SCALE).astype(BF16).astype(F32)
        q_scr[...] = jnp.concatenate([query, query], axis=1)
        groups = (2 * half, 2 * half + 1)
        for g in groups:
            fetch_cross(layer, g, 0).wait()
            fetch_cross(layer, g, 1).wait()
        scores, probs = [], []
        for i, g in enumerate(groups):
            q40 = q_scr[GR * i:GR * i + GR]
            qblk = jnp.where(keep, jnp.concatenate([q40, q40, q40, q40], axis=1), 0.0).astype(BF16)
            scores.append(dot(qblk, kbuf[GA * g:GA * g + GA].reshape(GA * HD, FRAMES)))
        for score in scores:
            expd = jnp.exp(score - jnp.max(score, axis=1, keepdims=True))
            probs.append((expd / jnp.sum(expd, axis=1, keepdims=True)).astype(BF16))
        outs = [fold_heads(dot_nt(prob, vbuf[GA * g:GA * g + GA].reshape(GA * HD, FRAMES)), keep) for g, prob in zip(groups, probs)]
        csend[layer, half] = jnp.concatenate(outs, axis=1).astype(BF16)
        gather_start(8 * layer + 2 + half, csend.at[layer, half], obuf.at[stage + 1, half])
        obuf[stage + 1, half, me] = csend[layer, half]

    def mlp_half(layer, half):
        stage = 2 * layer
        gather_wait(8 * layer + 2 + half, csend.at[layer, half], obuf.at[stage + 1, half])
        hid = hid_scr[half] + gathered_out(stage + 1, half, wcofull, layer, bco_ref)
        hid = hid.astype(BF16).astype(F32)
        inner = erf_gelu(dot(norm_of(hid, layer, 2), w1_ref[layer]) + row_of(b1_ref, pl.ds(layer, 1))).astype(BF16)
        part = dot(inner, w2_ref[layer]).astype(BF16)
        for t in range(TP):
            pbuf[layer, half, t] = part[QUART * (t % 2):QUART * (t % 2) + QUART, LANES * (t // 2):LANES * (t // 2) + LANES]
        for peer in peers:
            send(8 * layer + 4 + half, pbuf.at[layer, half, peer], rbuf.at[layer, half, me], peer).start()
        rbuf[layer, half, me] = pbuf[layer, half, me]
        base_scr[half] = hid + row_of(b2_ref, pl.ds(layer, 1))

    def reduce_half(layer, half):
        for peer in peers:
            arrival(8 * layer + 4 + half, rbuf.at[layer, half, peer], peer).wait_recv()
        total = rbuf[layer, half, 0].astype(F32)
        for t in range(1, TP):
            total = total + rbuf[layer, half, t].astype(F32)
        mine = base_scr[half, pl.ds(pl.multiple_of(QUART * core, 8), QUART), pl.ds(pl.multiple_of(LANES * lax.div(me, 2), LANES), LANES)]
        hblk[layer, half] = (mine + total).astype(BF16)
        gather_start(8 * layer + 6 + half, hblk.at[layer, half], hslots.at[layer, half])
        hslots[layer, half, me] = hblk[layer, half]

    def next_hidden(layer, half):
        gather_wait(8 * layer + 6 + half, hblk.at[layer, half], hslots.at[layer, half])
        for peer in peers:
            send(8 * layer + 4 + half, pbuf.at[layer, half, peer], rbuf.at[layer, half, me], peer).wait_send()
        cols = [jnp.concatenate([hslots[layer, half, 2 * c].astype(F32), hslots[layer, half, 2 * c + 1].astype(F32)], axis=0) for c in range(TP // 2)]
        return jnp.concatenate(cols, axis=1)

    lane_ctx = lax.broadcasted_iota(jnp.int32, (GB, CTX), 1)
    row_id = lax.broadcasted_iota(jnp.int32, (GB, 1), 0)
    keep8 = lax.broadcasted_iota(jnp.int32, (GB, D), 1) // HD == lax.broadcasted_iota(jnp.int32, (GB, D), 0)

    def self_half(layer, half, hid, keys, vals, base, slot):
        normed = norm_of(hid, layer, 0)
        query = ((dot_nt(normed, wq_ref[layer]) + row_of(bq_ref, pl.ds(layer, 1))) * SCALE).astype(BF16)
        key = (dot_nt(normed, wk_ref[layer]) * SCALE).astype(BF16)
        val = (dot_nt(normed, wv_ref[layer]) + row_of(bv_ref, pl.ds(layer, 1))).astype(BF16)
        knew_ref[slot] = key
        vnew_ref[slot] = val
        query = query.astype(F32)
        q_scr[...] = jnp.concatenate([query, query], axis=1)
        kv_scr[0] = jnp.broadcast_to(jnp.sum(query * key.astype(F32), axis=1, keepdims=True), (HALF, HD))
        kv_scr[1] = val.astype(F32)

        def attend(step, carry):
            if layer == 0:
                fetch_first(step, 0).wait()
                fetch_first(step, 1).wait()
            local = [step * SELF_UNROLL + u for u in range(SELF_UNROLL)]
            rows = [pl.ds(pl.multiple_of(g * GB, GB), GB) for g in local]
            slabs = [pl.ds(pl.multiple_of(base + g * GB, GB), GB) for g in local]
            scores, hits, probs, wides = [], [], [], []
            for g, row, slab in zip(local, rows, slabs):
                pos_col = jnp.zeros((GB, 1), jnp.int32)
                for j in range(GB):
                    pos_col = jnp.where(row_id == j, pos_ref[HALF * half + g * GB + j], pos_col)
                q8 = q_scr[row]
                qblk = jnp.where(keep8, jnp.concatenate([q8, q8, q8, q8], axis=1), 0.0).astype(BF16)
                score = dot(qblk, keys[slab].reshape(GB * HD, CTX))
                hit = lane_ctx == pos_col
                score = jnp.where(hit, kv_scr[0, row][:, :1], score)
                scores.append(jnp.where(lane_ctx <= pos_col, score, -1e30))
                hits.append(hit)
            for score in scores:
                expd = jnp.exp(score - jnp.max(score, axis=1, keepdims=True))
                probs.append((expd / jnp.sum(expd, axis=1, keepdims=True)).astype(BF16).astype(F32))
            for slab, prob, hit in zip(slabs, probs, hits):
                wides.append(dot_nt(jnp.where(hit, 0.0, prob).astype(BF16), vals[slab].reshape(GB * HD, CTX)))
            for row, wide, prob, hit in zip(rows, wides, probs, hits):
                fresh = jnp.sum(jnp.where(hit, prob, 0.0), axis=1, keepdims=True) * kv_scr[1, row]
                o_scr[row] = fold_heads(wide, keep8) + fresh
            return carry

        lax.fori_loop(0, GROUPS // SELF_UNROLL, attend, 0)
        osend[slot] = jnp.concatenate([o_scr[0:QUART], o_scr[QUART:HALF]], axis=1).astype(BF16)
        gather_start(8 * layer + half, osend.at[slot], obuf.at[2 * layer, half])
        obuf[2 * layer, half, me] = osend[slot]

    self_half(0, 1, h_ref[HALF:].astype(F32), sk0, sv0, 0, 0)
    weights_forward(0, 0)
    weights_settle(0, 0)
    for half in HALVES:
        gather_wait(half, osend.at[0] if half else o_ref, obuf.at[0, half])
        cross_half(0, half, h_ref[HALF * half:HALF * half + HALF].astype(F32))
        if half == 0:
            weights_forward(1, 0)
    weights_out(0, 1)
    weights_out(1, 1)
    weights_settle(1, 0)
    for g in range(AGROUPS):
        fetch_cross(1, g, 0).start()
        fetch_cross(1, g, 1).start()
    for half in HALVES:
        mlp_half(0, half)
    for half in HALVES:
        reduce_half(0, half)
    for half in HALVES:
        hid_scr[half] = next_hidden(0, half)
        fetch_self(half, 0).wait()
        fetch_self(half, 1).wait()
        self_half(1, half, hid_scr[half], sk, sv, HALF * half, 1 + half)
        weights_forward(half, 1)
    for which in (0, 1):
        weights_settle(which, 1)
    for half in HALVES:
        gather_wait(8 + half, osend.at[1 + half], obuf.at[2, half])
        cross_half(1, half, hid_scr[half])
    for half in HALVES:
        mlp_half(1, half)
    for half in HALVES:
        reduce_half(1, half)
    for half in HALVES:
        out_ref[HALF * half:HALF * half + HALF] = next_hidden(1, half).astype(BF16)


def write_kernel(pos_in, h_ref, knew_ref, vnew_ref, sk0_in, sv0_in, sk_in, sv_in, kprev, vprev, h_out, kout, vout, sk0, sv0, sk, sv,
                 pos_ref, new_scr, sem, out_sem):
    load = pltpu.make_async_copy(pos_in, pos_ref, sem.at[0])
    load.start()
    hidden = pltpu.make_async_copy(h_ref, h_out, sem.at[1])
    hidden.start()
    for part in range(3):
        new_scr[0, HALF * part:HALF * part + HALF] = knew_ref[part].astype(F32)
        new_scr[1, HALF * part:HALF * part + HALF] = vnew_ref[part].astype(F32)
    eye = (lax.broadcasted_iota(jnp.int32, (HD, HD), 0) == lax.broadcasted_iota(jnp.int32, (HD, HD), 1)).astype(BF16)
    load.wait()

    def rows(g, first=0):
        return pl.ds(pl.multiple_of(first + g * GB, GB), GB)

    pieces = (((sk0, sv0), 0, HALF, 0, GROUPS), ((sk, sv), 1, 0, HALF, 2 * GROUPS))

    def put(piece, g, which):
        bufs, layer, first = pieces[piece][:3]
        return pltpu.make_async_copy(bufs[which].at[rows(g)], (kout, vout)[which].at[layer, rows(g, first)], out_sem.at[piece, which, g])

    for piece, (bufs, layer, first, new_first, count) in enumerate(pieces):
        def insert(step, carry):
            groups = [step * 2 + u for u in range(2)]
            cols = [[dot_nt(eye, new_scr[which, rows(g, new_first)].astype(BF16)) for which in range(2)] for g in groups]
            for g, pair in zip(groups, cols):
                insert_columns(g, pos_ref, first, tuple(zip(bufs, pair)))
            for g in groups:
                put(piece, g, 0).start()
                put(piece, g, 1).start()
            return carry

        lax.fori_loop(0, count // 2, insert, 0)

    for piece in range(2):
        def finish(g, carry):
            put(piece, g, 0).wait()
            put(piece, g, 1).wait()
            return carry

        lax.fori_loop(0, pieces[piece][4], finish, 0)
    hidden.wait()


HBM = pl.BlockSpec(memory_space=pltpu.HBM)
VM = pl.BlockSpec(memory_space=pltpu.VMEM)


def in_hbm(*arrays):
    return [pltpu.with_memory_space_constraint(array, pltpu.HBM) for array in arrays]


def self_call(layer, positions, hidden, w, keys, vals):
    cache = jax.ShapeDtypeStruct(keys.shape, BF16)
    args = [positions, hidden, w['ln_gain'], w['ln_bias'], w['w_query'], w['b_query'], w['w_key'], w['w_value'], w['b_value'], keys, vals]
    return pl.pallas_call(
        functools.partial(self_kernel, layer),
        out_shape=(jax.ShapeDtypeStruct((QUART, LANES), BF16), cache, cache),
        in_specs=[HBM] * len(args),
        out_specs=(HBM, HBM, HBM),
        scratch_shapes=[
            pltpu.VMEM((QUART, LANES), BF16),
            pltpu.VMEM((HALF, HD, CTX), BF16),
            pltpu.VMEM((HALF, HD, CTX), BF16),
            pltpu.SMEM((BATCH,), jnp.int32),
            pltpu.VMEM((HALF, D), BF16),
            pltpu.VMEM((3, 2, D), BF16),
            pltpu.VMEM((3, 2, D), BF16),
            pltpu.VMEM((HD, D), BF16),
            pltpu.VMEM((2, HD), BF16),
            pltpu.VMEM((HD, D), BF16),
            pltpu.VMEM((HD, D), BF16),
            pltpu.VMEM((2, HD), BF16),
            pltpu.VMEM((HALF, 2 * HD), F32),
            pltpu.VMEM((HALF, D), F32),
            pltpu.VMEM((GROUPS, HD, GB), F32),
            pltpu.VMEM((GROUPS, HD, GB), F32),
            pltpu.VMEM((HALF, HD), F32),
            pltpu.SemaphoreType.DMA((9,)),
            pltpu.SemaphoreType.DMA((2, GROUPS)),
            pltpu.SemaphoreType.DMA((2, GROUPS)),
        ],
        compiler_params=pltpu.CompilerParams(vmem_limit_bytes=VMEM_LIMIT),
        cost_estimate=pl.CostEstimate(flops=10 ** 10, bytes_accessed=21 * 2 ** 20, transcendentals=HALF * CTX),
        name=f'self_attention_{layer}',
    )(*in_hbm(*args))


def tail_call(positions, hidden, heads, w, cross_k, cross_v, keys, vals):
    args = [hidden, heads, positions, w['ln_gain'], w['ln_bias'], w['w_query'], w['b_query'], w['w_key'], w['w_value'], w['b_value'], w['w_out'], w['b_out'],
            w['w_cquery'], w['b_cquery'], w['w_cout'], w['b_cout'], w['w_fc1'], w['b_fc1'], w['w_fc2'], w['b_fc2'], cross_k, cross_v, keys, vals]
    new = jax.ShapeDtypeStruct((3, HALF, HD), BF16)
    half = jax.ShapeDtypeStruct((HALF, HD, CTX), BF16)
    cache = jax.ShapeDtypeStruct((BATCH, HD, CTX), BF16)
    pair = (2, TP, QUART, LANES)
    return pl.pallas_call(
        tail_kernel,
        out_shape=(jax.ShapeDtypeStruct((BATCH, D), BF16), new, new, half, half, cache, cache),
        in_specs=[HBM] * len(args),
        out_specs=(VM,) * 7,
        scratch_shapes=[
            pltpu.VMEM((BATCH, D), BF16),
            pltpu.VMEM((QUART, LANES), BF16),
            pltpu.SMEM((BATCH,), jnp.int32),
            pltpu.VMEM((3, 2, D), BF16),
            pltpu.VMEM((3, 2, D), BF16),
            pltpu.VMEM((2, HD, D), BF16),
            pltpu.VMEM((2, HD), BF16),
            pltpu.VMEM((2, HD, D), BF16),
            pltpu.VMEM((2, HD, D), BF16),
            pltpu.VMEM((2, HD), BF16),
            pltpu.VMEM((2, D), BF16),
            pltpu.VMEM((2, HD, D), BF16),
            pltpu.VMEM((2, HD), BF16),
            pltpu.VMEM((2, D), BF16),
            pltpu.VMEM((2, D, 256), BF16),
            pltpu.VMEM((2, 256), BF16),
            pltpu.VMEM((2, 256, D), BF16),
            pltpu.VMEM((2, D), BF16),
            pltpu.VMEM((AUD, HD, FRAMES), BF16),
            pltpu.VMEM((AUD, HD, FRAMES), BF16),
            pltpu.VMEM((TP, 2, HD, D), BF16),
            pltpu.VMEM((TP, 2, HD, D), BF16),
            pltpu.VMEM((4,) + pair, BF16),
            pltpu.VMEM((3, QUART, LANES), BF16),
            pltpu.VMEM((2, 2, QUART, LANES), BF16),
            pltpu.VMEM((BATCH // 2, 2 * HD), F32),
            pltpu.VMEM((2, BATCH // 2, HD), F32),
            pltpu.VMEM((BATCH // 2, HD), F32),
            pltpu.VMEM((2, BATCH // 2, D), F32),
            pltpu.VMEM((2,) + pair, BF16),
            pltpu.VMEM((2,) + pair, BF16),
            pltpu.VMEM((2, BATCH // 2, D), F32),
            pltpu.VMEM((2, 2, QUART, LANES), BF16),
            pltpu.VMEM((2,) + pair, BF16),
            pltpu.SemaphoreType.DMA((18,)),
            pltpu.SemaphoreType.DMA((2,)),
            pltpu.SemaphoreType.DMA((2, 2, AGROUPS)),
            pltpu.SemaphoreType.DMA((2, 2)),
            pltpu.SemaphoreType.DMA((2, 2)),
            pltpu.SemaphoreType.DMA((2, 4, 4)),
            pltpu.SemaphoreType.DMA((2, 4, 4)),
            pltpu.SemaphoreType.DMA((16, TP)),
            pltpu.SemaphoreType.DMA((16, TP)),
        ],
        compiler_params=pltpu.CompilerParams(vmem_limit_bytes=TAIL_LIMIT, collective_id=0, has_side_effects=True),
        cost_estimate=pl.CostEstimate(flops=10 ** 10, bytes_accessed=46 * 2 ** 20, transcendentals=2 * BATCH * FRAMES),
        name='cross_mlp_and_next_layer',
    )(*in_hbm(*args))


def write_call(positions, hidden, knew, vnew, held, prev):
    shapes = [jax.ShapeDtypeStruct(x.shape, BF16) for x in (hidden, *prev, *held)]
    return pl.pallas_call(
        write_kernel,
        out_shape=tuple(shapes),
        in_specs=[HBM] + [VM] * 7 + [HBM, HBM],
        out_specs=(HBM, HBM, HBM, VM, VM, VM, VM),
        input_output_aliases={4: 3, 5: 4, 6: 5, 7: 6, 8: 1, 9: 2},
        scratch_shapes=[
            pltpu.SMEM((BATCH,), jnp.int32),
            pltpu.VMEM((2, 3 * HALF, HD), F32),
            pltpu.SemaphoreType.DMA((2,)),
            pltpu.SemaphoreType.DMA((2, 2, 2 * GROUPS)),
        ],
        compiler_params=pltpu.CompilerParams(vmem_limit_bytes=WRITE_LIMIT),
        cost_estimate=pl.CostEstimate(flops=10 ** 8, bytes_accessed=32 * 2 ** 20, transcendentals=0),
        name='write_caches',
    )(*in_hbm(positions), hidden, knew, vnew, *held, *in_hbm(*prev))


def solution(mesh):
    cache_spec = P(None, 'dp', None, 'tp', None)
    col_spec = P(None, None, 'tp')
    row_spec = P(None, 'tp', None)
    vec_spec = P(None, 'tp')
    param_specs = {'ln_gain': P(), 'ln_bias': P(), 'w_query': col_spec, 'b_query': vec_spec, 'w_key': col_spec, 'w_value': col_spec, 'b_value': vec_spec, 'w_out': row_spec, 'b_out': P(), 'w_cquery': col_spec, 'b_cquery': vec_spec, 'w_cout': row_spec, 'b_cout': P(), 'w_fc1': col_spec, 'b_fc1': vec_spec, 'w_fc2': row_spec, 'b_fc2': P()}
    in_specs = (P('dp', None), P('dp'), cache_spec, cache_spec, cache_spec, cache_spec) + tuple(param_specs[param_name] for param_name in PARAM_NAMES)

    def lanes_last(cache):
        return jnp.transpose(cache, (0, 1, 3, 4, 2)).reshape(cache.shape[0], cache.shape[1], cache.shape[4], cache.shape[2])

    def slots_back(cache):
        layers, beams, width, slots = cache.shape
        return jnp.transpose(cache.reshape(layers, beams, 1, width, slots), (0, 1, 4, 2, 3))

    def local_step(hidden, positions, self_keys, self_vals, cross_keys, cross_vals, *layer_params):
        w = dict(zip(PARAM_NAMES, layer_params))
        for name in ('w_query', 'w_key', 'w_value', 'w_cquery'):
            w[name] = jnp.transpose(w[name], (0, 2, 1))
        for name in ('ln_gain', 'ln_bias'):
            w[name] = jnp.transpose(w[name], (1, 0, 2))
        keys, vals, cross_k, cross_v = (lanes_last(c) for c in (self_keys, self_vals, cross_keys, cross_vals))
        heads, *prev = self_call(0, positions, hidden, w, keys, vals)
        hidden, knew, vnew, *held = tail_call(positions, hidden, heads, w, cross_k, cross_v, keys, vals)
        hidden, new_keys, new_vals = write_call(positions, hidden, knew, vnew, held, prev)[:3]
        return hidden, slots_back(new_keys), slots_back(new_vals)

    return jax.shard_map(local_step, mesh=mesh, in_specs=in_specs, out_specs=(P('dp', None), cache_spec, cache_spec), check_vma=False)
```

```python
import functools

import jax
import jax.numpy as jnp
from jax import lax
from jax.experimental import pallas as pl
from jax.experimental.pallas import tpu as pltpu
from jax.sharding import PartitionSpec as P

EPS = 1e-5
F32 = jnp.float32
BF16 = jnp.bfloat16
NT = (((1,), (1,)), ((), ()))
MESH = pl.DeviceIdType.MESH
PARAM_NAMES = ('ln_gain', 'ln_bias', 'w_query', 'b_query', 'w_key', 'w_value', 'b_value', 'w_out', 'b_out', 'w_cquery', 'b_cquery', 'w_cout', 'b_cout', 'w_fc1', 'b_fc1', 'w_fc2', 'b_fc2')

BATCH = 160
AUD = 32
BEAMS = 5
HD = 64
CTX = 448
FRAMES = 1500
D = 512
TP = 8
SCALE = HD ** -0.25
GB = 8
GROUPS = BATCH // GB // 2
VMEM_LIMIT = 67_000_000
TAIL_LIMIT = 20 * 2 ** 20
WRITE_LIMIT = 12 * 2 ** 20
SELF_UNROLL = 5
UNROLL = 2
GA = 8
AGROUPS = AUD // GA
GR = GA * BEAMS
HALF = BATCH // 2
QUART = BATCH // 4
HALVES = range(2)
LANES = 128


def layer_norm(wide, gain, bias):
    center = wide - jnp.mean(wide, axis=-1, keepdims=True)
    var_est = jnp.mean(center * center, axis=-1, keepdims=True)
    return (center * lax.rsqrt(var_est + EPS) * gain + bias).astype(BF16)


def row_of(ref, *idx):
    return ref[idx].astype(F32)


def dot_nt(a, b):
    return lax.dot_general(a, b, NT, preferred_element_type=F32)


def dot(a, b):
    return jnp.dot(a, b, preferred_element_type=F32)


def fold_heads(wide, keep):
    wide = jnp.where(keep, wide, 0.0)
    part = (wide[:, 0:LANES] + wide[:, LANES:256]) + (wide[:, 256:384] + wide[:, 384:512])
    return part[:, :HD] + part[:, HD:]


def insert_columns(g, pos_ref, first, pairs):
    lane128 = lax.broadcasted_iota(jnp.int32, (HD, LANES), 1)
    lane64 = lax.broadcasted_iota(jnp.int32, (HD, HD), 1) + 384
    row_id = lax.broadcasted_iota(jnp.int32, (GB, 1), 0)
    pos_col = jnp.zeros((GB, 1), jnp.int32)
    for j in range(GB):
        beam = g * GB + j
        pos = pos_ref[first + beam]
        pos_col = jnp.where(row_id == j, pos, pos_col)
        off = pl.multiple_of(jnp.minimum(pos // LANES, 2) * LANES, LANES)
        for buf, cols in pairs:
            col = jnp.broadcast_to(cols[:, j:j + 1], (HD, LANES)).astype(BF16)
            view = buf.at[beam, :, pl.ds(off, LANES)]
            view[...] = jnp.where(lane128 + off == pos, col, view[...])
            tail = buf.at[beam, :, pl.ds(384, 64)]
            tail[...] = jnp.where(lane64 == pos, col[:, :HD], tail[...])
    return pos_col


def self_kernel(layer, pos_in, h_in, gain_in, bias_in, wq_in, bq_in, wk_in, wv_in, bv_in, kin, vin, *rest):
    (o_out, kout, vout, o_ref, kbuf, vbuf, pos_ref, h_ref, gain_ref, bias_ref, wq_ref, bq_ref, wk_ref, wv_ref, bv_ref,
     q_scr, a_scr, kt_scr, vt_scr, o_scr, par_sem, in_sem, out_sem) = rest

    def rows(g):
        return pl.ds(pl.multiple_of(g * GB, GB), GB)

    def fetch(g, which):
        src, buf = ((kin, kbuf), (vin, vbuf))[which]
        return pltpu.make_async_copy(src.at[layer, rows(g)], buf.at[rows(g)], in_sem.at[which, g])

    def put(g, which):
        buf, dst = ((kbuf, kout), (vbuf, vout))[which]
        return pltpu.make_async_copy(buf.at[rows(g)], dst.at[layer, rows(g)], out_sem.at[which, g])

    params = [(pos_in, pos_ref), (gain_in, gain_ref), (bias_in, bias_ref), (bq_in, bq_ref), (bv_in, bv_ref),
              (wq_in.at[layer], wq_ref), (wk_in.at[layer], wk_ref), (wv_in.at[layer], wv_ref)]
    params.append((h_in.at[pl.ds(0, HALF)], h_ref))
    copies = [pltpu.make_async_copy(src, dst, par_sem.at[i]) for i, (src, dst) in enumerate(params)]
    for copy in copies:
        copy.start()

    def start_fetch(g, carry):
        fetch(g, 0).start()
        fetch(g, 1).start()
        return carry

    lax.fori_loop(0, GROUPS, start_fetch, 0)
    for copy in copies:
        copy.wait()

    normed = layer_norm(h_ref[...].astype(F32), row_of(gain_ref, 0, pl.ds(layer, 1)), row_of(bias_ref, 0, pl.ds(layer, 1)))
    query = ((dot_nt(normed, wq_ref[...]) + row_of(bq_ref, pl.ds(layer, 1))) * SCALE).astype(BF16).astype(F32)
    q_scr[...] = jnp.concatenate([query, query], axis=1)
    a_scr[...] = normed.astype(F32)
    eye = lax.broadcasted_iota(jnp.int32, (HD, HD), 0) == lax.broadcasted_iota(jnp.int32, (HD, HD), 1)
    bv_col = jnp.sum(jnp.where(eye, row_of(bv_ref, pl.ds(layer, 1)), 0.0), axis=1, keepdims=True)

    def project(g, carry):
        part = a_scr[rows(g)].astype(BF16)
        kt_scr[g] = dot_nt(wk_ref[...], part) * SCALE
        vt_scr[g] = dot_nt(wv_ref[...], part) + bv_col
        return carry

    lax.fori_loop(0, GROUPS, project, 0, unroll=5)

    lane_ctx = lax.broadcasted_iota(jnp.int32, (GB, CTX), 1)
    keep = lax.broadcasted_iota(jnp.int32, (GB, D), 1) // HD == lax.broadcasted_iota(jnp.int32, (GB, D), 0)

    def attend(step, carry):
        groups = [step * UNROLL + u for u in range(UNROLL)]
        pos_cols, scores, probs = [], [], []
        for g in groups:
            fetch(g, 0).wait()
            fetch(g, 1).wait()
        for g in groups:
            pos_cols.append(insert_columns(g, pos_ref, 0, ((kbuf, kt_scr[g]), (vbuf, vt_scr[g]))))
        for g, pos_col in zip(groups, pos_cols):
            q8 = q_scr[rows(g)]
            qblk = jnp.where(keep, jnp.concatenate([q8, q8, q8, q8], axis=1), 0.0).astype(BF16)
            scores.append(jnp.where(lane_ctx <= pos_col, dot(qblk, kbuf[rows(g)].reshape(GB * HD, CTX)), -1e30))
        for score in scores:
            expd = jnp.exp(score - jnp.max(score, axis=1, keepdims=True))
            probs.append((expd / jnp.sum(expd, axis=1, keepdims=True)).astype(BF16))
        wides = [dot_nt(prob, vbuf[rows(g)].reshape(GB * HD, CTX)) for g, prob in zip(groups, probs)]
        for g, wide in zip(groups, wides):
            o_scr[rows(g)] = fold_heads(wide, keep)
            put(g, 0).start()
            put(g, 1).start()
        return carry

    lax.fori_loop(0, GROUPS // UNROLL, attend, 0)
    o_ref[...] = jnp.concatenate([o_scr[0:QUART], o_scr[QUART:HALF]], axis=1).astype(BF16)
    heads_copy = pltpu.make_async_copy(o_ref, o_out, par_sem.at[0])
    heads_copy.start()

    def finish(g, carry):
        put(g, 0).wait()
        put(g, 1).wait()
        return carry

    lax.fori_loop(0, GROUPS, finish, 0)
    heads_copy.wait()


def erf_gelu(x):
    return 0.5 * x * (1.0 + lax.erf(x * (2.0 ** -0.5)))


def tail_kernel(h_in, o_in, pos_in, gain_in, bias_in, wq_in, bq_in, wk_in, wv_in, bv_in, wo0, wo2, wo4, wo6, bo_in, wcq_in, bcq_in, wco_in, bco_in,
                w1_in, b1_in, w2_in, b2_in, ckin, cvin, skin, svin,
                out_ref, knew_ref, vnew_ref, sk0, sv0, sk, sv,
                h_ref, o_ref, pos_ref, gain_ref, bias_ref, wq_ref, bq_ref, wk_ref, wv_ref, bv_ref, bo_ref, wcq_ref, bcq_ref, bco_ref,
                w1_ref, b1_ref, w2_ref, b2_ref,
                kbuf, vbuf, wofull, wcofull, obuf, osend, csend, q_scr, kv_scr, o_scr, hid_scr, pbuf, rbuf, base_scr, hblk, hslots,
                par_sem, wpar_sem, ck_sem, sk0_sem, sk_sem, wsend, wrecv, send_sem, recv_sem):
    me = lax.axis_index('tp')
    core = lax.rem(me, 2)
    chip_x = lax.rem(lax.div(me, 2), 2)
    sibling = me + 1 - 2 * core
    flip_x = 2 - 4 * chip_x
    across = lax.rem(me + 4, TP)
    holders = [me, me + flip_x, across, across + flip_x]
    far = [holders[3], holders[1], holders[2]]
    peers = far[:1] + [p + 1 - 2 * core for p in far[:1]] + far[1:] + [p + 1 - 2 * core for p in far[1:]] + [sibling]

    def fetch_cross(layer, g, which):
        src, buf = ((ckin, kbuf), (cvin, vbuf))[which]
        return pltpu.make_async_copy(src.at[layer, pl.ds(GA * g, GA)], buf.at[pl.ds(GA * g, GA)], ck_sem.at[layer, which, g])

    def fetch_self(half, which):
        src, buf = ((skin, sk), (svin, sv))[which]
        return pltpu.make_async_copy(src.at[1, pl.ds(HALF * half, HALF)], buf.at[pl.ds(HALF * half, HALF)], sk_sem.at[which, half])

    def fetch_first(step, which):
        src, buf = ((skin, sk0), (svin, sv0))[which]
        size = GB * SELF_UNROLL
        return pltpu.make_async_copy(src.at[0, pl.ds(HALF + size * step, size)], buf.at[pl.ds(size * step, size)], sk0_sem.at[which, step])

    params = [(o_in, o_ref), (h_in, h_ref), (gain_in, gain_ref), (bias_in, bias_ref), (bo_in, bo_ref), (wcq_in, wcq_ref), (bcq_in, bcq_ref),
              (bco_in, bco_ref), (w1_in, w1_ref), (b1_in, b1_ref), (w2_in, w2_ref), (b2_in, b2_ref), (pos_in, pos_ref), (wq_in, wq_ref),
              (bq_in, bq_ref), (wk_in, wk_ref), (wv_in, wv_ref), (bv_in, bv_ref)]
    copies = [pltpu.make_async_copy(src, dst, par_sem.at[i]) for i, (src, dst) in enumerate(params)]
    wo_src = (wo0, wo2, wo4, wo6)
    own = [pltpu.make_async_copy(wo_src[k], wofull.at[holders[k]], wpar_sem.at[k]) for k in range(4)]
    own.append(pltpu.make_async_copy(wco_in, wcofull.at[me], wpar_sem.at[4]))

    barrier = pltpu.get_barrier_semaphore()
    for peer in peers:
        pl.semaphore_signal(barrier, inc=1, device_id={'tp': peer}, device_id_type=MESH)
    for copy in copies + own:
        copy.start()
    for which in (0, 1):
        for step in HALVES:
            fetch_first(step, which).start()
    for g in range(AGROUPS):
        fetch_cross(0, g, 0).start()
        fetch_cross(0, g, 1).start()
    for half in HALVES:
        fetch_self(half, 0).start()
        fetch_self(half, 1).start()
    copies[0].wait()
    pl.semaphore_wait(barrier, TP - 1)

    def send(phase, src, dst, peer):
        return pltpu.make_async_remote_copy(src_ref=src, dst_ref=dst, send_sem=send_sem.at[phase, peer], recv_sem=recv_sem.at[phase, me],
                                            device_id={'tp': peer}, device_id_type=MESH)

    def arrival(phase, dst, peer):
        return pltpu.make_async_remote_copy(src_ref=dst, dst_ref=dst, send_sem=send_sem.at[phase, peer], recv_sem=recv_sem.at[phase, peer],
                                            device_id={'tp': peer}, device_id_type=MESH)

    def gather_start(phase, src, slots):
        for peer in peers:
            send(phase, src, slots.at[me], peer).start()

    def gather_wait(phase, src, slots):
        for peer in peers:
            arrival(phase, slots.at[peer], peer).wait_recv()
        for peer in peers:
            send(phase, src, slots.at[me], peer).wait_send()

    def weight_copy(row, k, src, dst, target):
        return pltpu.make_async_remote_copy(src_ref=src, dst_ref=dst, send_sem=wsend.at[row, k], recv_sem=wrecv.at[row, k],
                                            device_id={'tp': target}, device_id_type=MESH)

    wo_fwd = [weight_copy(0, k, wo_src[k], wofull.at[holders[k]], sibling) for k in range(4)]
    wco_out = [weight_copy(1, k, wco_in, wcofull.at[me], holders[k]) for k in range(1, 4)]
    wco_fwd = [weight_copy(2, 0, wco_in, wcofull.at[me], sibling)] + [
        weight_copy(2, k, wcofull.at[holders[k]], wcofull.at[holders[k]], sibling) for k in range(1, 4)]

    gather_start(0, o_ref, obuf.at[0, 0])
    for copy in wo_fwd:
        copy.start()
    obuf[0, 0, me] = o_ref[...]
    for copy in copies[1:]:
        copy.wait()

    low = lax.broadcasted_iota(jnp.int32, (QUART, LANES), 1) < HD

    def head_rows(stage, half):
        top, bottom = [], []
        for pair in range(TP // 2):
            left = obuf[stage, half, 2 * pair].astype(F32)
            right = obuf[stage, half, 2 * pair + 1].astype(F32)
            top.append(jnp.where(low, left, pltpu.roll(right, HD, 1)))
            bottom.append(jnp.where(low, pltpu.roll(left, HD, 1), right))
        return jnp.concatenate([jnp.concatenate(top, axis=1), jnp.concatenate(bottom, axis=1)], axis=0).astype(BF16)

    def norm_of(hid, layer, k):
        return layer_norm(hid, row_of(gain_ref, k, pl.ds(layer, 1)), row_of(bias_ref, k, pl.ds(layer, 1)))

    keep = lax.broadcasted_iota(jnp.int32, (GR, D), 1) // HD == lax.broadcasted_iota(jnp.int32, (GR, D), 0) // BEAMS

    def gathered_out(stage, half, full, layer, bias):
        return dot(head_rows(stage, half), full[:, layer].reshape(D, D)) + row_of(bias, pl.ds(layer, 1))

    def cross_half(layer, half, hid):
        stage = 2 * layer
        hid = hid + gathered_out(stage, half, wofull, layer, bo_ref)
        hid = hid.astype(BF16).astype(F32)
        hid_scr[half] = hid
        query = ((dot_nt(norm_of(hid, layer, 1), wcq_ref[layer]) + row_of(bcq_ref, pl.ds(layer, 1))) * SCALE).astype(BF16).astype(F32)
        q_scr[...] = jnp.concatenate([query, query], axis=1)
        groups = (2 * half, 2 * half + 1)
        for g in groups:
            fetch_cross(layer, g, 0).wait()
            fetch_cross(layer, g, 1).wait()
        scores, probs = [], []
        for i, g in enumerate(groups):
            q40 = q_scr[GR * i:GR * i + GR]
            qblk = jnp.where(keep, jnp.concatenate([q40, q40, q40, q40], axis=1), 0.0).astype(BF16)
            scores.append(dot(qblk, kbuf[GA * g:GA * g + GA].reshape(GA * HD, FRAMES)))
        for score in scores:
            expd = jnp.exp(score - jnp.max(score, axis=1, keepdims=True))
            probs.append((expd / jnp.sum(expd, axis=1, keepdims=True)).astype(BF16))
        outs = [fold_heads(dot_nt(prob, vbuf[GA * g:GA * g + GA].reshape(GA * HD, FRAMES)), keep) for g, prob in zip(groups, probs)]
        csend[layer, half] = jnp.concatenate(outs, axis=1).astype(BF16)
        gather_start(8 * layer + 2 + half, csend.at[layer, half], obuf.at[stage + 1, half])
        obuf[stage + 1, half, me] = csend[layer, half]

    def mlp_half(layer, half):
        stage = 2 * layer
        gather_wait(8 * layer + 2 + half, csend.at[layer, half], obuf.at[stage + 1, half])
        hid = hid_scr[half] + gathered_out(stage + 1, half, wcofull, layer, bco_ref)
        hid = hid.astype(BF16).astype(F32)
        inner = erf_gelu(dot(norm_of(hid, layer, 2), w1_ref[layer]) + row_of(b1_ref, pl.ds(layer, 1))).astype(BF16)
        part = dot(inner, w2_ref[layer]).astype(BF16)
        for t in range(TP):
            pbuf[layer, half, t] = part[QUART * (t % 2):QUART * (t % 2) + QUART, LANES * (t // 2):LANES * (t // 2) + LANES]
        for peer in peers:
            send(8 * layer + 4 + half, pbuf.at[layer, half, peer], rbuf.at[layer, half, me], peer).start()
        rbuf[layer, half, me] = pbuf[layer, half, me]
        base_scr[half] = hid + row_of(b2_ref, pl.ds(layer, 1))

    def reduce_half(layer, half):
        for peer in peers:
            arrival(8 * layer + 4 + half, rbuf.at[layer, half, peer], peer).wait_recv()
        total = rbuf[layer, half, 0].astype(F32)
        for t in range(1, TP):
            total = total + rbuf[layer, half, t].astype(F32)
        mine = base_scr[half, pl.ds(pl.multiple_of(QUART * core, 8), QUART), pl.ds(pl.multiple_of(LANES * lax.div(me, 2), LANES), LANES)]
        hblk[layer, half] = (mine + total).astype(BF16)
        gather_start(8 * layer + 6 + half, hblk.at[layer, half], hslots.at[layer, half])
        hslots[layer, half, me] = hblk[layer, half]

    def next_hidden(layer, half):
        gather_wait(8 * layer + 6 + half, hblk.at[layer, half], hslots.at[layer, half])
        for peer in peers:
            send(8 * layer + 4 + half, pbuf.at[layer, half, peer], rbuf.at[layer, half, me], peer).wait_send()
        cols = [jnp.concatenate([hslots[layer, half, 2 * c].astype(F32), hslots[layer, half, 2 * c + 1].astype(F32)], axis=0) for c in range(TP // 2)]
        return jnp.concatenate(cols, axis=1)

    lane_ctx = lax.broadcasted_iota(jnp.int32, (GB, CTX), 1)
    row_id = lax.broadcasted_iota(jnp.int32, (GB, 1), 0)
    keep8 = lax.broadcasted_iota(jnp.int32, (GB, D), 1) // HD == lax.broadcasted_iota(jnp.int32, (GB, D), 0)

    def self_half(layer, half, hid, keys, vals, base, slot):
        normed = norm_of(hid, layer, 0)
        query = ((dot_nt(normed, wq_ref[layer]) + row_of(bq_ref, pl.ds(layer, 1))) * SCALE).astype(BF16)
        key = (dot_nt(normed, wk_ref[layer]) * SCALE).astype(BF16)
        val = (dot_nt(normed, wv_ref[layer]) + row_of(bv_ref, pl.ds(layer, 1))).astype(BF16)
        knew_ref[slot] = key
        vnew_ref[slot] = val
        query = query.astype(F32)
        q_scr[...] = jnp.concatenate([query, query], axis=1)
        kv_scr[0] = jnp.broadcast_to(jnp.sum(query * key.astype(F32), axis=1, keepdims=True), (HALF, HD))
        kv_scr[1] = val.astype(F32)

        def attend(step, carry):
            if layer == 0:
                fetch_first(step, 0).wait()
                fetch_first(step, 1).wait()
            local = [step * SELF_UNROLL + u for u in range(SELF_UNROLL)]
            rows = [pl.ds(pl.multiple_of(g * GB, GB), GB) for g in local]
            slabs = [pl.ds(pl.multiple_of(base + g * GB, GB), GB) for g in local]
            scores, hits, probs, wides = [], [], [], []
            for g, row, slab in zip(local, rows, slabs):
                pos_col = jnp.zeros((GB, 1), jnp.int32)
                for j in range(GB):
                    pos_col = jnp.where(row_id == j, pos_ref[HALF * half + g * GB + j], pos_col)
                q8 = q_scr[row]
                qblk = jnp.where(keep8, jnp.concatenate([q8, q8, q8, q8], axis=1), 0.0).astype(BF16)
                score = dot(qblk, keys[slab].reshape(GB * HD, CTX))
                hit = lane_ctx == pos_col
                score = jnp.where(hit, kv_scr[0, row][:, :1], score)
                scores.append(jnp.where(lane_ctx <= pos_col, score, -1e30))
                hits.append(hit)
            for score in scores:
                expd = jnp.exp(score - jnp.max(score, axis=1, keepdims=True))
                probs.append((expd / jnp.sum(expd, axis=1, keepdims=True)).astype(BF16).astype(F32))
            for slab, prob, hit in zip(slabs, probs, hits):
                wides.append(dot_nt(jnp.where(hit, 0.0, prob).astype(BF16), vals[slab].reshape(GB * HD, CTX)))
            for row, wide, prob, hit in zip(rows, wides, probs, hits):
                fresh = jnp.sum(jnp.where(hit, prob, 0.0), axis=1, keepdims=True) * kv_scr[1, row]
                o_scr[row] = fold_heads(wide, keep8) + fresh
            return carry

        lax.fori_loop(0, GROUPS // SELF_UNROLL, attend, 0)
        osend[slot] = jnp.concatenate([o_scr[0:QUART], o_scr[QUART:HALF]], axis=1).astype(BF16)
        gather_start(8 * layer + half, osend.at[slot], obuf.at[2 * layer, half])
        obuf[2 * layer, half, me] = osend[slot]

    self_half(0, 1, h_ref[HALF:].astype(F32), sk0, sv0, 0, 0)
    for copy in wco_out + wco_fwd[:1]:
        copy.start()
    for copy in own + wo_fwd:
        copy.wait()
    for half in HALVES:
        gather_wait(half, osend.at[0] if half else o_ref, obuf.at[0, half])
        cross_half(0, half, h_ref[HALF * half:HALF * half + HALF].astype(F32))
        if half == 1:
            for k in range(1, 4):
                weight_copy(1, k, wco_in, wcofull.at[holders[k]], holders[k]).wait_recv()
            for copy in wco_fwd[1:]:
                copy.start()
    for copy in wco_out + wco_fwd:
        copy.wait_send()
    for k in range(4):
        other = holders[k] + 1 - 2 * core
        weight_copy(2, k, wco_in, wcofull.at[other], sibling).wait_recv()
    for g in range(AGROUPS):
        fetch_cross(1, g, 0).start()
        fetch_cross(1, g, 1).start()
    for half in HALVES:
        mlp_half(0, half)
    for half in HALVES:
        reduce_half(0, half)
    for half in HALVES:
        hid_scr[half] = next_hidden(0, half)
        fetch_self(half, 0).wait()
        fetch_self(half, 1).wait()
        self_half(1, half, hid_scr[half], sk, sv, HALF * half, 1 + half)
    for half in HALVES:
        gather_wait(8 + half, osend.at[1 + half], obuf.at[2, half])
        cross_half(1, half, hid_scr[half])
    for half in HALVES:
        mlp_half(1, half)
    for half in HALVES:
        reduce_half(1, half)
    for half in HALVES:
        out_ref[HALF * half:HALF * half + HALF] = next_hidden(1, half).astype(BF16)


def write_kernel(pos_in, h_ref, knew_ref, vnew_ref, sk0_in, sv0_in, sk_in, sv_in, kprev, vprev, h_out, kout, vout, sk0, sv0, sk, sv,
                 pos_ref, new_scr, sem, out_sem):
    load = pltpu.make_async_copy(pos_in, pos_ref, sem.at[0])
    load.start()
    hidden = pltpu.make_async_copy(h_ref, h_out, sem.at[1])
    hidden.start()
    for part in range(3):
        new_scr[0, HALF * part:HALF * part + HALF] = knew_ref[part].astype(F32)
        new_scr[1, HALF * part:HALF * part + HALF] = vnew_ref[part].astype(F32)
    eye = (lax.broadcasted_iota(jnp.int32, (HD, HD), 0) == lax.broadcasted_iota(jnp.int32, (HD, HD), 1)).astype(BF16)
    load.wait()

    def rows(g, first=0):
        return pl.ds(pl.multiple_of(first + g * GB, GB), GB)

    pieces = (((sk0, sv0), 0, HALF, 0, GROUPS), ((sk, sv), 1, 0, HALF, 2 * GROUPS))

    def put(piece, g, which):
        bufs, layer, first = pieces[piece][:3]
        return pltpu.make_async_copy(bufs[which].at[rows(g)], (kout, vout)[which].at[layer, rows(g, first)], out_sem.at[piece, which, g])

    for piece, (bufs, layer, first, new_first, count) in enumerate(pieces):
        def insert(step, carry):
            groups = [step * 2 + u for u in range(2)]
            cols = [[dot_nt(eye, new_scr[which, rows(g, new_first)].astype(BF16)) for which in range(2)] for g in groups]
            for g, pair in zip(groups, cols):
                insert_columns(g, pos_ref, first, tuple(zip(bufs, pair)))
            for g in groups:
                put(piece, g, 0).start()
                put(piece, g, 1).start()
            return carry

        lax.fori_loop(0, count // 2, insert, 0)

    for piece in range(2):
        def finish(g, carry):
            put(piece, g, 0).wait()
            put(piece, g, 1).wait()
            return carry

        lax.fori_loop(0, pieces[piece][4], finish, 0)
    hidden.wait()


HBM = pl.BlockSpec(memory_space=pltpu.HBM)
VM = pl.BlockSpec(memory_space=pltpu.VMEM)


def in_hbm(*arrays):
    return [pltpu.with_memory_space_constraint(array, pltpu.HBM) for array in arrays]


def self_call(layer, positions, hidden, w, keys, vals):
    cache = jax.ShapeDtypeStruct(keys.shape, BF16)
    args = [positions, hidden, w['ln_gain'], w['ln_bias'], w['w_query'], w['b_query'], w['w_key'], w['w_value'], w['b_value'], keys, vals]
    return pl.pallas_call(
        functools.partial(self_kernel, layer),
        out_shape=(jax.ShapeDtypeStruct((QUART, LANES), BF16), cache, cache),
        in_specs=[HBM] * len(args),
        out_specs=(HBM, HBM, HBM),
        scratch_shapes=[
            pltpu.VMEM((QUART, LANES), BF16),
            pltpu.VMEM((HALF, HD, CTX), BF16),
            pltpu.VMEM((HALF, HD, CTX), BF16),
            pltpu.SMEM((BATCH,), jnp.int32),
            pltpu.VMEM((HALF, D), BF16),
            pltpu.VMEM((3, 2, D), BF16),
            pltpu.VMEM((3, 2, D), BF16),
            pltpu.VMEM((HD, D), BF16),
            pltpu.VMEM((2, HD), BF16),
            pltpu.VMEM((HD, D), BF16),
            pltpu.VMEM((HD, D), BF16),
            pltpu.VMEM((2, HD), BF16),
            pltpu.VMEM((HALF, 2 * HD), F32),
            pltpu.VMEM((HALF, D), F32),
            pltpu.VMEM((GROUPS, HD, GB), F32),
            pltpu.VMEM((GROUPS, HD, GB), F32),
            pltpu.VMEM((HALF, HD), F32),
            pltpu.SemaphoreType.DMA((9,)),
            pltpu.SemaphoreType.DMA((2, GROUPS)),
            pltpu.SemaphoreType.DMA((2, GROUPS)),
        ],
        compiler_params=pltpu.CompilerParams(vmem_limit_bytes=VMEM_LIMIT),
        cost_estimate=pl.CostEstimate(flops=10 ** 10, bytes_accessed=21 * 2 ** 20, transcendentals=HALF * CTX),
        name=f'self_attention_{layer}',
    )(*in_hbm(*args))


def tail_call(positions, hidden, heads, w, wo, cross_k, cross_v, keys, vals):
    args = [hidden, heads, positions, w['ln_gain'], w['ln_bias'], w['w_query'], w['b_query'], w['w_key'], w['w_value'], w['b_value'], *wo, w['b_out'],
            w['w_cquery'], w['b_cquery'], w['w_cout'], w['b_cout'], w['w_fc1'], w['b_fc1'], w['w_fc2'], w['b_fc2'], cross_k, cross_v, keys, vals]
    new = jax.ShapeDtypeStruct((3, HALF, HD), BF16)
    half = jax.ShapeDtypeStruct((HALF, HD, CTX), BF16)
    cache = jax.ShapeDtypeStruct((BATCH, HD, CTX), BF16)
    pair = (2, TP, QUART, LANES)
    return pl.pallas_call(
        tail_kernel,
        out_shape=(jax.ShapeDtypeStruct((BATCH, D), BF16), new, new, half, half, cache, cache),
        in_specs=[HBM] * len(args),
        out_specs=(VM,) * 7,
        scratch_shapes=[
            pltpu.VMEM((BATCH, D), BF16),
            pltpu.VMEM((QUART, LANES), BF16),
            pltpu.SMEM((BATCH,), jnp.int32),
            pltpu.VMEM((3, 2, D), BF16),
            pltpu.VMEM((3, 2, D), BF16),
            pltpu.VMEM((2, HD, D), BF16),
            pltpu.VMEM((2, HD), BF16),
            pltpu.VMEM((2, HD, D), BF16),
            pltpu.VMEM((2, HD, D), BF16),
            pltpu.VMEM((2, HD), BF16),
            pltpu.VMEM((2, D), BF16),
            pltpu.VMEM((2, HD, D), BF16),
            pltpu.VMEM((2, HD), BF16),
            pltpu.VMEM((2, D), BF16),
            pltpu.VMEM((2, D, 256), BF16),
            pltpu.VMEM((2, 256), BF16),
            pltpu.VMEM((2, 256, D), BF16),
            pltpu.VMEM((2, D), BF16),
            pltpu.VMEM((AUD, HD, FRAMES), BF16),
            pltpu.VMEM((AUD, HD, FRAMES), BF16),
            pltpu.VMEM((TP, 2, HD, D), BF16),
            pltpu.VMEM((TP, 2, HD, D), BF16),
            pltpu.VMEM((4,) + pair, BF16),
            pltpu.VMEM((3, QUART, LANES), BF16),
            pltpu.VMEM((2, 2, QUART, LANES), BF16),
            pltpu.VMEM((BATCH // 2, 2 * HD), F32),
            pltpu.VMEM((2, BATCH // 2, HD), F32),
            pltpu.VMEM((BATCH // 2, HD), F32),
            pltpu.VMEM((2, BATCH // 2, D), F32),
            pltpu.VMEM((2,) + pair, BF16),
            pltpu.VMEM((2,) + pair, BF16),
            pltpu.VMEM((2, BATCH // 2, D), F32),
            pltpu.VMEM((2, 2, QUART, LANES), BF16),
            pltpu.VMEM((2,) + pair, BF16),
            pltpu.SemaphoreType.DMA((18,)),
            pltpu.SemaphoreType.DMA((5,)),
            pltpu.SemaphoreType.DMA((2, 2, AGROUPS)),
            pltpu.SemaphoreType.DMA((2, 2)),
            pltpu.SemaphoreType.DMA((2, 2)),
            pltpu.SemaphoreType.DMA((3, 4)),
            pltpu.SemaphoreType.DMA((3, 4)),
            pltpu.SemaphoreType.DMA((16, TP)),
            pltpu.SemaphoreType.DMA((16, TP)),
        ],
        compiler_params=pltpu.CompilerParams(vmem_limit_bytes=TAIL_LIMIT, collective_id=0, has_side_effects=True),
        cost_estimate=pl.CostEstimate(flops=10 ** 10, bytes_accessed=46 * 2 ** 20, transcendentals=2 * BATCH * FRAMES),
        name='cross_mlp_and_next_layer',
    )(*in_hbm(*args))


def write_call(positions, hidden, knew, vnew, held, prev):
    shapes = [jax.ShapeDtypeStruct(x.shape, BF16) for x in (hidden, *prev, *held)]
    return pl.pallas_call(
        write_kernel,
        out_shape=tuple(shapes),
        in_specs=[HBM] + [VM] * 7 + [HBM, HBM],
        out_specs=(HBM, HBM, HBM, VM, VM, VM, VM),
        input_output_aliases={4: 3, 5: 4, 6: 5, 7: 6, 8: 1, 9: 2},
        scratch_shapes=[
            pltpu.SMEM((BATCH,), jnp.int32),
            pltpu.VMEM((2, 3 * HALF, HD), F32),
            pltpu.SemaphoreType.DMA((2,)),
            pltpu.SemaphoreType.DMA((2, 2, 2 * GROUPS)),
        ],
        compiler_params=pltpu.CompilerParams(vmem_limit_bytes=WRITE_LIMIT),
        cost_estimate=pl.CostEstimate(flops=10 ** 8, bytes_accessed=32 * 2 ** 20, transcendentals=0),
        name='write_caches',
    )(*in_hbm(positions), hidden, knew, vnew, *held, *in_hbm(*prev))


def solution(mesh):
    cache_spec = P(None, 'dp', None, 'tp', None)
    col_spec = P(None, None, 'tp')
    row_spec = P(None, 'tp', None)
    vec_spec = P(None, 'tp')
    param_specs = {'ln_gain': P(), 'ln_bias': P(), 'w_query': col_spec, 'b_query': vec_spec, 'w_key': col_spec, 'w_value': col_spec, 'b_value': vec_spec, 'w_out': row_spec, 'b_out': P(), 'w_cquery': col_spec, 'b_cquery': vec_spec, 'w_cout': row_spec, 'b_cout': P(), 'w_fc1': col_spec, 'b_fc1': vec_spec, 'w_fc2': row_spec, 'b_fc2': P()}
    in_specs = (P('dp', None), P('dp'), cache_spec, cache_spec, cache_spec, cache_spec) + tuple(param_specs[param_name] for param_name in PARAM_NAMES)

    def lanes_last(cache):
        return jnp.transpose(cache, (0, 1, 3, 4, 2)).reshape(cache.shape[0], cache.shape[1], cache.shape[4], cache.shape[2])

    def slots_back(cache):
        layers, beams, width, slots = cache.shape
        return jnp.transpose(cache.reshape(layers, beams, 1, width, slots), (0, 1, 4, 2, 3))

    def local_step(hidden, positions, self_keys, self_vals, cross_keys, cross_vals, *layer_params):
        w = dict(zip(PARAM_NAMES, layer_params))
        for name in ('w_query', 'w_key', 'w_value', 'w_cquery'):
            w[name] = jnp.transpose(w[name], (0, 2, 1))
        for name in ('ln_gain', 'ln_bias'):
            w[name] = jnp.transpose(w[name], (1, 0, 2))
        keys, vals, cross_k, cross_v = (lanes_last(c) for c in (self_keys, self_vals, cross_keys, cross_vals))
        wo = [w['w_out']] + [lax.ppermute(w['w_out'], 'tp', [(i, i ^ flip) for i in range(TP)]) for flip in (2, 4, 6)]
        heads, *prev = self_call(0, positions, hidden, w, keys, vals)
        hidden, knew, vnew, *held = tail_call(positions, hidden, heads, w, wo, cross_k, cross_v, keys, vals)
        hidden, new_keys, new_vals = write_call(positions, hidden, knew, vnew, held, prev)[:3]
        return hidden, slots_back(new_keys), slots_back(new_vals)

    return jax.shard_map(local_step, mesh=mesh, in_specs=in_specs, out_specs=(P('dp', None), cache_spec, cache_spec), check_vma=False)
```

```python
import functools

import jax
import jax.numpy as jnp
from jax import lax
from jax.experimental import pallas as pl
from jax.experimental.pallas import tpu as pltpu
from jax.sharding import PartitionSpec as P

EPS = 1e-5
F32 = jnp.float32
BF16 = jnp.bfloat16
NT = (((1,), (1,)), ((), ()))
MESH = pl.DeviceIdType.MESH
PARAM_NAMES = ('ln_gain', 'ln_bias', 'w_query', 'b_query', 'w_key', 'w_value', 'b_value', 'w_out', 'b_out', 'w_cquery', 'b_cquery', 'w_cout', 'b_cout', 'w_fc1', 'b_fc1', 'w_fc2', 'b_fc2')

BATCH = 160
AUD = 32
BEAMS = 5
HD = 64
CTX = 448
FRAMES = 1500
D = 512
TP = 8
SCALE = HD ** -0.25
GB = 8
GROUPS = BATCH // GB
VMEM_LIMIT = 67_000_000
TAIL_LIMIT = 30 * 2 ** 20
WRITE_LIMIT = 12 * 2 ** 20
SELF_UNROLL = 5
UNROLL = 4
GA = 8
AGROUPS = AUD // GA
GR = GA * BEAMS
HALF = BATCH // 2
QUART = BATCH // 4
HALVES = range(2)
LANES = 128


def layer_norm(wide, gain, bias):
    center = wide - jnp.mean(wide, axis=-1, keepdims=True)
    var_est = jnp.mean(center * center, axis=-1, keepdims=True)
    return (center * lax.rsqrt(var_est + EPS) * gain + bias).astype(BF16)


def row_of(ref, *idx):
    return ref[idx].astype(F32)


def dot_nt(a, b):
    return lax.dot_general(a, b, NT, preferred_element_type=F32)


def dot(a, b):
    return jnp.dot(a, b, preferred_element_type=F32)


def fold_heads(wide, keep):
    wide = jnp.where(keep, wide, 0.0)
    part = (wide[:, 0:LANES] + wide[:, LANES:256]) + (wide[:, 256:384] + wide[:, 384:512])
    return part[:, :HD] + part[:, HD:]


def insert_columns(g, pos_ref, pairs):
    lane128 = lax.broadcasted_iota(jnp.int32, (HD, LANES), 1)
    lane64 = lax.broadcasted_iota(jnp.int32, (HD, HD), 1) + 384
    row_id = lax.broadcasted_iota(jnp.int32, (GB, 1), 0)
    pos_col = jnp.zeros((GB, 1), jnp.int32)
    for j in range(GB):
        beam = g * GB + j
        pos = pos_ref[beam]
        pos_col = jnp.where(row_id == j, pos, pos_col)
        off = pl.multiple_of(jnp.minimum(pos // LANES, 2) * LANES, LANES)
        for buf, cols in pairs:
            col = jnp.broadcast_to(cols[:, j:j + 1], (HD, LANES)).astype(BF16)
            view = buf.at[beam, :, pl.ds(off, LANES)]
            view[...] = jnp.where(lane128 + off == pos, col, view[...])
            tail = buf.at[beam, :, pl.ds(384, 64)]
            tail[...] = jnp.where(lane64 == pos, col[:, :HD], tail[...])
    return pos_col


def self_kernel(layer, pos_in, h_in, gain_in, bias_in, wq_in, bq_in, wk_in, wv_in, bv_in, kin, vin, *rest):
    (o_out, kout, vout, o_ref, kbuf, vbuf, pos_ref, h_ref, gain_ref, bias_ref, wq_ref, bq_ref, wk_ref, wv_ref, bv_ref,
     q_scr, a_scr, kt_scr, vt_scr, o_scr, par_sem, in_sem, out_sem) = rest

    def rows(g):
        return pl.ds(pl.multiple_of(g * GB, GB), GB)

    def fetch(g, which):
        src, buf = ((kin, kbuf), (vin, vbuf))[which]
        return pltpu.make_async_copy(src.at[layer, rows(g)], buf.at[rows(g)], in_sem.at[which, g])

    def put(g, which):
        buf, dst = ((kbuf, kout), (vbuf, vout))[which]
        return pltpu.make_async_copy(buf.at[rows(g)], dst.at[layer, rows(g)], out_sem.at[which, g])

    params = [(pos_in, pos_ref), (gain_in, gain_ref), (bias_in, bias_ref), (bq_in, bq_ref), (bv_in, bv_ref),
              (wq_in.at[layer], wq_ref), (wk_in.at[layer], wk_ref), (wv_in.at[layer], wv_ref)]
    params.append((h_in, h_ref))
    copies = [pltpu.make_async_copy(src, dst, par_sem.at[i]) for i, (src, dst) in enumerate(params)]
    for copy in copies:
        copy.start()

    def start_fetch(g, carry):
        fetch(g, 0).start()
        fetch(g, 1).start()
        return carry

    lax.fori_loop(0, GROUPS, start_fetch, 0)
    for copy in copies:
        copy.wait()

    normed = layer_norm(h_ref[...].astype(F32), row_of(gain_ref, 0, pl.ds(layer, 1)), row_of(bias_ref, 0, pl.ds(layer, 1)))
    query = ((dot_nt(normed, wq_ref[...]) + row_of(bq_ref, pl.ds(layer, 1))) * SCALE).astype(BF16).astype(F32)
    q_scr[...] = jnp.concatenate([query, query], axis=1)
    a_scr[...] = normed.astype(F32)
    eye = lax.broadcasted_iota(jnp.int32, (HD, HD), 0) == lax.broadcasted_iota(jnp.int32, (HD, HD), 1)
    bv_col = jnp.sum(jnp.where(eye, row_of(bv_ref, pl.ds(layer, 1)), 0.0), axis=1, keepdims=True)

    def project(g, carry):
        part = a_scr[rows(g)].astype(BF16)
        kt_scr[g] = dot_nt(wk_ref[...], part) * SCALE
        vt_scr[g] = dot_nt(wv_ref[...], part) + bv_col
        return carry

    lax.fori_loop(0, GROUPS, project, 0, unroll=4)

    lane_ctx = lax.broadcasted_iota(jnp.int32, (GB, CTX), 1)
    keep = lax.broadcasted_iota(jnp.int32, (GB, D), 1) // HD == lax.broadcasted_iota(jnp.int32, (GB, D), 0)

    def attend(step, carry):
        groups = [step * UNROLL + u for u in range(UNROLL)]
        pos_cols, scores, probs = [], [], []
        for g in groups:
            fetch(g, 0).wait()
            fetch(g, 1).wait()
        for g in groups:
            pos_cols.append(insert_columns(g, pos_ref, ((kbuf, kt_scr[g]), (vbuf, vt_scr[g]))))
        for g, pos_col in zip(groups, pos_cols):
            q8 = q_scr[rows(g)]
            qblk = jnp.where(keep, jnp.concatenate([q8, q8, q8, q8], axis=1), 0.0).astype(BF16)
            scores.append(jnp.where(lane_ctx <= pos_col, dot(qblk, kbuf[rows(g)].reshape(GB * HD, CTX)), -1e30))
        for score in scores:
            expd = jnp.exp(score - jnp.max(score, axis=1, keepdims=True))
            probs.append((expd / jnp.sum(expd, axis=1, keepdims=True)).astype(BF16))
        wides = [dot_nt(prob, vbuf[rows(g)].reshape(GB * HD, CTX)) for g, prob in zip(groups, probs)]
        for g, wide in zip(groups, wides):
            o_scr[rows(g)] = fold_heads(wide, keep)
            put(g, 0).start()
            put(g, 1).start()
        return carry

    lax.fori_loop(0, GROUPS // UNROLL, attend, 0)
    for half in HALVES:
        o_ref[half] = jnp.concatenate([o_scr[HALF * half:HALF * half + QUART], o_scr[HALF * half + QUART:HALF * half + HALF]], axis=1).astype(BF16)
    heads_copy = pltpu.make_async_copy(o_ref, o_out, par_sem.at[0])
    heads_copy.start()

    def finish(g, carry):
        put(g, 0).wait()
        put(g, 1).wait()
        return carry

    lax.fori_loop(0, GROUPS, finish, 0)
    heads_copy.wait()


def erf_gelu(x):
    return 0.5 * x * (1.0 + lax.erf(x * (2.0 ** -0.5)))


def tail_kernel(h_in, o_in, pos_in, gain_in, bias_in, wq_in, bq_in, wk_in, wv_in, bv_in, wo0, wo2, wo4, wo6, bo_in, wcq_in, bcq_in, wco_in, bco_in,
                w1_in, b1_in, w2_in, b2_in, ckin, cvin, skin, svin,
                out_ref, knew_ref, vnew_ref, sk, sv,
                h_ref, o_ref, pos_ref, gain_ref, bias_ref, wq_ref, bq_ref, wk_ref, wv_ref, bv_ref, bo_ref, wcq_ref, bcq_ref, bco_ref,
                w1_ref, b1_ref, w2_ref, b2_ref,
                kbuf, vbuf, wofull, wcofull, obuf, osend, q_scr, kv_scr, o_scr, hid_scr, pbuf, rbuf, base_scr, hblk, hslots,
                par_sem, wpar_sem, ck_sem, sk_sem, wsend, wrecv, send_sem, recv_sem):
    me = lax.axis_index('tp')
    core = lax.rem(me, 2)
    chip_x = lax.rem(lax.div(me, 2), 2)
    sibling = me + 1 - 2 * core
    flip_x = 2 - 4 * chip_x
    across = lax.rem(me + 4, TP)
    holders = [me, me + flip_x, across, across + flip_x]
    far = [holders[3], holders[1], holders[2]]
    peers = far[:1] + [p + 1 - 2 * core for p in far[:1]] + far[1:] + [p + 1 - 2 * core for p in far[1:]] + [sibling]

    def fetch_cross(layer, g, which):
        src, buf = ((ckin, kbuf), (cvin, vbuf))[which]
        return pltpu.make_async_copy(src.at[layer, pl.ds(GA * g, GA)], buf.at[pl.ds(GA * g, GA)], ck_sem.at[layer, which, g])

    def fetch_self(half, which):
        src, buf = ((skin, sk), (svin, sv))[which]
        return pltpu.make_async_copy(src.at[1, pl.ds(HALF * half, HALF)], buf.at[pl.ds(HALF * half, HALF)], sk_sem.at[which, half])

    params = [(o_in, o_ref), (h_in, h_ref), (gain_in, gain_ref), (bias_in, bias_ref), (bo_in, bo_ref), (wcq_in, wcq_ref), (bcq_in, bcq_ref),
              (bco_in, bco_ref), (w1_in, w1_ref), (b1_in, b1_ref), (w2_in, w2_ref), (b2_in, b2_ref), (pos_in, pos_ref), (wq_in.at[1], wq_ref),
              (bq_in, bq_ref), (wk_in.at[1], wk_ref), (wv_in.at[1], wv_ref), (bv_in, bv_ref)]
    copies = [pltpu.make_async_copy(src, dst, par_sem.at[i]) for i, (src, dst) in enumerate(params)]
    wo_src = (wo0, wo2, wo4, wo6)
    own = [pltpu.make_async_copy(wo_src[k], wofull.at[holders[k]], wpar_sem.at[k]) for k in range(4)]
    own.append(pltpu.make_async_copy(wco_in, wcofull.at[me], wpar_sem.at[4]))

    barrier = pltpu.get_barrier_semaphore()
    for peer in peers:
        pl.semaphore_signal(barrier, inc=1, device_id={'tp': peer}, device_id_type=MESH)
    for copy in copies + own:
        copy.start()
    for g in range(AGROUPS):
        fetch_cross(0, g, 0).start()
        fetch_cross(0, g, 1).start()
    for half in HALVES:
        fetch_self(half, 0).start()
        fetch_self(half, 1).start()
    copies[0].wait()
    pl.semaphore_wait(barrier, TP - 1)

    def send(phase, src, dst, peer):
        return pltpu.make_async_remote_copy(src_ref=src, dst_ref=dst, send_sem=send_sem.at[phase, peer], recv_sem=recv_sem.at[phase, me],
                                            device_id={'tp': peer}, device_id_type=MESH)

    def arrival(phase, dst, peer):
        return pltpu.make_async_remote_copy(src_ref=dst, dst_ref=dst, send_sem=send_sem.at[phase, peer], recv_sem=recv_sem.at[phase, peer],
                                            device_id={'tp': peer}, device_id_type=MESH)

    def gather_start(phase, src, slots):
        for peer in peers:
            send(phase, src, slots.at[me], peer).start()

    def gather_wait(phase, src, slots):
        for peer in peers:
            arrival(phase, slots.at[peer], peer).wait_recv()
        for peer in peers:
            send(phase, src, slots.at[me], peer).wait_send()

    def weight_copy(row, k, src, dst, target):
        return pltpu.make_async_remote_copy(src_ref=src, dst_ref=dst, send_sem=wsend.at[row, k], recv_sem=wrecv.at[row, k],
                                            device_id={'tp': target}, device_id_type=MESH)

    wo_fwd = [weight_copy(0, k, wo_src[k], wofull.at[holders[k]], sibling) for k in range(4)]

    def wco_out(layer, k, slot):
        return weight_copy(1 + layer, k, wco_in.at[layer], wcofull.at[slot, layer], holders[k])

    def wco_fwd(layer, k, slot):
        src = wcofull.at[holders[k], layer] if k else wco_in.at[layer]
        return weight_copy(3 + layer, k, src, wcofull.at[slot, layer], sibling)

    def wco_send(layer):
        for k in (3, 1, 2):
            wco_out(layer, k, me).start()
        wco_fwd(layer, 0, me).start()

    def wco_forward(layer):
        for k in (1, 2, 3):
            wco_out(layer, k, holders[k]).wait_recv()
            wco_fwd(layer, k, holders[k]).start()

    def wco_settle(layer):
        for k in range(4):
            wco_fwd(layer, k, holders[k] + 1 - 2 * core).wait_recv()
            wco_fwd(layer, k, holders[k]).wait_send()
        for k in (1, 2, 3):
            wco_out(layer, k, me).wait_send()

    for half in HALVES:
        gather_start(half, o_ref.at[half], obuf.at[0, half])
    for copy in wo_fwd:
        copy.start()
    wco_send(0)
    for half in HALVES:
        obuf[0, half, me] = o_ref[half]
    for copy in copies[1:] + own:
        copy.wait()

    low = lax.broadcasted_iota(jnp.int32, (QUART, LANES), 1) < HD

    def head_rows(stage, half):
        top, bottom = [], []
        for pair in range(TP // 2):
            left = obuf[stage, half, 2 * pair].astype(F32)
            right = obuf[stage, half, 2 * pair + 1].astype(F32)
            top.append(jnp.where(low, left, pltpu.roll(right, HD, 1)))
            bottom.append(jnp.where(low, pltpu.roll(left, HD, 1), right))
        return jnp.concatenate([jnp.concatenate(top, axis=1), jnp.concatenate(bottom, axis=1)], axis=0).astype(BF16)

    def norm_of(hid, layer, k):
        return layer_norm(hid, row_of(gain_ref, k, pl.ds(layer, 1)), row_of(bias_ref, k, pl.ds(layer, 1)))

    keep = lax.broadcasted_iota(jnp.int32, (GR, D), 1) // HD == lax.broadcasted_iota(jnp.int32, (GR, D), 0) // BEAMS

    def gathered_out(stage, half, full, layer, bias):
        return dot(head_rows(stage, half), full[:, layer].reshape(D, D)) + row_of(bias, pl.ds(layer, 1))

    def cross_half(layer, half, hid):
        stage = 2 * layer
        hid = hid + gathered_out(stage, half, wofull, layer, bo_ref)
        hid = hid.astype(BF16).astype(F32)
        hid_scr[half] = hid
        query = ((dot_nt(norm_of(hid, layer, 1), wcq_ref[layer]) + row_of(bcq_ref, pl.ds(layer, 1))) * SCALE).astype(BF16).astype(F32)
        q_scr[...] = jnp.concatenate([query, query], axis=1)
        groups = (2 * half, 2 * half + 1)
        for g in groups:
            fetch_cross(layer, g, 0).wait()
            fetch_cross(layer, g, 1).wait()
        scores, probs = [], []
        for i, g in enumerate(groups):
            q40 = q_scr[GR * i:GR * i + GR]
            qblk = jnp.where(keep, jnp.concatenate([q40, q40, q40, q40], axis=1), 0.0).astype(BF16)
            scores.append(dot(qblk, kbuf[GA * g:GA * g + GA].reshape(GA * HD, FRAMES)))
        for score in scores:
            expd = jnp.exp(score - jnp.max(score, axis=1, keepdims=True))
            probs.append((expd / jnp.sum(expd, axis=1, keepdims=True)).astype(BF16))
        outs = [fold_heads(dot_nt(prob, vbuf[GA * g:GA * g + GA].reshape(GA * HD, FRAMES)), keep) for g, prob in zip(groups, probs)]
        osend[stage, half] = jnp.concatenate(outs, axis=1).astype(BF16)
        gather_start(8 * layer + 2 + half, osend.at[stage, half], obuf.at[stage + 1, half])
        obuf[stage + 1, half, me] = osend[stage, half]

    def mlp_half(layer, half):
        stage = 2 * layer
        gather_wait(8 * layer + 2 + half, osend.at[stage, half], obuf.at[stage + 1, half])
        hid = hid_scr[half] + gathered_out(stage + 1, half, wcofull, layer, bco_ref)
        hid = hid.astype(BF16).astype(F32)
        inner = erf_gelu(dot(norm_of(hid, layer, 2), w1_ref[layer]) + row_of(b1_ref, pl.ds(layer, 1))).astype(BF16)
        part = dot(inner, w2_ref[layer]).astype(BF16)
        for t in range(TP):
            pbuf[layer, half, t] = part[QUART * (t % 2):QUART * (t % 2) + QUART, LANES * (t // 2):LANES * (t // 2) + LANES]
        for peer in peers:
            send(8 * layer + 4 + half, pbuf.at[layer, half, peer], rbuf.at[layer, half, me], peer).start()
        rbuf[layer, half, me] = pbuf[layer, half, me]
        base_scr[half] = hid + row_of(b2_ref, pl.ds(layer, 1))

    def reduce_half(layer, half):
        for peer in peers:
            arrival(8 * layer + 4 + half, rbuf.at[layer, half, peer], peer).wait_recv()
        total = rbuf[layer, half, 0].astype(F32)
        for t in range(1, TP):
            total = total + rbuf[layer, half, t].astype(F32)
        mine = base_scr[half, pl.ds(pl.multiple_of(QUART * core, 8), QUART), pl.ds(pl.multiple_of(LANES * lax.div(me, 2), LANES), LANES)]
        hblk[layer, half] = (mine + total).astype(BF16)
        gather_start(8 * layer + 6 + half, hblk.at[layer, half], hslots.at[layer, half])
        hslots[layer, half, me] = hblk[layer, half]

    def next_hidden(layer, half):
        gather_wait(8 * layer + 6 + half, hblk.at[layer, half], hslots.at[layer, half])
        for peer in peers:
            send(8 * layer + 4 + half, pbuf.at[layer, half, peer], rbuf.at[layer, half, me], peer).wait_send()
        cols = [jnp.concatenate([hslots[layer, half, 2 * c].astype(F32), hslots[layer, half, 2 * c + 1].astype(F32)], axis=0) for c in range(TP // 2)]
        return jnp.concatenate(cols, axis=1)

    lane_ctx = lax.broadcasted_iota(jnp.int32, (GB, CTX), 1)
    row_id = lax.broadcasted_iota(jnp.int32, (GB, 1), 0)
    keep8 = lax.broadcasted_iota(jnp.int32, (GB, D), 1) // HD == lax.broadcasted_iota(jnp.int32, (GB, D), 0)

    def self_half(half, hid):
        hid_scr[half] = hid
        normed = norm_of(hid, 1, 0)
        query = ((dot_nt(normed, wq_ref[...]) + row_of(bq_ref, pl.ds(1, 1))) * SCALE).astype(BF16)
        key = (dot_nt(normed, wk_ref[...]) * SCALE).astype(BF16)
        val = (dot_nt(normed, wv_ref[...]) + row_of(bv_ref, pl.ds(1, 1))).astype(BF16)
        knew_ref[half] = key
        vnew_ref[half] = val
        query = query.astype(F32)
        q_scr[...] = jnp.concatenate([query, query], axis=1)
        kv_scr[0] = jnp.broadcast_to(jnp.sum(query * key.astype(F32), axis=1, keepdims=True), (HALF, HD))
        kv_scr[1] = val.astype(F32)
        fetch_self(half, 0).wait()
        fetch_self(half, 1).wait()

        def attend(step, carry):
            local = [step * SELF_UNROLL + u for u in range(SELF_UNROLL)]
            rows = [pl.ds(pl.multiple_of(g * GB, GB), GB) for g in local]
            slabs = [pl.ds(pl.multiple_of(HALF * half + g * GB, GB), GB) for g in local]
            scores, hits, probs, wides = [], [], [], []
            for g, row, slab in zip(local, rows, slabs):
                pos_col = jnp.zeros((GB, 1), jnp.int32)
                for j in range(GB):
                    pos_col = jnp.where(row_id == j, pos_ref[HALF * half + g * GB + j], pos_col)
                q8 = q_scr[row]
                qblk = jnp.where(keep8, jnp.concatenate([q8, q8, q8, q8], axis=1), 0.0).astype(BF16)
                score = dot(qblk, sk[slab].reshape(GB * HD, CTX))
                hit = lane_ctx == pos_col
                score = jnp.where(hit, kv_scr[0, row][:, :1], score)
                scores.append(jnp.where(lane_ctx <= pos_col, score, -1e30))
                hits.append(hit)
            for score in scores:
                expd = jnp.exp(score - jnp.max(score, axis=1, keepdims=True))
                probs.append((expd / jnp.sum(expd, axis=1, keepdims=True)).astype(BF16).astype(F32))
            for slab, prob, hit in zip(slabs, probs, hits):
                wides.append(dot_nt(jnp.where(hit, 0.0, prob).astype(BF16), sv[slab].reshape(GB * HD, CTX)))
            for row, wide, prob, hit in zip(rows, wides, probs, hits):
                fresh = jnp.sum(jnp.where(hit, prob, 0.0), axis=1, keepdims=True) * kv_scr[1, row]
                o_scr[row] = fold_heads(wide, keep8) + fresh
            return carry

        lax.fori_loop(0, 10 // SELF_UNROLL, attend, 0)
        osend[1, half] = jnp.concatenate([o_scr[0:QUART], o_scr[QUART:HALF]], axis=1).astype(BF16)
        gather_start(8 + half, osend.at[1, half], obuf.at[2, half])
        obuf[2, half, me] = osend[1, half]

    for half in HALVES:
        gather_wait(half, o_ref.at[half], obuf.at[0, half])
        if half == 0:
            for copy in wo_fwd:
                copy.wait()
        cross_half(0, half, h_ref[HALF * half:HALF * half + HALF].astype(F32))
        if half == 0:
            wco_forward(0)
    wco_settle(0)
    for g in range(AGROUPS):
        fetch_cross(1, g, 0).start()
        fetch_cross(1, g, 1).start()
    for half in HALVES:
        mlp_half(0, half)
    for half in HALVES:
        reduce_half(0, half)
    for half in HALVES:
        hid = next_hidden(0, half)
        if half == 0:
            wco_send(1)
        self_half(half, hid)
    wco_forward(1)
    for half in HALVES:
        gather_wait(8 + half, osend.at[1, half], obuf.at[2, half])
        cross_half(1, half, hid_scr[half])
    wco_settle(1)
    for half in HALVES:
        mlp_half(1, half)
    for half in HALVES:
        reduce_half(1, half)
    for half in HALVES:
        out_ref[HALF * half:HALF * half + HALF] = next_hidden(1, half).astype(BF16)


def write_kernel(pos_in, h_ref, knew_ref, vnew_ref, sk_in, sv_in, kprev, vprev, h_out, kout, vout, sk, sv, pos_ref, new_scr, sem, out_sem):
    load = pltpu.make_async_copy(pos_in, pos_ref, sem.at[0])
    load.start()
    hidden = pltpu.make_async_copy(h_ref, h_out, sem.at[1])
    hidden.start()
    for half in HALVES:
        new_scr[0, HALF * half:HALF * half + HALF] = knew_ref[half].astype(F32)
        new_scr[1, HALF * half:HALF * half + HALF] = vnew_ref[half].astype(F32)
    eye = (lax.broadcasted_iota(jnp.int32, (HD, HD), 0) == lax.broadcasted_iota(jnp.int32, (HD, HD), 1)).astype(BF16)
    load.wait()

    def rows(g):
        return pl.ds(pl.multiple_of(g * GB, GB), GB)

    def put(g, which):
        buf, dst = ((sk, kout), (sv, vout))[which]
        return pltpu.make_async_copy(buf.at[rows(g)], dst.at[1, rows(g)], out_sem.at[which, g])

    def insert(step, carry):
        groups = [step * 2 + u for u in HALVES]
        cols = [[dot_nt(eye, new_scr[which, rows(g)].astype(BF16)) for which in HALVES] for g in groups]
        for g, pair in zip(groups, cols):
            insert_columns(g, pos_ref, ((sk, pair[0]), (sv, pair[1])))
        for g in groups:
            put(g, 0).start()
            put(g, 1).start()
        return carry

    lax.fori_loop(0, GROUPS // 2, insert, 0)

    def finish(g, carry):
        put(g, 0).wait()
        put(g, 1).wait()
        return carry

    lax.fori_loop(0, GROUPS, finish, 0)
    hidden.wait()


HBM = pl.BlockSpec(memory_space=pltpu.HBM)
VM = pl.BlockSpec(memory_space=pltpu.VMEM)


def in_hbm(*arrays):
    return [pltpu.with_memory_space_constraint(array, pltpu.HBM) for array in arrays]


def self_call(layer, positions, hidden, w, keys, vals):
    cache = jax.ShapeDtypeStruct(keys.shape, BF16)
    args = [positions, hidden, w['ln_gain'], w['ln_bias'], w['w_query'], w['b_query'], w['w_key'], w['w_value'], w['b_value'], keys, vals]
    return pl.pallas_call(
        functools.partial(self_kernel, layer),
        out_shape=(jax.ShapeDtypeStruct((2, BATCH // 4, 2 * HD), BF16), cache, cache),
        in_specs=[HBM] * len(args),
        out_specs=(HBM, HBM, HBM),
        scratch_shapes=[
            pltpu.VMEM((2, BATCH // 4, 2 * HD), BF16),
            pltpu.VMEM((BATCH, HD, CTX), BF16),
            pltpu.VMEM((BATCH, HD, CTX), BF16),
            pltpu.SMEM((BATCH,), jnp.int32),
            pltpu.VMEM((BATCH, D), BF16),
            pltpu.VMEM((3, 2, D), BF16),
            pltpu.VMEM((3, 2, D), BF16),
            pltpu.VMEM((HD, D), BF16),
            pltpu.VMEM((2, HD), BF16),
            pltpu.VMEM((HD, D), BF16),
            pltpu.VMEM((HD, D), BF16),
            pltpu.VMEM((2, HD), BF16),
            pltpu.VMEM((BATCH, 2 * HD), F32),
            pltpu.VMEM((BATCH, D), F32),
            pltpu.VMEM((GROUPS, HD, GB), F32),
            pltpu.VMEM((GROUPS, HD, GB), F32),
            pltpu.VMEM((BATCH, HD), F32),
            pltpu.SemaphoreType.DMA((9,)),
            pltpu.SemaphoreType.DMA((2, GROUPS)),
            pltpu.SemaphoreType.DMA((2, GROUPS)),
        ],
        compiler_params=pltpu.CompilerParams(vmem_limit_bytes=VMEM_LIMIT),
        cost_estimate=pl.CostEstimate(flops=10 ** 10, bytes_accessed=42 * 2 ** 20, transcendentals=BATCH * CTX),
        name=f'self_attention_{layer}',
    )(*in_hbm(*args))


def tail_call(positions, hidden, heads, w, wo, cross_k, cross_v, keys, vals):
    args = [hidden, heads, positions, w['ln_gain'], w['ln_bias'], w['w_query'], w['b_query'], w['w_key'], w['w_value'], w['b_value'], *wo, w['b_out'],
            w['w_cquery'], w['b_cquery'], w['w_cout'], w['b_cout'], w['w_fc1'], w['b_fc1'], w['w_fc2'], w['b_fc2'], cross_k, cross_v, keys, vals]
    new = jax.ShapeDtypeStruct((2, BATCH // 2, HD), BF16)
    cache = jax.ShapeDtypeStruct((BATCH, HD, CTX), BF16)
    pair = (2, TP, QUART, LANES)
    return pl.pallas_call(
        tail_kernel,
        out_shape=(jax.ShapeDtypeStruct((BATCH, D), BF16), new, new, cache, cache),
        in_specs=[HBM] * len(args),
        out_specs=(VM,) * 5,
        scratch_shapes=[
            pltpu.VMEM((BATCH, D), BF16),
            pltpu.VMEM((2, BATCH // 4, 2 * HD), BF16),
            pltpu.SMEM((BATCH,), jnp.int32),
            pltpu.VMEM((3, 2, D), BF16),
            pltpu.VMEM((3, 2, D), BF16),
            pltpu.VMEM((HD, D), BF16),
            pltpu.VMEM((2, HD), BF16),
            pltpu.VMEM((HD, D), BF16),
            pltpu.VMEM((HD, D), BF16),
            pltpu.VMEM((2, HD), BF16),
            pltpu.VMEM((2, D), BF16),
            pltpu.VMEM((2, HD, D), BF16),
            pltpu.VMEM((2, HD), BF16),
            pltpu.VMEM((2, D), BF16),
            pltpu.VMEM((2, D, 256), BF16),
            pltpu.VMEM((2, 256), BF16),
            pltpu.VMEM((2, 256, D), BF16),
            pltpu.VMEM((2, D), BF16),
            pltpu.VMEM((AUD, HD, FRAMES), BF16),
            pltpu.VMEM((AUD, HD, FRAMES), BF16),
            pltpu.VMEM((TP, 2, HD, D), BF16),
            pltpu.VMEM((TP, 2, HD, D), BF16),
            pltpu.VMEM((4,) + pair, BF16),
            pltpu.VMEM((3, 2, QUART, LANES), BF16),
            pltpu.VMEM((BATCH // 2, 2 * HD), F32),
            pltpu.VMEM((2, BATCH // 2, HD), F32),
            pltpu.VMEM((BATCH // 2, HD), F32),
            pltpu.VMEM((2, BATCH // 2, D), F32),
            pltpu.VMEM((2,) + pair, BF16),
            pltpu.VMEM((2,) + pair, BF16),
            pltpu.VMEM((2, BATCH // 2, D), F32),
            pltpu.VMEM((2, 2, QUART, LANES), BF16),
            pltpu.VMEM((2,) + pair, BF16),
            pltpu.SemaphoreType.DMA((18,)),
            pltpu.SemaphoreType.DMA((5,)),
            pltpu.SemaphoreType.DMA((2, 2, AGROUPS)),
            pltpu.SemaphoreType.DMA((2, 2)),
            pltpu.SemaphoreType.DMA((5, 4)),
            pltpu.SemaphoreType.DMA((5, 4)),
            pltpu.SemaphoreType.DMA((16, TP)),
            pltpu.SemaphoreType.DMA((16, TP)),
        ],
        compiler_params=pltpu.CompilerParams(vmem_limit_bytes=TAIL_LIMIT, collective_id=0, has_side_effects=True),
        cost_estimate=pl.CostEstimate(flops=10 ** 10, bytes_accessed=46 * 2 ** 20, transcendentals=2 * BATCH * FRAMES),
        name='cross_mlp_and_next_layer',
    )(*in_hbm(*args))


def write_call(positions, hidden, knew, vnew, sk, sv, kprev, vprev):
    held = jax.ShapeDtypeStruct(sk.shape, BF16)
    cache = jax.ShapeDtypeStruct(kprev.shape, BF16)
    return pl.pallas_call(
        write_kernel,
        out_shape=(jax.ShapeDtypeStruct(hidden.shape, BF16), cache, cache, held, held),
        in_specs=[HBM, VM, VM, VM, VM, VM, HBM, HBM],
        out_specs=(HBM, HBM, HBM, VM, VM),
        input_output_aliases={4: 3, 5: 4, 6: 1, 7: 2},
        scratch_shapes=[
            pltpu.SMEM((BATCH,), jnp.int32),
            pltpu.VMEM((2, BATCH, HD), F32),
            pltpu.SemaphoreType.DMA((2,)),
            pltpu.SemaphoreType.DMA((2, GROUPS)),
        ],
        compiler_params=pltpu.CompilerParams(vmem_limit_bytes=WRITE_LIMIT),
        cost_estimate=pl.CostEstimate(flops=10 ** 8, bytes_accessed=21 * 2 ** 20, transcendentals=0),
        name='write_caches',
    )(*in_hbm(positions), hidden, knew, vnew, sk, sv, *in_hbm(kprev, vprev))


def solution(mesh):
    cache_spec = P(None, 'dp', None, 'tp', None)
    col_spec = P(None, None, 'tp')
    row_spec = P(None, 'tp', None)
    vec_spec = P(None, 'tp')
    param_specs = {'ln_gain': P(), 'ln_bias': P(), 'w_query': col_spec, 'b_query': vec_spec, 'w_key': col_spec, 'w_value': col_spec, 'b_value': vec_spec, 'w_out': row_spec, 'b_out': P(), 'w_cquery': col_spec, 'b_cquery': vec_spec, 'w_cout': row_spec, 'b_cout': P(), 'w_fc1': col_spec, 'b_fc1': vec_spec, 'w_fc2': row_spec, 'b_fc2': P()}
    in_specs = (P('dp', None), P('dp'), cache_spec, cache_spec, cache_spec, cache_spec) + tuple(param_specs[param_name] for param_name in PARAM_NAMES)

    def lanes_last(cache):
        return jnp.transpose(cache, (0, 1, 3, 4, 2)).reshape(cache.shape[0], cache.shape[1], cache.shape[4], cache.shape[2])

    def slots_back(cache):
        layers, beams, width, slots = cache.shape
        return jnp.transpose(cache.reshape(layers, beams, 1, width, slots), (0, 1, 4, 2, 3))

    def local_step(hidden, positions, self_keys, self_vals, cross_keys, cross_vals, *layer_params):
        w = dict(zip(PARAM_NAMES, layer_params))
        for name in ('w_query', 'w_key', 'w_value', 'w_cquery'):
            w[name] = jnp.transpose(w[name], (0, 2, 1))
        for name in ('ln_gain', 'ln_bias'):
            w[name] = jnp.transpose(w[name], (1, 0, 2))
        keys, vals, cross_k, cross_v = (lanes_last(c) for c in (self_keys, self_vals, cross_keys, cross_vals))
        wo = [w['w_out']] + [lax.ppermute(w['w_out'], 'tp', [(i, i ^ flip) for i in range(TP)]) for flip in (2, 4, 6)]
        heads, *prev = self_call(0, positions, hidden, w, keys, vals)
        hidden, *held = tail_call(positions, hidden, heads, w, wo, cross_k, cross_v, keys, vals)
        hidden, *prev = write_call(positions, hidden, *held, *prev)
        return hidden, slots_back(prev[0]), slots_back(prev[1])

    return jax.shard_map(local_step, mesh=mesh, in_specs=in_specs, out_specs=(P('dp', None), cache_spec, cache_spec), check_vma=False)
```

```python
import functools

import jax
import jax.numpy as jnp
from jax import lax
from jax.experimental import pallas as pl
from jax.experimental.pallas import tpu as pltpu
from jax.sharding import PartitionSpec as P

EPS = 1e-5
F32 = jnp.float32
BF16 = jnp.bfloat16
NT = (((1,), (1,)), ((), ()))
MESH = pl.DeviceIdType.MESH
PARAM_NAMES = ('ln_gain', 'ln_bias', 'w_query', 'b_query', 'w_key', 'w_value', 'b_value', 'w_out', 'b_out', 'w_cquery', 'b_cquery', 'w_cout', 'b_cout', 'w_fc1', 'b_fc1', 'w_fc2', 'b_fc2')

BATCH = 160
AUD = 32
BEAMS = 5
HD = 64
CTX = 448
FRAMES = 1500
D = 512
TP = 8
SCALE = HD ** -0.25
GB = 8
GROUPS = BATCH // GB
VMEM_LIMIT = 67_000_000
TAIL_LIMIT = 30 * 2 ** 20
WRITE_LIMIT = 12 * 2 ** 20
SELF_UNROLL = 5
UNROLL = 4
GA = 8
AGROUPS = AUD // GA
GR = GA * BEAMS
HALF = BATCH // 2
QUART = BATCH // 4
HALVES = range(2)
LANES = 128


def layer_norm(wide, gain, bias):
    center = wide - jnp.mean(wide, axis=-1, keepdims=True)
    var_est = jnp.mean(center * center, axis=-1, keepdims=True)
    return (center * lax.rsqrt(var_est + EPS) * gain + bias).astype(BF16)


def row_of(ref, *idx):
    return ref[idx].astype(F32)


def dot_nt(a, b):
    return lax.dot_general(a, b, NT, preferred_element_type=F32)


def dot(a, b):
    return jnp.dot(a, b, preferred_element_type=F32)


def fold_heads(wide, keep):
    wide = jnp.where(keep, wide, 0.0)
    part = (wide[:, 0:LANES] + wide[:, LANES:256]) + (wide[:, 256:384] + wide[:, 384:512])
    return part[:, :HD] + part[:, HD:]


def insert_columns(g, pos_ref, pairs):
    lane128 = lax.broadcasted_iota(jnp.int32, (HD, LANES), 1)
    lane64 = lax.broadcasted_iota(jnp.int32, (HD, HD), 1) + 384
    row_id = lax.broadcasted_iota(jnp.int32, (GB, 1), 0)
    pos_col = jnp.zeros((GB, 1), jnp.int32)
    for j in range(GB):
        beam = g * GB + j
        pos = pos_ref[beam]
        pos_col = jnp.where(row_id == j, pos, pos_col)
        off = pl.multiple_of(jnp.minimum(pos // LANES, 2) * LANES, LANES)
        for buf, cols in pairs:
            col = jnp.broadcast_to(cols[:, j:j + 1], (HD, LANES)).astype(BF16)
            view = buf.at[beam, :, pl.ds(off, LANES)]
            view[...] = jnp.where(lane128 + off == pos, col, view[...])
            tail = buf.at[beam, :, pl.ds(384, 64)]
            tail[...] = jnp.where(lane64 == pos, col[:, :HD], tail[...])
    return pos_col


def self_kernel(layer, pos_in, h_in, gain_in, bias_in, wq_in, bq_in, wk_in, wv_in, bv_in, kin, vin, *rest):
    (o_out, kout, vout, o_ref, kbuf, vbuf, pos_ref, h_ref, gain_ref, bias_ref, wq_ref, bq_ref, wk_ref, wv_ref, bv_ref,
     q_scr, a_scr, kt_scr, vt_scr, o_scr, par_sem, in_sem, out_sem) = rest

    def rows(g):
        return pl.ds(pl.multiple_of(g * GB, GB), GB)

    def fetch(g, which):
        src, buf = ((kin, kbuf), (vin, vbuf))[which]
        return pltpu.make_async_copy(src.at[layer, rows(g)], buf.at[rows(g)], in_sem.at[which, g])

    def put(g, which):
        buf, dst = ((kbuf, kout), (vbuf, vout))[which]
        return pltpu.make_async_copy(buf.at[rows(g)], dst.at[layer, rows(g)], out_sem.at[which, g])

    params = [(pos_in, pos_ref), (gain_in, gain_ref), (bias_in, bias_ref), (bq_in, bq_ref), (bv_in, bv_ref),
              (wq_in.at[layer], wq_ref), (wk_in.at[layer], wk_ref), (wv_in.at[layer], wv_ref)]
    params.append((h_in, h_ref))
    copies = [pltpu.make_async_copy(src, dst, par_sem.at[i]) for i, (src, dst) in enumerate(params)]
    for copy in copies:
        copy.start()

    def start_fetch(g, carry):
        fetch(g, 0).start()
        fetch(g, 1).start()
        return carry

    lax.fori_loop(0, GROUPS, start_fetch, 0)
    for copy in copies:
        copy.wait()

    normed = layer_norm(h_ref[...].astype(F32), row_of(gain_ref, 0, pl.ds(layer, 1)), row_of(bias_ref, 0, pl.ds(layer, 1)))
    query = ((dot_nt(normed, wq_ref[...]) + row_of(bq_ref, pl.ds(layer, 1))) * SCALE).astype(BF16).astype(F32)
    q_scr[...] = jnp.concatenate([query, query], axis=1)
    a_scr[...] = normed.astype(F32)
    eye = lax.broadcasted_iota(jnp.int32, (HD, HD), 0) == lax.broadcasted_iota(jnp.int32, (HD, HD), 1)
    bv_col = jnp.sum(jnp.where(eye, row_of(bv_ref, pl.ds(layer, 1)), 0.0), axis=1, keepdims=True)

    def project(g, carry):
        part = a_scr[rows(g)].astype(BF16)
        kt_scr[g] = dot_nt(wk_ref[...], part) * SCALE
        vt_scr[g] = dot_nt(wv_ref[...], part) + bv_col
        return carry

    lax.fori_loop(0, GROUPS, project, 0, unroll=4)

    lane_ctx = lax.broadcasted_iota(jnp.int32, (GB, CTX), 1)
    keep = lax.broadcasted_iota(jnp.int32, (GB, D), 1) // HD == lax.broadcasted_iota(jnp.int32, (GB, D), 0)

    def attend(step, carry):
        groups = [step * UNROLL + u for u in range(UNROLL)]
        pos_cols, scores, probs = [], [], []
        for g in groups:
            fetch(g, 0).wait()
            fetch(g, 1).wait()
        for g in groups:
            pos_cols.append(insert_columns(g, pos_ref, ((kbuf, kt_scr[g]), (vbuf, vt_scr[g]))))
        for g, pos_col in zip(groups, pos_cols):
            q8 = q_scr[rows(g)]
            qblk = jnp.where(keep, jnp.concatenate([q8, q8, q8, q8], axis=1), 0.0).astype(BF16)
            scores.append(jnp.where(lane_ctx <= pos_col, dot(qblk, kbuf[rows(g)].reshape(GB * HD, CTX)), -1e30))
        for score in scores:
            expd = jnp.exp(score - jnp.max(score, axis=1, keepdims=True))
            probs.append((expd / jnp.sum(expd, axis=1, keepdims=True)).astype(BF16))
        wides = [dot_nt(prob, vbuf[rows(g)].reshape(GB * HD, CTX)) for g, prob in zip(groups, probs)]
        for g, wide in zip(groups, wides):
            o_scr[rows(g)] = fold_heads(wide, keep)
            put(g, 0).start()
            put(g, 1).start()
        return carry

    lax.fori_loop(0, GROUPS // UNROLL, attend, 0)
    for half in HALVES:
        o_ref[half] = jnp.concatenate([o_scr[HALF * half:HALF * half + QUART], o_scr[HALF * half + QUART:HALF * half + HALF]], axis=1).astype(BF16)
    heads_copy = pltpu.make_async_copy(o_ref, o_out, par_sem.at[0])
    heads_copy.start()

    def finish(g, carry):
        put(g, 0).wait()
        put(g, 1).wait()
        return carry

    lax.fori_loop(0, GROUPS, finish, 0)
    heads_copy.wait()


def erf_gelu(x):
    return 0.5 * x * (1.0 + lax.erf(x * (2.0 ** -0.5)))


def tail_kernel(h_in, o_in, pos_in, gain_in, bias_in, wq_in, bq_in, wk_in, wv_in, bv_in, wo0, wo2, wo4, wo6, bo_in, wcq_in, bcq_in, wco_in, bco_in,
                w1_in, b1_in, w2_in, b2_in, ckin, cvin, skin, svin,
                out_ref, knew_ref, vnew_ref, sk, sv,
                h_ref, o_ref, pos_ref, gain_ref, bias_ref, wq_ref, bq_ref, wk_ref, wv_ref, bv_ref, bo_ref, wcq_ref, bcq_ref, bco_ref,
                w1_ref, b1_ref, w2_ref, b2_ref,
                kbuf, vbuf, wofull, wcofull, obuf, osend, q_scr, kv_scr, o_scr, hid_scr, pbuf, rbuf, base_scr, hblk, hslots,
                par_sem, wpar_sem, ck_sem, sk_sem, wsend, wrecv, send_sem, recv_sem):
    me = lax.axis_index('tp')
    peers = [lax.rem(me + d, TP) for d in (6, 4, 2, 7, 5, 3, 1)]
    core = lax.rem(me, 2)
    chip_x = lax.rem(lax.div(me, 2), 2)
    sibling = me + 1 - 2 * core
    flip_x = 2 - 4 * chip_x
    across = lax.rem(me + 4, TP)
    holders = [me, me + flip_x, across, across + flip_x]

    def fetch_cross(layer, g, which):
        src, buf = ((ckin, kbuf), (cvin, vbuf))[which]
        return pltpu.make_async_copy(src.at[layer, pl.ds(GA * g, GA)], buf.at[pl.ds(GA * g, GA)], ck_sem.at[layer, which, g])

    def fetch_self(half, which):
        src, buf = ((skin, sk), (svin, sv))[which]
        return pltpu.make_async_copy(src.at[1, pl.ds(HALF * half, HALF)], buf.at[pl.ds(HALF * half, HALF)], sk_sem.at[which, half])

    params = [(o_in, o_ref), (h_in, h_ref), (gain_in, gain_ref), (bias_in, bias_ref), (bo_in, bo_ref), (wcq_in, wcq_ref), (bcq_in, bcq_ref),
              (bco_in, bco_ref), (w1_in, w1_ref), (b1_in, b1_ref), (w2_in, w2_ref), (b2_in, b2_ref), (pos_in, pos_ref), (wq_in.at[1], wq_ref),
              (bq_in, bq_ref), (wk_in.at[1], wk_ref), (wv_in.at[1], wv_ref), (bv_in, bv_ref)]
    copies = [pltpu.make_async_copy(src, dst, par_sem.at[i]) for i, (src, dst) in enumerate(params)]
    wo_src = (wo0, wo2, wo4, wo6)
    own = [pltpu.make_async_copy(wo_src[k], wofull.at[holders[k]], wpar_sem.at[k]) for k in range(4)]
    own.append(pltpu.make_async_copy(wco_in, wcofull.at[me], wpar_sem.at[4]))

    barrier = pltpu.get_barrier_semaphore()
    for peer in peers:
        pl.semaphore_signal(barrier, inc=1, device_id={'tp': peer}, device_id_type=MESH)
    for copy in copies + own:
        copy.start()
    for g in range(AGROUPS):
        fetch_cross(0, g, 0).start()
        fetch_cross(0, g, 1).start()
    for half in HALVES:
        fetch_self(half, 0).start()
        fetch_self(half, 1).start()
    copies[0].wait()
    pl.semaphore_wait(barrier, TP - 1)

    def send(phase, src, dst, peer):
        return pltpu.make_async_remote_copy(src_ref=src, dst_ref=dst, send_sem=send_sem.at[phase, peer], recv_sem=recv_sem.at[phase, me],
                                            device_id={'tp': peer}, device_id_type=MESH)

    def arrival(phase, dst, peer):
        return pltpu.make_async_remote_copy(src_ref=dst, dst_ref=dst, send_sem=send_sem.at[phase, peer], recv_sem=recv_sem.at[phase, peer],
                                            device_id={'tp': peer}, device_id_type=MESH)

    def gather_start(phase, src, slots):
        for peer in peers:
            send(phase, src, slots.at[me], peer).start()

    def gather_wait(phase, src, slots):
        for peer in peers:
            arrival(phase, slots.at[peer], peer).wait_recv()
        for peer in peers:
            send(phase, src, slots.at[me], peer).wait_send()

    def weight_copy(row, k, src, dst, target):
        return pltpu.make_async_remote_copy(src_ref=src, dst_ref=dst, send_sem=wsend.at[row, k], recv_sem=wrecv.at[row, k],
                                            device_id={'tp': target}, device_id_type=MESH)

    wo_fwd = [weight_copy(0, k, wo_src[k], wofull.at[holders[k]], sibling) for k in range(4)]
    wco_out = [weight_copy(1, k, wco_in, wcofull.at[me], holders[k]) for k in range(1, 4)]
    wco_fwd = [weight_copy(2, 0, wco_in, wcofull.at[me], sibling)] + [
        weight_copy(2, k, wcofull.at[holders[k]], wcofull.at[holders[k]], sibling) for k in range(1, 4)]

    for half in HALVES:
        gather_start(half, o_ref.at[half], obuf.at[0, half])
    for copy in wo_fwd + wco_out + wco_fwd[:1]:
        copy.start()
    for half in HALVES:
        obuf[0, half, me] = o_ref[half]
    for copy in copies[1:] + own:
        copy.wait()

    low = lax.broadcasted_iota(jnp.int32, (QUART, LANES), 1) < HD

    def head_rows(stage, half):
        top, bottom = [], []
        for pair in range(TP // 2):
            left = obuf[stage, half, 2 * pair].astype(F32)
            right = obuf[stage, half, 2 * pair + 1].astype(F32)
            top.append(jnp.where(low, left, pltpu.roll(right, HD, 1)))
            bottom.append(jnp.where(low, pltpu.roll(left, HD, 1), right))
        return jnp.concatenate([jnp.concatenate(top, axis=1), jnp.concatenate(bottom, axis=1)], axis=0).astype(BF16)

    def norm_of(hid, layer, k):
        return layer_norm(hid, row_of(gain_ref, k, pl.ds(layer, 1)), row_of(bias_ref, k, pl.ds(layer, 1)))

    keep = lax.broadcasted_iota(jnp.int32, (GR, D), 1) // HD == lax.broadcasted_iota(jnp.int32, (GR, D), 0) // BEAMS

    def gathered_out(stage, half, full, layer, bias):
        return dot(head_rows(stage, half), full[:, layer].reshape(D, D)) + row_of(bias, pl.ds(layer, 1))

    def cross_half(layer, half, hid):
        stage = 2 * layer
        hid = hid + gathered_out(stage, half, wofull, layer, bo_ref)
        hid = hid.astype(BF16).astype(F32)
        hid_scr[half] = hid
        query = ((dot_nt(norm_of(hid, layer, 1), wcq_ref[layer]) + row_of(bcq_ref, pl.ds(layer, 1))) * SCALE).astype(BF16).astype(F32)
        q_scr[...] = jnp.concatenate([query, query], axis=1)
        groups = (2 * half, 2 * half + 1)
        for g in groups:
            fetch_cross(layer, g, 0).wait()
            fetch_cross(layer, g, 1).wait()
        scores, probs = [], []
        for i, g in enumerate(groups):
            q40 = q_scr[GR * i:GR * i + GR]
            qblk = jnp.where(keep, jnp.concatenate([q40, q40, q40, q40], axis=1), 0.0).astype(BF16)
            scores.append(dot(qblk, kbuf[GA * g:GA * g + GA].reshape(GA * HD, FRAMES)))
        for score in scores:
            expd = jnp.exp(score - jnp.max(score, axis=1, keepdims=True))
            probs.append((expd / jnp.sum(expd, axis=1, keepdims=True)).astype(BF16))
        outs = [fold_heads(dot_nt(prob, vbuf[GA * g:GA * g + GA].reshape(GA * HD, FRAMES)), keep) for g, prob in zip(groups, probs)]
        osend[stage, half] = jnp.concatenate(outs, axis=1).astype(BF16)
        gather_start(8 * layer + 2 + half, osend.at[stage, half], obuf.at[stage + 1, half])
        obuf[stage + 1, half, me] = osend[stage, half]

    def mlp_half(layer, half):
        stage = 2 * layer
        gather_wait(8 * layer + 2 + half, osend.at[stage, half], obuf.at[stage + 1, half])
        hid = hid_scr[half] + gathered_out(stage + 1, half, wcofull, layer, bco_ref)
        hid = hid.astype(BF16).astype(F32)
        inner = erf_gelu(dot(norm_of(hid, layer, 2), w1_ref[layer]) + row_of(b1_ref, pl.ds(layer, 1))).astype(BF16)
        part = dot(inner, w2_ref[layer]).astype(BF16)
        for t in range(TP):
            pbuf[layer, half, t] = part[QUART * (t % 2):QUART * (t % 2) + QUART, LANES * (t // 2):LANES * (t // 2) + LANES]
        for peer in peers:
            send(8 * layer + 4 + half, pbuf.at[layer, half, peer], rbuf.at[layer, half, me], peer).start()
        rbuf[layer, half, me] = pbuf[layer, half, me]
        base_scr[half] = hid + row_of(b2_ref, pl.ds(layer, 1))

    def reduce_half(layer, half):
        for peer in peers:
            arrival(8 * layer + 4 + half, rbuf.at[layer, half, peer], peer).wait_recv()
        total = rbuf[layer, half, 0].astype(F32)
        for t in range(1, TP):
            total = total + rbuf[layer, half, t].astype(F32)
        mine = base_scr[half, pl.ds(pl.multiple_of(QUART * core, 8), QUART), pl.ds(pl.multiple_of(LANES * lax.div(me, 2), LANES), LANES)]
        hblk[layer, half] = (mine + total).astype(BF16)
        gather_start(8 * layer + 6 + half, hblk.at[layer, half], hslots.at[layer, half])
        hslots[layer, half, me] = hblk[layer, half]

    def next_hidden(layer, half):
        gather_wait(8 * layer + 6 + half, hblk.at[layer, half], hslots.at[layer, half])
        for peer in peers:
            send(8 * layer + 4 + half, pbuf.at[layer, half, peer], rbuf.at[layer, half, me], peer).wait_send()
        cols = [jnp.concatenate([hslots[layer, half, 2 * c].astype(F32), hslots[layer, half, 2 * c + 1].astype(F32)], axis=0) for c in range(TP // 2)]
        return jnp.concatenate(cols, axis=1)

    lane_ctx = lax.broadcasted_iota(jnp.int32, (GB, CTX), 1)
    row_id = lax.broadcasted_iota(jnp.int32, (GB, 1), 0)
    keep8 = lax.broadcasted_iota(jnp.int32, (GB, D), 1) // HD == lax.broadcasted_iota(jnp.int32, (GB, D), 0)

    def self_half(half, hid):
        hid_scr[half] = hid
        normed = norm_of(hid, 1, 0)
        query = ((dot_nt(normed, wq_ref[...]) + row_of(bq_ref, pl.ds(1, 1))) * SCALE).astype(BF16)
        key = (dot_nt(normed, wk_ref[...]) * SCALE).astype(BF16)
        val = (dot_nt(normed, wv_ref[...]) + row_of(bv_ref, pl.ds(1, 1))).astype(BF16)
        knew_ref[half] = key
        vnew_ref[half] = val
        query = query.astype(F32)
        q_scr[...] = jnp.concatenate([query, query], axis=1)
        kv_scr[0] = jnp.broadcast_to(jnp.sum(query * key.astype(F32), axis=1, keepdims=True), (HALF, HD))
        kv_scr[1] = val.astype(F32)
        fetch_self(half, 0).wait()
        fetch_self(half, 1).wait()

        def attend(step, carry):
            local = [step * SELF_UNROLL + u for u in range(SELF_UNROLL)]
            rows = [pl.ds(pl.multiple_of(g * GB, GB), GB) for g in local]
            slabs = [pl.ds(pl.multiple_of(HALF * half + g * GB, GB), GB) for g in local]
            scores, hits, probs, wides = [], [], [], []
            for g, row, slab in zip(local, rows, slabs):
                pos_col = jnp.zeros((GB, 1), jnp.int32)
                for j in range(GB):
                    pos_col = jnp.where(row_id == j, pos_ref[HALF * half + g * GB + j], pos_col)
                q8 = q_scr[row]
                qblk = jnp.where(keep8, jnp.concatenate([q8, q8, q8, q8], axis=1), 0.0).astype(BF16)
                score = dot(qblk, sk[slab].reshape(GB * HD, CTX))
                hit = lane_ctx == pos_col
                score = jnp.where(hit, kv_scr[0, row][:, :1], score)
                scores.append(jnp.where(lane_ctx <= pos_col, score, -1e30))
                hits.append(hit)
            for score in scores:
                expd = jnp.exp(score - jnp.max(score, axis=1, keepdims=True))
                probs.append((expd / jnp.sum(expd, axis=1, keepdims=True)).astype(BF16).astype(F32))
            for slab, prob, hit in zip(slabs, probs, hits):
                wides.append(dot_nt(jnp.where(hit, 0.0, prob).astype(BF16), sv[slab].reshape(GB * HD, CTX)))
            for row, wide, prob, hit in zip(rows, wides, probs, hits):
                fresh = jnp.sum(jnp.where(hit, prob, 0.0), axis=1, keepdims=True) * kv_scr[1, row]
                o_scr[row] = fold_heads(wide, keep8) + fresh
            return carry

        lax.fori_loop(0, 10 // SELF_UNROLL, attend, 0)
        osend[1, half] = jnp.concatenate([o_scr[0:QUART], o_scr[QUART:HALF]], axis=1).astype(BF16)
        gather_start(8 + half, osend.at[1, half], obuf.at[2, half])
        obuf[2, half, me] = osend[1, half]

    for half in HALVES:
        gather_wait(half, o_ref.at[half], obuf.at[0, half])
        if half == 0:
            for copy in wo_fwd:
                copy.wait()
        cross_half(0, half, h_ref[HALF * half:HALF * half + HALF].astype(F32))
        if half == 0:
            for k in range(1, 4):
                weight_copy(1, k, wco_in, wcofull.at[holders[k]], holders[k]).wait_recv()
            for copy in wco_fwd[1:]:
                copy.start()
    for copy in wco_out + wco_fwd:
        copy.wait_send()
    for k in range(4):
        other = holders[k] + 1 - 2 * core
        weight_copy(2, k, wco_in, wcofull.at[other], sibling).wait_recv()
    for g in range(AGROUPS):
        fetch_cross(1, g, 0).start()
        fetch_cross(1, g, 1).start()
    for half in HALVES:
        mlp_half(0, half)
    for half in HALVES:
        reduce_half(0, half)
    for half in HALVES:
        self_half(half, next_hidden(0, half))
    for half in HALVES:
        gather_wait(8 + half, osend.at[1, half], obuf.at[2, half])
        cross_half(1, half, hid_scr[half])
    for half in HALVES:
        mlp_half(1, half)
    for half in HALVES:
        reduce_half(1, half)
    for half in HALVES:
        out_ref[HALF * half:HALF * half + HALF] = next_hidden(1, half).astype(BF16)


def write_kernel(pos_ref, h_ref, knew_ref, vnew_ref, sk_in, sv_in, kprev, vprev, h_out, kout, vout, sk, sv, new_scr, sem, out_sem):
    hidden = pltpu.make_async_copy(h_ref, h_out, sem.at[0])
    hidden.start()
    for half in HALVES:
        new_scr[0, HALF * half:HALF * half + HALF] = knew_ref[half].astype(F32)
        new_scr[1, HALF * half:HALF * half + HALF] = vnew_ref[half].astype(F32)
    eye = (lax.broadcasted_iota(jnp.int32, (HD, HD), 0) == lax.broadcasted_iota(jnp.int32, (HD, HD), 1)).astype(BF16)

    def rows(g):
        return pl.ds(pl.multiple_of(g * GB, GB), GB)

    def put(g, which):
        buf, dst = ((sk, kout), (sv, vout))[which]
        return pltpu.make_async_copy(buf.at[rows(g)], dst.at[1, rows(g)], out_sem.at[which, g])

    def insert(step, carry):
        groups = [step]
        cols = [[dot_nt(eye, new_scr[which, rows(g)].astype(BF16)) for which in HALVES] for g in groups]
        for g, pair in zip(groups, cols):
            insert_columns(g, pos_ref, ((sk, pair[0]), (sv, pair[1])))
        for g in groups:
            put(g, 0).start()
            put(g, 1).start()
        return carry

    lax.fori_loop(0, GROUPS, insert, 0)

    def finish(g, carry):
        put(g, 0).wait()
        put(g, 1).wait()
        return carry

    lax.fori_loop(0, GROUPS, finish, 0)
    hidden.wait()


HBM = pl.BlockSpec(memory_space=pltpu.HBM)
VM = pl.BlockSpec(memory_space=pltpu.VMEM)
SM = pl.BlockSpec(memory_space=pltpu.SMEM)


def in_hbm(*arrays):
    return [pltpu.with_memory_space_constraint(array, pltpu.HBM) for array in arrays]


def self_call(layer, positions, hidden, w, keys, vals):
    cache = jax.ShapeDtypeStruct(keys.shape, BF16)
    args = [positions, hidden, w['ln_gain'], w['ln_bias'], w['w_query'], w['b_query'], w['w_key'], w['w_value'], w['b_value'], keys, vals]
    return pl.pallas_call(
        functools.partial(self_kernel, layer),
        out_shape=(jax.ShapeDtypeStruct((2, BATCH // 4, 2 * HD), BF16), cache, cache),
        in_specs=[HBM] * len(args),
        out_specs=(HBM, HBM, HBM),
        scratch_shapes=[
            pltpu.VMEM((2, BATCH // 4, 2 * HD), BF16),
            pltpu.VMEM((BATCH, HD, CTX), BF16),
            pltpu.VMEM((BATCH, HD, CTX), BF16),
            pltpu.SMEM((BATCH,), jnp.int32),
            pltpu.VMEM((BATCH, D), BF16),
            pltpu.VMEM((3, 2, D), BF16),
            pltpu.VMEM((3, 2, D), BF16),
            pltpu.VMEM((HD, D), BF16),
            pltpu.VMEM((2, HD), BF16),
            pltpu.VMEM((HD, D), BF16),
            pltpu.VMEM((HD, D), BF16),
            pltpu.VMEM((2, HD), BF16),
            pltpu.VMEM((BATCH, 2 * HD), F32),
            pltpu.VMEM((BATCH, D), F32),
            pltpu.VMEM((GROUPS, HD, GB), F32),
            pltpu.VMEM((GROUPS, HD, GB), F32),
            pltpu.VMEM((BATCH, HD), F32),
            pltpu.SemaphoreType.DMA((9,)),
            pltpu.SemaphoreType.DMA((2, GROUPS)),
            pltpu.SemaphoreType.DMA((2, GROUPS)),
        ],
        compiler_params=pltpu.CompilerParams(vmem_limit_bytes=VMEM_LIMIT),
        cost_estimate=pl.CostEstimate(flops=10 ** 10, bytes_accessed=42 * 2 ** 20, transcendentals=BATCH * CTX),
        name=f'self_attention_{layer}',
    )(*in_hbm(*args))


def tail_call(positions, hidden, heads, w, wo, cross_k, cross_v, keys, vals):
    args = [hidden, heads, positions, w['ln_gain'], w['ln_bias'], w['w_query'], w['b_query'], w['w_key'], w['w_value'], w['b_value'], *wo, w['b_out'],
            w['w_cquery'], w['b_cquery'], w['w_cout'], w['b_cout'], w['w_fc1'], w['b_fc1'], w['w_fc2'], w['b_fc2'], cross_k, cross_v, keys, vals]
    new = jax.ShapeDtypeStruct((2, BATCH // 2, HD), BF16)
    cache = jax.ShapeDtypeStruct((BATCH, HD, CTX), BF16)
    pair = (2, TP, QUART, LANES)
    return pl.pallas_call(
        tail_kernel,
        out_shape=(jax.ShapeDtypeStruct((BATCH, D), BF16), new, new, cache, cache),
        in_specs=[HBM] * len(args),
        out_specs=(VM,) * 5,
        scratch_shapes=[
            pltpu.VMEM((BATCH, D), BF16),
            pltpu.VMEM((2, BATCH // 4, 2 * HD), BF16),
            pltpu.SMEM((BATCH,), jnp.int32),
            pltpu.VMEM((3, 2, D), BF16),
            pltpu.VMEM((3, 2, D), BF16),
            pltpu.VMEM((HD, D), BF16),
            pltpu.VMEM((2, HD), BF16),
            pltpu.VMEM((HD, D), BF16),
            pltpu.VMEM((HD, D), BF16),
            pltpu.VMEM((2, HD), BF16),
            pltpu.VMEM((2, D), BF16),
            pltpu.VMEM((2, HD, D), BF16),
            pltpu.VMEM((2, HD), BF16),
            pltpu.VMEM((2, D), BF16),
            pltpu.VMEM((2, D, 256), BF16),
            pltpu.VMEM((2, 256), BF16),
            pltpu.VMEM((2, 256, D), BF16),
            pltpu.VMEM((2, D), BF16),
            pltpu.VMEM((AUD, HD, FRAMES), BF16),
            pltpu.VMEM((AUD, HD, FRAMES), BF16),
            pltpu.VMEM((TP, 2, HD, D), BF16),
            pltpu.VMEM((TP, 2, HD, D), BF16),
            pltpu.VMEM((4,) + pair, BF16),
            pltpu.VMEM((3, 2, QUART, LANES), BF16),
            pltpu.VMEM((BATCH // 2, 2 * HD), F32),
            pltpu.VMEM((2, BATCH // 2, HD), F32),
            pltpu.VMEM((BATCH // 2, HD), F32),
            pltpu.VMEM((2, BATCH // 2, D), F32),
            pltpu.VMEM((2,) + pair, BF16),
            pltpu.VMEM((2,) + pair, BF16),
            pltpu.VMEM((2, BATCH // 2, D), F32),
            pltpu.VMEM((2, 2, QUART, LANES), BF16),
            pltpu.VMEM((2,) + pair, BF16),
            pltpu.SemaphoreType.DMA((18,)),
            pltpu.SemaphoreType.DMA((5,)),
            pltpu.SemaphoreType.DMA((2, 2, AGROUPS)),
            pltpu.SemaphoreType.DMA((2, 2)),
            pltpu.SemaphoreType.DMA((3, 4)),
            pltpu.SemaphoreType.DMA((3, 4)),
            pltpu.SemaphoreType.DMA((16, TP)),
            pltpu.SemaphoreType.DMA((16, TP)),
        ],
        compiler_params=pltpu.CompilerParams(vmem_limit_bytes=TAIL_LIMIT, collective_id=0, has_side_effects=True),
        cost_estimate=pl.CostEstimate(flops=10 ** 10, bytes_accessed=46 * 2 ** 20, transcendentals=2 * BATCH * FRAMES),
        name='cross_mlp_and_next_layer',
    )(*in_hbm(*args))


def write_call(positions, hidden, knew, vnew, sk, sv, kprev, vprev):
    held = jax.ShapeDtypeStruct(sk.shape, BF16)
    cache = jax.ShapeDtypeStruct(kprev.shape, BF16)
    return pl.pallas_call(
        write_kernel,
        out_shape=(jax.ShapeDtypeStruct(hidden.shape, BF16), cache, cache, held, held),
        in_specs=[SM, VM, VM, VM, VM, VM, HBM, HBM],
        out_specs=(HBM, HBM, HBM, VM, VM),
        input_output_aliases={4: 3, 5: 4, 6: 1, 7: 2},
        scratch_shapes=[
            pltpu.VMEM((2, BATCH, HD), F32),
            pltpu.SemaphoreType.DMA((1,)),
            pltpu.SemaphoreType.DMA((2, GROUPS)),
        ],
        compiler_params=pltpu.CompilerParams(vmem_limit_bytes=WRITE_LIMIT),
        cost_estimate=pl.CostEstimate(flops=10 ** 8, bytes_accessed=21 * 2 ** 20, transcendentals=0),
        name='write_caches',
    )(positions, hidden, knew, vnew, sk, sv, *in_hbm(kprev, vprev))


def solution(mesh):
    cache_spec = P(None, 'dp', None, 'tp', None)
    col_spec = P(None, None, 'tp')
    row_spec = P(None, 'tp', None)
    vec_spec = P(None, 'tp')
    param_specs = {'ln_gain': P(), 'ln_bias': P(), 'w_query': col_spec, 'b_query': vec_spec, 'w_key': col_spec, 'w_value': col_spec, 'b_value': vec_spec, 'w_out': row_spec, 'b_out': P(), 'w_cquery': col_spec, 'b_cquery': vec_spec, 'w_cout': row_spec, 'b_cout': P(), 'w_fc1': col_spec, 'b_fc1': vec_spec, 'w_fc2': row_spec, 'b_fc2': P()}
    in_specs = (P('dp', None), P('dp'), cache_spec, cache_spec, cache_spec, cache_spec) + tuple(param_specs[param_name] for param_name in PARAM_NAMES)

    def lanes_last(cache):
        return jnp.transpose(cache, (0, 1, 3, 4, 2)).reshape(cache.shape[0], cache.shape[1], cache.shape[4], cache.shape[2])

    def slots_back(cache):
        layers, beams, width, slots = cache.shape
        return jnp.transpose(cache.reshape(layers, beams, 1, width, slots), (0, 1, 4, 2, 3))

    def local_step(hidden, positions, self_keys, self_vals, cross_keys, cross_vals, *layer_params):
        w = dict(zip(PARAM_NAMES, layer_params))
        for name in ('w_query', 'w_key', 'w_value', 'w_cquery'):
            w[name] = jnp.transpose(w[name], (0, 2, 1))
        for name in ('ln_gain', 'ln_bias'):
            w[name] = jnp.transpose(w[name], (1, 0, 2))
        keys, vals, cross_k, cross_v = (lanes_last(c) for c in (self_keys, self_vals, cross_keys, cross_vals))
        wo = [w['w_out']] + [lax.ppermute(w['w_out'], 'tp', [(i, i ^ flip) for i in range(TP)]) for flip in (2, 4, 6)]
        heads, *prev = self_call(0, positions, hidden, w, keys, vals)
        hidden, *held = tail_call(positions, hidden, heads, w, wo, cross_k, cross_v, keys, vals)
        hidden, *prev = write_call(positions, hidden, *held, *prev)
        return hidden, slots_back(prev[0]), slots_back(prev[1])

    return jax.shard_map(local_step, mesh=mesh, in_specs=in_specs, out_specs=(P('dp', None), cache_spec, cache_spec), check_vma=False)
```
